16 devices in a mesh: replica: 2 (over z), data: 8 (over y, x, core).
Axes of the slice: x: 2, y: 2, z: 2, core: 2. Of those that a mesh axis runs over, the one named last changes fastest.
Arguments:
- w_one: bfloat16 [4, 1280, 5120], replicated
- w_two: bfloat16 [4, 5120, 1280], replicated
- x_in: bfloat16 [48, 2, 128, 1280], P(('replica', 'data'))
- dy_in: bfloat16 [48, 2, 128, 1280], P(('replica', 'data'))
Outputs:
- output 1: bfloat16 [4, 1280, 5120], replicated
- output 2: bfloat16 [4, 5120, 1280], replicated
- output 3: bfloat16 [48, 2, 128, 1280], P(('replica', 'data'))
All inputs are finite; a program needn't handle non-finite values.
Results may differ from the reference program's by a relative error of at most 0.0160137.
Values are sent between devices in bfloat16 or wider.
A program may use at most 1 GiB of HBM per device.

```python
import jax
import jax.numpy as jnp
from jax import lax

N_REPLICA = 2
N_DATA = 8
D_MODEL = 1280
D_FF = 5120
LAYERS = 4
MICROBATCHES = 3
MB_SEQS = 2
SEQ_LEN = 128


def setup_inputs(seed: int = 0) -> dict:
    base_key = jax.random.key(seed)
    k_x, k_dy, k_one, k_two = jax.random.split(base_key, 4)
    row_count = N_REPLICA * N_DATA * MICROBATCHES
    shape_x = (row_count, MB_SEQS, SEQ_LEN, D_MODEL)
    x_in = jax.random.normal(k_x, shape_x, jnp.float32).astype(jnp.bfloat16)
    dy_in = jax.random.normal(k_dy, shape_x, jnp.float32).astype(jnp.bfloat16)
    w_one = (jax.random.normal(k_one, (LAYERS, D_MODEL, D_FF), jnp.float32) * D_MODEL ** -0.5).astype(jnp.bfloat16)
    w_two = (jax.random.normal(k_two, (LAYERS, D_FF, D_MODEL), jnp.float32) * D_FF ** -0.5).astype(jnp.bfloat16)
    return {"w_one": w_one, "w_two": w_two, "x_in": x_in, "dy_in": dy_in}


def gelu_tanh(value):
    return jax.nn.gelu(value, approximate=True)


def block_forward(hidden, weights):
    w_up, w_down = weights
    pre_act = jnp.dot(hidden, w_up, preferred_element_type=jnp.float32).astype(jnp.bfloat16)
    gelu_out = gelu_tanh(pre_act.astype(jnp.float32)).astype(jnp.bfloat16)
    new_hidden = (hidden.astype(jnp.float32) + jnp.dot(gelu_out, w_down, preferred_element_type=jnp.float32)).astype(jnp.bfloat16)
    return new_hidden, (hidden, pre_act, gelu_out)


def block_backward(upstream, block_data):
    w_up, w_down, hidden, pre_act, gelu_out = block_data
    grad_b = upstream.astype(jnp.bfloat16)
    d_two = jnp.dot(gelu_out.T, grad_b, preferred_element_type=jnp.float32)
    d_act = jnp.dot(grad_b, w_down.T, preferred_element_type=jnp.float32)
    d_pre = jax.vjp(gelu_tanh, pre_act.astype(jnp.float32))[1](d_act)[0].astype(jnp.bfloat16)
    d_one = jnp.dot(hidden.T, d_pre, preferred_element_type=jnp.float32)
    new_upstream = upstream + jnp.dot(d_pre, w_up.T, preferred_element_type=jnp.float32)
    return new_upstream, (d_one, d_two)


def micro_grads(w_one, w_two, x_mb, dy_mb):
    tokens = x_mb.reshape(-1, D_MODEL)
    _, saved_acts = lax.scan(block_forward, tokens, (w_one, w_two))
    upstream = dy_mb.reshape(-1, D_MODEL).astype(jnp.float32)
    grad_in, (d_one, d_two) = lax.scan(block_backward, upstream, (w_one, w_two) + saved_acts, reverse=True)
    return d_one, d_two, grad_in.astype(jnp.bfloat16).reshape(x_mb.shape)


def reference(w_one, w_two, x_in, dy_in):
    def micro_body(acc_pair, mb_pair):
        acc_one, acc_two = acc_pair
        d_one, d_two, dx_mb = micro_grads(w_one, w_two, mb_pair[0], mb_pair[1])
        return (acc_one + d_one, acc_two + d_two), dx_mb
    start_acc = (jnp.zeros(w_one.shape, jnp.float32), jnp.zeros(w_two.shape, jnp.float32))
    (acc_one, acc_two), dx_out = lax.scan(micro_body, start_acc, (x_in, dy_in))
    return acc_one.astype(jnp.bfloat16), acc_two.astype(jnp.bfloat16), dx_out
```

```python
import functools

import jax
import jax.numpy as jnp
from jax import lax
from jax.experimental import pallas as pl
from jax.experimental.pallas import tpu as pltpu
from jax.sharding import PartitionSpec as P

AXES = ("replica", "data")


def gelu_tanh(value):
    return jax.nn.gelu(value, approximate=True)


def dot(lhs, rhs, lhs_dim, rhs_dim):
    return lax.dot_general(lhs, rhs, (((lhs_dim,), (rhs_dim,)), ((), ())), preferred_element_type=jnp.float32)


def place_body(piece_ref, *refs):
    refs[-1][0] = piece_ref[...]


def place(piece, stacked, layer, layers):
    rows, cols = piece.shape
    step = rows // 10
    spec = pl.BlockSpec((step, cols), lambda i: (i, 0))
    args, specs, alias = [piece], [spec], {}
    if stacked is not None:
        args.append(stacked)
        specs.append(pl.BlockSpec(memory_space=pl.ANY))
        alias = {1: 0}
    return pl.pallas_call(
        place_body,
        grid=(10,),
        out_shape=jax.ShapeDtypeStruct((layers, rows, cols), piece.dtype),
        in_specs=specs,
        out_specs=pl.BlockSpec((1, step, cols), lambda i: (layer, i, 0)),
        input_output_aliases=alias,
        cost_estimate=pl.CostEstimate(flops=rows * cols * 60, bytes_accessed=4 * rows * cols, transcendentals=0),
        name="place",
    )(*args)


def total(grad):
    shard = lax.psum_scatter(grad.astype(jnp.bfloat16), AXES, scatter_dimension=0, tiled=True)
    return lax.all_gather(shard, AXES, axis=0, tiled=True)


def solution(mesh):
    batch_spec = P(AXES)

    def per_device(w_one, w_two, x_loc, dy_loc):
        layers, width, _ = w_one.shape
        hidden = x_loc.reshape(-1, width)
        saved = []
        for layer in range(layers):
            pre_act = dot(hidden, w_one[layer], 1, 0).astype(jnp.bfloat16)
            act = gelu_tanh(pre_act.astype(jnp.float32)).astype(jnp.bfloat16)
            saved.append((hidden, pre_act, act))
            if layer < layers - 1:
                hidden = (hidden.astype(jnp.float32) + dot(act, w_two[layer], 1, 0)).astype(jnp.bfloat16)
        grad = dy_loc.reshape(-1, width).astype(jnp.float32)
        out_one = out_two = None
        for layer in reversed(range(layers)):
            hidden, pre_act, act = saved[layer]
            grad_b = grad.astype(jnp.bfloat16)
            t_two = total(dot(act, grad_b, 0, 0))
            d_act = dot(grad_b, w_two[layer], 1, 1)
            d_pre = jax.vjp(gelu_tanh, pre_act.astype(jnp.float32))[1](d_act)[0].astype(jnp.bfloat16)
            t_one = total(dot(hidden, d_pre, 0, 0))
            grad = grad + dot(d_pre, w_one[layer], 1, 1)
            out_two = place(t_two, out_two, layer, layers)
            out_one = place(t_one, out_one, layer, layers)
        return out_one, out_two, grad.astype(jnp.bfloat16).reshape(x_loc.shape)

    return jax.shard_map(per_device, mesh=mesh, in_specs=(P(), P(), batch_spec, batch_spec), out_specs=(P(), P(), batch_spec), check_vma=False)
```

```python
import functools

import jax
import jax.numpy as jnp
from jax import lax
from jax.experimental import pallas as pl
from jax.experimental.pallas import tpu as pltpu
from jax.sharding import PartitionSpec as P

AXES = ("replica", "data")
MESH = pl.DeviceIdType.MESH
BF16, F32 = jnp.bfloat16, jnp.float32
VMEM_LIMIT = 67_043_328
C0, C1 = 0.7978845608028654, 0.044715
UNIT_ROWS = 256
SLOTS, RECV, LAG = 9, 6, 2


def gelu(v):
    return 0.5 * v * (1.0 + jnp.tanh(C0 * (v + C1 * (v * v * v))))


def gelu_slope(v):
    sq = v * v
    t = jnp.tanh(C0 * (v + C1 * (sq * v)))
    return 0.5 * (1.0 + t) + 0.5 * v * (1.0 - t * t) * (C0 * (1.0 + 3.0 * C1 * sq))


def mm(lhs, rhs, lhs_dim, rhs_dim):
    return lax.dot_general(lhs, rhs, (((lhs_dim,), (rhs_dim,)), ((), ())), preferred_element_type=F32)


def forward_body(x_ref, w1_ref, w2_ref, u_ref, a_ref, h_ref, hid, acc, *, layers, chunks):
    layer, j = pl.program_id(0), pl.program_id(1)

    @pl.when(jnp.logical_and(layer == 0, j == 0))
    def _():
        hid[...] = x_ref[...]

    @pl.when(j == 0)
    def _():
        h_ref[0] = hid[...]
        acc[...] = hid[...].astype(F32)

    pre = mm(hid[...], w1_ref[0], 1, 0).astype(BF16)
    u_ref[0] = pre
    act = gelu(pre.astype(F32)).astype(BF16)
    a_ref[0] = act

    @pl.when(layer < layers - 1)
    def _():
        acc[...] += mm(act, w2_ref[0], 1, 0)

        @pl.when(j == chunks - 1)
        def _():
            hid[...] = acc[...].astype(BF16)


def forward(x, w_one, w_two):
    layers, width, wide = w_one.shape
    tokens = x.shape[0]
    chunk = width
    chunks = wide // chunk
    act = jax.ShapeDtypeStruct((layers, tokens, wide), BF16)
    return pl.pallas_call(
        functools.partial(forward_body, layers=layers, chunks=chunks),
        grid=(layers, chunks),
        out_shape=[act, act, jax.ShapeDtypeStruct((layers, tokens, width), BF16)],
        in_specs=[
            pl.BlockSpec((tokens, width), lambda l, j: (0, 0)),
            pl.BlockSpec((1, width, chunk), lambda l, j: (l, 0, j)),
            pl.BlockSpec((1, chunk, width), lambda l, j: (l, j, 0)),
        ],
        out_specs=[
            pl.BlockSpec((1, tokens, chunk), lambda l, j: (l, 0, j)),
            pl.BlockSpec((1, tokens, chunk), lambda l, j: (l, 0, j)),
            pl.BlockSpec((1, tokens, width), lambda l, j: (l, 0, 0)),
        ],
        scratch_shapes=[pltpu.VMEM((tokens, width), BF16), pltpu.VMEM((tokens, width), F32)],
        compiler_params=pltpu.CompilerParams(vmem_limit_bytes=VMEM_LIMIT),
        name="forward",
    )(x, w_one, w_two)


def backward_body(
    w1, w2, u, a, h, dy,
    tot, dx, a_sib, h_sib, du_sib, gb_sib,
    a_cat, du_cat, h_cat, gb_cat, g, w2c, w1c, uc, du_st, unit, rcv1, rcv2, rcv3,
    s_rs1, s_rs2, s_rs3, s_ag1, s_ag2, s_ag3, s_fwd, s_own,
    r_rs1, r_rs2, r_rs3, r_ag1, r_ag2, r_ag3, r_fwd,
    c_rs1, c_rs2, c_rs3,
    s_a, r_a, l_a, l_a2, s_du, r_du, l_du, s_gb, r_gb, l_gb, l_gb2, s_h, r_h, l_h, l_h2, l_w2, l_w1, l_u, l_dx,
    *, layers, tokens, width, wide, rows,
):
    half = wide // 2
    nu = half // rows
    nm = width // rows
    hn = nu // 2
    chunk = wide // nu
    units = 2 * nu * layers
    z, rest = lax.axis_index("replica"), lax.axis_index("data")
    core, x, y = rest % 2, (rest // 2) % 2, rest // 4

    def pick(axis):
        return (1 - axis) * (2 - axis) // 2, axis * (2 - axis), axis * (axis - 1) // 2

    def bit(axis):
        ex, ey, ez = pick(axis)
        return ex * x + ey * y + ez * z

    def peer(axis):
        ex, ey, ez = pick(axis)
        px, py, pz = x + ex * (1 - 2 * x), y + ey * (1 - 2 * y), z + ez * (1 - 2 * z)
        return (pz, (py * 2 + px) * 2 + core)

    sibling = (z, (y * 2 + x) * 2 + 1 - core)

    def send(src, dst, ssem, rsem, to):
        return pltpu.make_async_remote_copy(src_ref=src, dst_ref=dst, send_sem=ssem, recv_sem=rsem, device_id=to, device_id_type=MESH)

    def place(n):
        p, q, r = n % 3, (n + 1) % 3, (n + 2) % 3
        k1 = 4 * bit(p)
        k2 = k1 + 2 * bit(q)
        return p, q, r, k1, k2, k2 + bit(r)

    def rs1(n):
        p, q, r, k1, k2, own = place(n)
        return send(unit.at[n % SLOTS, pl.ds(4 - k1, 4)], rcv1.at[n % RECV], s_rs1.at[n % SLOTS], r_rs1.at[n % RECV], peer(p))

    def rs2(n):
        p, q, r, k1, k2, own = place(n)
        return send(unit.at[n % SLOTS, pl.ds(k1 + 2 - (k2 - k1), 2)], rcv2.at[n % RECV], s_rs2.at[n % SLOTS], r_rs2.at[n % RECV], peer(q))

    def rs3(n):
        p, q, r, k1, k2, own = place(n)
        return send(unit.at[n % SLOTS, pl.ds(k2 + 1 - (own - k2), 1)], rcv3.at[n % RECV], s_rs3.at[n % SLOTS], r_rs3.at[n % RECV], peer(r))

    def own_copy(n):
        own = place(n)[5]
        return pltpu.make_async_copy(unit.at[n % SLOTS, pl.ds(own, 1)], tot.at[n, core, pl.ds(own, 1)], s_own.at[n % SLOTS])

    def ag1(n):
        p, q, r, k1, k2, own = place(n)
        return send(unit.at[n % SLOTS, pl.ds(own, 1)], tot.at[n, core, pl.ds(own, 1)], s_ag1.at[n % SLOTS], r_ag1.at[n % SLOTS], peer(r))

    def ag2(n):
        p, q, r, k1, k2, own = place(n)
        part = tot.at[n, core, pl.ds(k2, 2)]
        return send(part, part, s_ag2.at[n % SLOTS], r_ag2.at[n % SLOTS], peer(q))

    def ag3(n):
        p, q, r, k1, k2, own = place(n)
        part = tot.at[n, core, pl.ds(k1, 4)]
        return send(part, part, s_ag3.at[n % SLOTS], r_ag3.at[n % SLOTS], peer(p))

    def fwd(n):
        part = tot.at[n, core]
        return send(part, part, s_fwd.at[n % SLOTS], r_fwd.at[n % SLOTS], sibling)

    def add(n, block, rcv, j):
        slot = n % SLOTS
        unit[slot, block] = (unit[slot, block].astype(F32) + rcv[n % RECV, j].astype(F32)).astype(BF16)

    def credit(sem, n, axis):
        @pl.when(n + RECV < units)
        def _():
            pl.semaphore_signal(sem.at[n % RECV], inc=1, device_id=peer(axis), device_id_type=MESH)

    def spend(sem, n):
        @pl.when(n >= RECV)
        def _():
            pl.semaphore_wait(sem.at[n % RECV], 1)

    def live(n):
        return jnp.logical_and(n >= 0, n < units)

    def comm(t):
        n1, n2, n3, n4, n5, n6, n7 = (t - k * LAG for k in range(1, 8))

        @pl.when(live(n3))
        def _():
            p, q, r, k1, k2, own = place(n3)
            rs3(n3).wait_recv()
            add(n3, own, rcv3, 0)
            credit(c_rs3, n3, r)
            rs2(n3).wait_send()

        @pl.when(live(n2))
        def _():
            p, q, r, k1, k2, own = place(n2)
            rs2(n2).wait_recv()
            add(n2, k2 + 1 - (own - k2), rcv2, 1 - (own - k2))
            add(n2, own, rcv2, own - k2)
            credit(c_rs2, n2, q)
            rs1(n2).wait_send()

        @pl.when(live(n1))
        def _():
            p, q, r, k1, k2, own = place(n1)
            rs1(n1).wait_recv()
            keep = k2 - k1
            for j in range(2):
                add(n1, k1 + 2 - keep + j, rcv1, 2 - keep + j)
            for j in range(2):
                add(n1, k2 + j, rcv1, keep + j)
            credit(c_rs1, n1, p)

        @pl.when(live(n3))
        def _():
            own_copy(n3).start()
            ag1(n3).start()

        @pl.when(live(n2))
        def _():
            spend(c_rs3, n2)
            rs3(n2).start()

        @pl.when(live(n1))
        def _():
            spend(c_rs2, n1)
            rs2(n1).start()

        @pl.when(live(n4))
        def _():
            rs3(n4).wait_send()
            own_copy(n4).wait()
            ag1(n4).wait()
            ag2(n4).start()

        @pl.when(live(n5))
        def _():
            ag2(n5).wait()
            ag3(n5).start()

        @pl.when(live(n6))
        def _():
            ag3(n6).wait()
            fwd(n6).start()

        @pl.when(live(n7))
        def _():
            fwd(n7).wait()

    def push_unit(t):
        spend(c_rs1, t)
        rs1(t).start()

    def chunk_at(i):
        mine = i // hn
        return pl.multiple_of(((1 - core) + mine * (2 * core - 1)) * half + (i % hn) * chunk, 128)

    def loads(layer, i, slot):
        f0 = chunk_at(i)
        return (
            pltpu.make_async_copy(w2.at[layer, pl.ds(f0, chunk)], w2c.at[slot], l_w2.at[slot]),
            pltpu.make_async_copy(w1.at[layer, :, pl.ds(f0, chunk)], w1c.at[slot], l_w1.at[slot]),
            pltpu.make_async_copy(u.at[layer, :, pl.ds(f0, chunk)], uc.at[slot], l_u.at[slot]),
        )

    def cols(i):
        return pl.ds(pl.multiple_of(i * rows, 128), rows)

    def a_half(layer, i, which):
        return a.at[layer, :, pl.ds(pl.multiple_of(which * half + i * rows, 128), rows)]

    def a_load(layer, i):
        return pltpu.make_async_copy(a_half(layer, i, core), a_cat.at[pl.ds(0, tokens), cols(i)], l_a.at[i])

    def a_load2(layer, i):
        return pltpu.make_async_copy(a_sib.at[layer, :, cols(i)], a_cat.at[pl.ds(tokens, tokens), cols(i)], l_a2.at[i])

    def a_first(i):
        return send(a_half(layers - 1, i, 1 - core), a_cat.at[pl.ds(tokens, tokens), cols(i)], s_a.at[i], l_a2.at[i], sibling)

    def a_push(layer, i):
        return send(a_half(layer, i, 1 - core), a_sib.at[layer, :, cols(i)], s_a.at[i], r_a.at[layer % 2, i], sibling)

    def du_cols(i):
        return pl.ds(pl.multiple_of((i % hn) * chunk, 128), chunk)

    def du_push(layer, i):
        return send(du_st.at[i % 2], du_sib.at[layer, :, du_cols(i)], s_du.at[i % hn], r_du.at[i % hn], sibling)

    def du_load(layer, i):
        return pltpu.make_async_copy(du_sib.at[layer, :, du_cols(i)], du_cat.at[pl.ds(tokens, tokens), du_cols(i)], l_du.at[i % hn])

    own_rows, sib_rows = pl.ds(0, tokens), pl.ds(tokens, tokens)

    def h_push(layer):
        return send(h.at[layer], h_sib.at[layer], s_h, r_h, sibling)

    def h_load(layer):
        return pltpu.make_async_copy(h.at[layer], h_cat.at[own_rows], l_h)

    def h_load2(layer):
        return pltpu.make_async_copy(h_sib.at[layer], h_cat.at[sib_rows], l_h2)

    def gb_push(layer):
        return send(gb_cat.at[own_rows], gb_sib.at[layer], s_gb, r_gb, sibling)

    def gb_load2(layer):
        return pltpu.make_async_copy(gb_sib.at[layer], gb_cat.at[sib_rows], l_gb2)

    def dx_store():
        return pltpu.make_async_copy(gb_cat.at[own_rows], dx, l_dx)

    barrier = pltpu.get_barrier_semaphore()
    for to in (peer(0), peer(1), peer(2), sibling):
        pl.semaphore_signal(barrier, inc=1, device_id=to, device_id_type=MESH)
    top = layers - 1
    gb_first = pltpu.make_async_copy(dy, gb_cat.at[own_rows], l_gb)
    gb_first.start()
    for i in range(nu):
        a_load(top, i).start()
    for load in loads(top, 0, 0):
        load.start()
    pl.semaphore_wait(barrier, 4)
    dy_push = send(dy, gb_cat.at[sib_rows], s_gb, l_gb2, sibling)
    dy_push.start()
    for i in range(nu):
        a_first(i).start()
    gb_first.wait()
    g[...] = gb_cat[own_rows].astype(F32)
    dy_push.wait_send()
    for i in range(nu):
        a_first(i).wait_send()

    def layer_step(li, carry):
        layer = layers - 1 - li
        base = li * 2 * nu
        gb_load2(layer).wait()

        def first(i, carry):
            t = base + i
            a_load(layer, i).wait()
            a_load2(layer, i).wait()
            part = mm(a_cat[:, cols(i)], gb_cat[...], 0, 0)
            unit[t % SLOTS] = part.reshape(8, rows // 8, width).astype(BF16)

            @pl.when(i < nu - 1)
            def _():
                for load in loads(layer, i + 1, (i + 1) % 2):
                    load.start()

            comm(t)
            push_unit(t)

            @pl.when(i == 0)
            def _():
                h_push(layer).start()
                h_load(layer).start()

            @pl.when(i == hn)
            def _():
                h_push(layer).wait()
                h_load2(layer).start()

            @pl.when(layer > 0)
            def _():
                @pl.when(i > 0)
                def _():
                    a_push(layer - 1, i - 1).wait_send()

                a_push(layer - 1, i).start()

            for load in loads(layer, i, i % 2):
                load.wait()
            d_act = mm(gb_cat[own_rows], w2c[i % 2], 1, 1)
            du = (d_act * gelu_slope(uc[i % 2].astype(F32))).astype(BF16)

            @pl.when(jnp.logical_and(i >= 2, i < hn + 2))
            def _():
                du_push(layer, i - 2).wait_send()

            @pl.when(i < hn)
            def _():
                du_st[i % 2] = du

            @pl.when(i >= hn)
            def _():
                du_cat[own_rows, du_cols(i)] = du
                du_push(layer, i - hn).wait_recv()
                du_load(layer, i - hn).start()

            g[...] += mm(du, w1c[i % 2], 1, 1)

            @pl.when(i < hn)
            def _():
                du_push(layer, i).start()

            return carry

        lax.fori_loop(0, nu, first, 0)
        gb_cat[own_rows] = g[...].astype(BF16)
        h_load(layer).wait()
        h_load2(layer).wait()
        for i in range(hn):
            du_load(layer, i).wait()

        def second(i, carry):
            t = base + nu + i
            mi, fi = i % nm, i // nm
            part = mm(h_cat[:, cols(mi)], du_cat[:, pl.ds(pl.multiple_of(fi * width, 128), width)], 0, 0)
            unit[t % SLOTS] = part.reshape(8, rows // 8, width).astype(BF16)
            comm(t)
            push_unit(t)

            @pl.when(layer > 0)
            def _():
                @pl.when(i == 0)
                def _():
                    for load in loads(layer - 1, 0, 0):
                        load.start()
                    a_push(layer - 1, nu - 1).wait_send()
                    gb_push(layer - 1).start()

                @pl.when(i == hn)
                def _():
                    gb_push(layer - 1).wait()
                    gb_load2(layer - 1).start()

                a_push(layer - 1, i).wait_recv()
                a_load(layer - 1, i).start()
                a_load2(layer - 1, i).start()

            @pl.when(jnp.logical_and(layer == 0, i == 0))
            def _():
                dx_store().start()

            return carry

        lax.fori_loop(0, nu, second, 0)
        return carry

    lax.fori_loop(0, layers, layer_step, 0)

    def drain(t, carry):
        comm(t)
        return carry

    lax.fori_loop(units, units + 7 * LAG, drain, 0)
    dx_store().wait()


def backward(w_one, w_two, u, a, h, dy, rows):
    layers, width, wide = w_one.shape
    tokens = dy.shape[0]
    half = wide // 2
    nu = half // rows
    hn = nu // 2
    chunk = wide // nu
    units = 2 * nu * layers
    dma, reg = pltpu.SemaphoreType.DMA, pltpu.SemaphoreType.REGULAR
    hbm = pl.BlockSpec(memory_space=pl.ANY)
    sub = rows // 8
    shape = jax.ShapeDtypeStruct
    outs = [
        shape((units, 2, 8, sub, width), BF16),
        shape((tokens, width), BF16),
        shape((layers, tokens, half), BF16),
        shape((layers, tokens, width), BF16),
        shape((layers, tokens, half), BF16),
        shape((layers, tokens, width), BF16),
    ]
    scratch = [
        pltpu.VMEM((2 * tokens, half), BF16),
        pltpu.VMEM((2 * tokens, half), BF16),
        pltpu.VMEM((2 * tokens, width), BF16),
        pltpu.VMEM((2 * tokens, width), BF16),
        pltpu.VMEM((tokens, width), F32),
        pltpu.VMEM((2, chunk, width), BF16),
        pltpu.VMEM((2, width, chunk), BF16),
        pltpu.VMEM((2, tokens, chunk), BF16),
        pltpu.VMEM((2, tokens, chunk), BF16),
        pltpu.VMEM((SLOTS, 8, sub, width), BF16),
        pltpu.VMEM((RECV, 4, sub, width), BF16),
        pltpu.VMEM((RECV, 2, sub, width), BF16),
        pltpu.VMEM((RECV, 1, sub, width), BF16),
        *[dma((SLOTS,))] * 8,
        *[dma((RECV,))] * 3,
        *[dma((SLOTS,))] * 4,
        *[reg((RECV,))] * 3,
        dma((nu,)), dma((2, nu)), dma((nu,)), dma((nu,)),
        dma((hn,)), dma((hn,)), dma((hn,)),
        dma, dma, dma, dma,
        dma, dma, dma, dma,
        dma((2,)), dma((2,)), dma((2,)), dma,
    ]
    return pl.pallas_call(
        functools.partial(backward_body, layers=layers, tokens=tokens, width=width, wide=wide, rows=rows),
        out_shape=outs,
        in_specs=[hbm] * 6,
        out_specs=[hbm] * 6,
        scratch_shapes=scratch,
        compiler_params=pltpu.CompilerParams(collective_id=0, has_side_effects=True, vmem_limit_bytes=VMEM_LIMIT),
        name="backward",
    )(w_one, w_two, u, a, h, dy)


def assemble_body(tot_ref, out_ref):
    out_ref[0] = tot_ref[0, 0].reshape(out_ref.shape[1:])


def assemble(tot, layers, width, wide, rows):
    nu = wide // 2 // rows
    nm = width // rows
    nf = wide // width
    sub = rows // 8

    def call(grid, index, shape, out_index):
        return pl.pallas_call(
            assemble_body,
            grid=grid,
            out_shape=jax.ShapeDtypeStruct(shape, BF16),
            in_specs=[pl.BlockSpec((1, 1, 8, sub, width), index)],
            out_specs=pl.BlockSpec((1, rows, width), out_index),
            name="assemble",
        )(tot)

    one = call(
        (layers, nm, nf),
        lambda l, m, f: ((layers - 1 - l) * 2 * nu + nu + (f % (nf // 2)) * nm + m, f // (nf // 2), 0, 0, 0),
        (layers, width, wide),
        lambda l, m, f: (l, m, f),
    )
    two = call(
        (layers, 2 * nu),
        lambda l, j: ((layers - 1 - l) * 2 * nu + j % nu, j // nu, 0, 0, 0),
        (layers, wide, width),
        lambda l, j: (l, j, 0),
    )
    return one, two


def solution(mesh, rows=UNIT_ROWS):
    batch_spec = P(AXES)

    def per_device(w_one, w_two, x_loc, dy_loc):
        layers, width, wide = w_one.shape
        x = x_loc.reshape(-1, width)
        dy = dy_loc.reshape(-1, width)
        u, a, h = forward(x, w_one, w_two)
        tot, dx = backward(w_one, w_two, u, a, h, dy, rows)[:2]
        one, two = assemble(tot, layers, width, wide, rows)
        return one, two, dx.reshape(x_loc.shape)

    return jax.shard_map(per_device, mesh=mesh, in_specs=(P(), P(), batch_spec, batch_spec), out_specs=(P(), P(), batch_spec), check_vma=False)
```

```python
import functools

import jax
import jax.numpy as jnp
from jax import lax
from jax.experimental import pallas as pl
from jax.experimental.pallas import tpu as pltpu
from jax.sharding import PartitionSpec as P

AXES = ("replica", "data")
MESH = pl.DeviceIdType.MESH
BF16, F32 = jnp.bfloat16, jnp.float32
VMEM_LIMIT = 67_043_328
C0, C1 = 0.7978845608028654, 0.044715
UNIT_ROWS = 256
LAG = 3
SLOTS, RECV = 12, 8
X, Y, Z = 0, 1, 2


def gelu(v):
    return 0.5 * v * (1.0 + jnp.tanh(C0 * (v + C1 * (v * v * v))))


def gelu_slope(v):
    sq = v * v
    t = jnp.tanh(C0 * (v + C1 * (sq * v)))
    return 0.5 * (1.0 + t) + 0.5 * v * (1.0 - t * t) * (C0 * (1.0 + 3.0 * C1 * sq))


def mm(lhs, rhs, lhs_dim, rhs_dim):
    return lax.dot_general(lhs, rhs, (((lhs_dim,), (rhs_dim,)), ((), ())), preferred_element_type=F32)


def forward_body(z_ref, x_ref, w1_ref, w2_ref, u_ref, a_ref, h_ref, hid, acc, act_s, *, layers, chunks, rows):
    layer, j = pl.program_id(0), pl.program_id(1)
    part = rows // 2
    shift = z_ref[0] * part

    def pick(ref, k):
        return ref[:, pl.ds(pl.multiple_of(k * rows + shift, part), part)]

    @pl.when(jnp.logical_and(layer == 0, j == 0))
    def _():
        hid[...] = x_ref[...]

    @pl.when(j == 0)
    def _():
        for k in range(hid.shape[1] // rows):
            h_ref[0, :, k * part : (k + 1) * part] = pick(hid, k)
        acc[...] = hid[...].astype(F32)

    pre = mm(hid[...], w1_ref[0], 1, 0).astype(BF16)
    u_ref[0] = pre
    act = gelu(pre.astype(F32)).astype(BF16)
    act_s[...] = act

    @pl.when(layer < layers - 1)
    def _():
        acc[...] += mm(act, w2_ref[0], 1, 0)

        @pl.when(j == chunks - 1)
        def _():
            hid[...] = acc[...].astype(BF16)

    for k in range(act_s.shape[1] // rows):
        a_ref[0, :, k * part : (k + 1) * part] = pick(act_s, k)


def forward(z, x, w_one, w_two, rows):
    layers, width, wide = w_one.shape
    tokens = x.shape[0]
    chunk = width
    chunks = wide // chunk
    shape = jax.ShapeDtypeStruct
    return pl.pallas_call(
        functools.partial(forward_body, layers=layers, chunks=chunks, rows=rows),
        grid=(layers, chunks),
        out_shape=[shape((layers, tokens, wide), BF16), shape((layers, tokens, wide // 2), BF16), shape((layers, tokens, width // 2), BF16)],
        in_specs=[
            pl.BlockSpec(memory_space=pltpu.SMEM),
            pl.BlockSpec((tokens, width), lambda l, j: (0, 0)),
            pl.BlockSpec((1, width, chunk), lambda l, j: (l, 0, j)),
            pl.BlockSpec((1, chunk, width), lambda l, j: (l, j, 0)),
        ],
        out_specs=[
            pl.BlockSpec((1, tokens, chunk), lambda l, j: (l, 0, j)),
            pl.BlockSpec((1, tokens, chunk // 2), lambda l, j: (l, 0, j)),
            pl.BlockSpec((1, tokens, width // 2), lambda l, j: (l, 0, 0)),
        ],
        scratch_shapes=[pltpu.VMEM((tokens, width), BF16), pltpu.VMEM((tokens, width), F32), pltpu.VMEM((tokens, chunk), BF16)],
        compiler_params=pltpu.CompilerParams(vmem_limit_bytes=VMEM_LIMIT),
        cost_estimate=pl.CostEstimate(
            flops=(4 * layers - 2) * tokens * width * wide, bytes_accessed=4 * layers * width * wide, transcendentals=layers * tokens * wide
        ),
        name="forward",
    )(z, x, w_one, w_two)


def backward_body(
    w1, w2, u_own, u_nbr, a_own, a_nbr, h_own, h_nbr, dy_own, dy_nbr,
    tot, dx, a_sib, h_sib, du_sib, gb_sib,
    a_cat, du_cat, h_cat, gb_cat, g, w2c, w1c, uc, du_st, unit, rcv1, rcv2,
    s_rs1, s_rs2, s_ag1, s_ag2, s_ag3, s_fwd, s_own,
    r_rs1, r_rs2, r_ag1, r_ag2, r_ag3, r_fwd,
    c_rs1, c_rs2,
    s_a, r_a, l_a, l_a2, s_du, r_du, l_du, s_gb, r_gb, l_gb, l_gb2, s_h, r_h, l_h, l_h2, l_w2, l_w1, l_u, l_dx,
    *, layers, tokens, width, wide, rows,
):
    half = wide // 2
    part = rows // 2
    nu = half // rows
    nm = width // rows
    hn = nu // 2
    chunk = wide // nu
    units = 2 * nu * layers
    step = tokens // 2
    z, rest = lax.axis_index("replica"), lax.axis_index("data")
    core, x, y = rest % 2, (rest // 2) % 2, rest // 4

    def choose(axis):
        return (1 - axis) * (2 - axis) // 2, axis * (2 - axis), axis * (axis - 1) // 2

    def peer(axis):
        ex, ey, ez = choose(axis)
        px, py, pz = x + ex * (1 - 2 * x), y + ey * (1 - 2 * y), z + ez * (1 - 2 * z)
        return (pz, (py * 2 + px) * 2 + core)

    sibling = (z, (y * 2 + x) * 2 + 1 - core)

    def send(src, dst, ssem, rsem, to):
        return pltpu.make_async_remote_copy(src_ref=src, dst_ref=dst, send_sem=ssem, recv_sem=rsem, device_id=to, device_id_type=MESH)

    def place(n):
        mid = (n % 3) // 2
        a_axis = (1 - mid) * (n % 3) + mid * ((n // 3) % 2)
        b_axis = 1 - a_axis
        bit_a = x + a_axis * (y - x)
        bit_b = x + b_axis * (y - x)
        own = (1 - mid) * (4 * z + 2 * bit_a + bit_b) + mid * (4 * bit_a + 2 * z + bit_b)
        return mid, a_axis, b_axis, bit_a, bit_b, own

    def rs1(n):
        mid, a_axis, b_axis, bit_a, bit_b, own = place(n)
        return send(unit.at[n % SLOTS, pl.ds(2 - 2 * bit_a, 2)], rcv1.at[n % RECV], s_rs1.at[n % SLOTS], r_rs1.at[n % RECV], peer(a_axis))

    def rs2(n):
        mid, a_axis, b_axis, bit_a, bit_b, own = place(n)
        return send(unit.at[n % SLOTS, pl.ds(2 * bit_a + 1 - bit_b, 1)], rcv2.at[n % RECV], s_rs2.at[n % SLOTS], r_rs2.at[n % RECV], peer(b_axis))

    def own_copy(n):
        mid, a_axis, b_axis, bit_a, bit_b, own = place(n)
        return pltpu.make_async_copy(unit.at[n % SLOTS, pl.ds(2 * bit_a + bit_b, 1)], tot.at[n, core, pl.ds(own, 1)], s_own.at[n % SLOTS])

    def ag1(n):
        mid, a_axis, b_axis, bit_a, bit_b, own = place(n)
        return send(
            unit.at[n % SLOTS, pl.ds(2 * bit_a + bit_b, 1)], tot.at[n, core, pl.ds(own, 1)], s_ag1.at[n % SLOTS], r_ag1.at[n % SLOTS], peer(b_axis)
        )

    def ag2(n):
        mid, a_axis, b_axis, bit_a, bit_b, own = place(n)
        piece = tot.at[n, core, pl.ds(own // 2 * 2, 2)]
        return send(piece, piece, s_ag2.at[n % SLOTS], r_ag2.at[n % SLOTS], peer(a_axis + mid * (Z - a_axis)))

    def ag3(n):
        mid, a_axis, b_axis, bit_a, bit_b, own = place(n)
        piece = tot.at[n, core, pl.ds(own // 4 * 4, 4)]
        return send(piece, piece, s_ag3.at[n % SLOTS], r_ag3.at[n % SLOTS], peer(Z + mid * (a_axis - Z)))

    def fwd(n):
        piece = tot.at[n, core]
        return send(piece, piece, s_fwd.at[n % SLOTS], r_fwd.at[n % SLOTS], sibling)

    def add(n, block, rcv, j):
        slot = n % SLOTS
        unit[slot, block] = (unit[slot, block].astype(F32) + rcv[n % RECV, j].astype(F32)).astype(BF16)

    def credit(sem, n, axis):
        @pl.when(n + RECV < units)
        def _():
            pl.semaphore_signal(sem.at[n % RECV], inc=1, device_id=peer(axis), device_id_type=MESH)

    def spend(sem, n):
        @pl.when(n >= RECV)
        def _():
            pl.semaphore_wait(sem.at[n % RECV], 1)

    def live(n):
        return jnp.logical_and(n >= 0, n < units)

    def comm(t):
        n1, n2, n3, n4, n5, n6 = (t - k * LAG for k in range(1, 7))

        @pl.when(live(n2))
        def _():
            mid, a_axis, b_axis, bit_a, bit_b, own = place(n2)
            rs2(n2).wait_recv()
            add(n2, 2 * bit_a + bit_b, rcv2, 0)
            credit(c_rs2, n2, b_axis)
            rs1(n2).wait_send()

        @pl.when(live(n1))
        def _():
            mid, a_axis, b_axis, bit_a, bit_b, own = place(n1)
            rs1(n1).wait_recv()
            add(n1, 2 * bit_a + 1 - bit_b, rcv1, 1 - bit_b)
            add(n1, 2 * bit_a + bit_b, rcv1, bit_b)
            credit(c_rs1, n1, a_axis)

        @pl.when(live(n2))
        def _():
            own_copy(n2).start()
            ag1(n2).start()

        @pl.when(live(n1))
        def _():
            spend(c_rs2, n1)
            rs2(n1).start()

        @pl.when(live(n3))
        def _():
            rs2(n3).wait_send()
            own_copy(n3).wait()
            ag1(n3).wait()
            ag2(n3).start()

        @pl.when(live(n4))
        def _():
            ag2(n4).wait()
            ag3(n4).start()

        @pl.when(live(n5))
        def _():
            ag3(n5).wait()
            fwd(n5).start()

        @pl.when(live(n6))
        def _():
            fwd(n6).wait()

    def push_unit(t):
        spend(c_rs1, t)
        rs1(t).start()

    sets = (0, 1)
    us, as_, hs, dys = (u_own, u_nbr), (a_own, a_nbr), (h_own, h_nbr), (dy_own, dy_nbr)

    def mine(k):
        return pl.ds(k * tokens, tokens)

    def theirs(k):
        return pl.ds((2 + k) * tokens, tokens)

    def chunk_at(i):
        late = i // hn
        return pl.multiple_of(((1 - core) + late * (2 * core - 1)) * half + (i % hn) * chunk, 128)

    def loads(layer, i):
        f0, slot = chunk_at(i), i % 2
        return (
            pltpu.make_async_copy(w2.at[layer, pl.ds(f0, chunk)], w2c.at[slot], l_w2.at[slot]),
            pltpu.make_async_copy(w1.at[layer, :, pl.ds(f0, chunk)], w1c.at[slot], l_w1.at[slot]),
            *(pltpu.make_async_copy(us[k].at[layer, :, pl.ds(f0, chunk)], uc.at[slot, k], l_u.at[slot, k]) for k in sets),
        )

    def cols(i, size):
        return pl.ds(pl.multiple_of(i * size, 128), size)

    def a_load(layer, k):
        return pltpu.make_async_copy(as_[k].at[layer, :, cols(core, half // 2)], a_cat.at[mine(k)], l_a.at[k])

    def a_load2(layer, k):
        return pltpu.make_async_copy(a_sib.at[layer, k], a_cat.at[theirs(k)], l_a2.at[k])

    def a_first(k):
        return send(as_[k].at[layers - 1, :, cols(1 - core, half // 2)], a_cat.at[theirs(k)], s_a.at[k], l_a2.at[k], sibling)

    def a_push(layer, k):
        return send(as_[k].at[layer, :, cols(1 - core, half // 2)], a_sib.at[layer, k], s_a.at[k], r_a.at[k], sibling)

    def du_push(layer, i, k):
        return send(du_st.at[k], du_sib.at[layer, k, :, cols(i % hn, chunk)], s_du.at[k], r_du.at[i % hn, k], sibling)

    def du_load(layer, i, k):
        return pltpu.make_async_copy(du_sib.at[layer, k, :, cols(i % hn, chunk)], du_cat.at[theirs(k), cols(i % hn, chunk)], l_du.at[i % hn, k])

    def h_push(layer, k):
        return send(hs[k].at[layer], h_sib.at[layer, k], s_h.at[k], r_h.at[k], sibling)

    def h_load(layer, k):
        return pltpu.make_async_copy(hs[k].at[layer], h_cat.at[mine(k)], l_h.at[k])

    def h_load2(layer, k):
        return pltpu.make_async_copy(h_sib.at[layer, k], h_cat.at[theirs(k)], l_h2.at[k])

    def gb_push(layer, k):
        return send(gb_cat.at[mine(k)], gb_sib.at[layer, k], s_gb.at[k], r_gb.at[k], sibling)

    def gb_load2(layer, k):
        return pltpu.make_async_copy(gb_sib.at[layer, k], gb_cat.at[theirs(k)], l_gb2.at[k])

    def gb_first(k):
        return pltpu.make_async_copy(dys[k], gb_cat.at[mine(k)], l_gb.at[k])

    def dy_push(k):
        return send(dys[k], gb_cat.at[theirs(k)], s_gb.at[k], l_gb2.at[k], sibling)

    def dx_store():
        return pltpu.make_async_copy(gb_cat.at[mine(0)], dx, l_dx)

    barrier = pltpu.get_barrier_semaphore()
    for to in (peer(X), peer(Y), peer(Z), sibling):
        pl.semaphore_signal(barrier, inc=1, device_id=to, device_id_type=MESH)
    top = layers - 1
    for k in sets:
        gb_first(k).start()
        a_load(top, k).start()
    for load in loads(top, 0):
        load.start()
    pl.semaphore_wait(barrier, 4)
    for k in sets:
        dy_push(k).start()
        a_first(k).start()
    for k in sets:
        gb_first(k).wait()
        g[mine(k)] = gb_cat[mine(k)].astype(F32)
    for k in sets:
        dy_push(k).wait_send()
        a_first(k).wait_send()

    def layer_step(li, carry):
        layer = layers - 1 - li
        base = li * 2 * nu
        for k in sets:
            gb_load2(layer, k).wait()
            a_load(layer, k).wait()
            a_load2(layer, k).wait()

        def first(i, carry):
            t = base + i
            out = mm(a_cat[:, cols(i, part)], gb_cat[...], 0, 0)
            unit[t % SLOTS] = out.reshape(4, rows // 8, width).astype(BF16)

            @pl.when(i < nu - 1)
            def _():
                for load in loads(layer, i + 1):
                    load.start()

            comm(t)
            push_unit(t)

            @pl.when(i == 0)
            def _():
                for k in sets:
                    h_push(layer, k).start()
                    h_load(layer, k).start()

            @pl.when(i == hn)
            def _():
                for k in sets:
                    h_push(layer, k).wait()
                    h_load2(layer, k).start()

            @pl.when(jnp.logical_and(layer > 0, i == 2))
            def _():
                for k in sets:
                    a_push(layer - 1, k).start()

            for load in loads(layer, i):
                load.wait()

            def token_set(k, carry):
                @pl.when(jnp.logical_and(i >= 1, i <= hn))
                def _():
                    du_push(layer, i - 1, k).wait_send()

                def block(b, carry):
                    at = pl.ds(pl.multiple_of(b * step, 16), step)
                    rows_b = pl.ds(pl.multiple_of(k * tokens + b * step, 16), step)
                    d_act = mm(gb_cat[rows_b], w2c[i % 2], 1, 1)
                    du = (d_act * gelu_slope(uc[i % 2, k, at].astype(F32))).astype(BF16)

                    @pl.when(i < hn)
                    def _():
                        du_st[k, at] = du

                    @pl.when(i >= hn)
                    def _():
                        du_cat[rows_b, cols(i % hn, chunk)] = du

                    @pl.when(jnp.logical_or(layer > 0, k == 0))
                    def _():
                        g[rows_b] += mm(du, w1c[i % 2], 1, 1)

                    return carry

                lax.fori_loop(0, tokens // step, block, 0)

                @pl.when(i < hn)
                def _():
                    du_push(layer, i, k).start()

                @pl.when(i >= hn)
                def _():
                    du_push(layer, i - hn, k).wait_recv()
                    du_load(layer, i - hn, k).start()

                return carry

            lax.fori_loop(0, 2, token_set, 0)
            return carry

        lax.fori_loop(0, nu, first, 0)
        for k in sets:
            gb_cat[mine(k)] = g[mine(k)].astype(BF16)
        for k in sets:
            h_load(layer, k).wait()
            h_load2(layer, k).wait()
            for i in range(hn):
                du_load(layer, i, k).wait()

        def second(i, carry):
            t = base + nu + i
            mi, fi = i % nm, i // nm
            out = mm(h_cat[:, cols(mi, part)], du_cat[:, cols(fi, width)], 0, 0)
            unit[t % SLOTS] = out.reshape(4, rows // 8, width).astype(BF16)
            comm(t)
            push_unit(t)

            @pl.when(layer > 0)
            def _():
                @pl.when(i == 0)
                def _():
                    for load in loads(layer - 1, 0):
                        load.start()
                    for k in sets:
                        a_push(layer - 1, k).wait()
                        a_load(layer - 1, k).start()
                        a_load2(layer - 1, k).start()
                    for k in sets:
                        gb_push(layer - 1, k).start()

                @pl.when(i == hn)
                def _():
                    for k in sets:
                        gb_push(layer - 1, k).wait()
                        gb_load2(layer - 1, k).start()

            @pl.when(jnp.logical_and(layer == 0, i == 0))
            def _():
                dx_store().start()

            return carry

        lax.fori_loop(0, nu, second, 0)
        return carry

    lax.fori_loop(0, layers, layer_step, 0)

    def drain(t, carry):
        comm(t)
        return carry

    lax.fori_loop(units, units + 6 * LAG, drain, 0)
    dx_store().wait()


def backward(w_one, w_two, us, as_, hs, dys, rows):
    layers, width, wide = w_one.shape
    tokens = dys[0].shape[0]
    half = wide // 2
    nu = half // rows
    hn = nu // 2
    chunk = wide // nu
    units = 2 * nu * layers
    dma, reg = pltpu.SemaphoreType.DMA, pltpu.SemaphoreType.REGULAR
    hbm = pl.BlockSpec(memory_space=pl.ANY)
    sub = rows // 8
    shape = jax.ShapeDtypeStruct
    outs = [
        shape((units, 2, 8, sub, width), BF16),
        shape((tokens, width), BF16),
        shape((layers, 2, tokens, half // 2), BF16),
        shape((layers, 2, tokens, width // 2), BF16),
        shape((layers, 2, tokens, half), BF16),
        shape((layers, 2, tokens, width), BF16),
    ]
    scratch = [
        pltpu.VMEM((4 * tokens, half // 2), BF16),
        pltpu.VMEM((4 * tokens, half), BF16),
        pltpu.VMEM((4 * tokens, width // 2), BF16),
        pltpu.VMEM((4 * tokens, width), BF16),
        pltpu.VMEM((2 * tokens, width), F32),
        pltpu.VMEM((2, chunk, width), BF16),
        pltpu.VMEM((2, width, chunk), BF16),
        pltpu.VMEM((2, 2, tokens, chunk), BF16),
        pltpu.VMEM((2, tokens, chunk), BF16),
        pltpu.VMEM((SLOTS, 4, sub, width), BF16),
        pltpu.VMEM((RECV, 2, sub, width), BF16),
        pltpu.VMEM((RECV, 1, sub, width), BF16),
        *[dma((SLOTS,))] * 7,
        *[dma((RECV,))] * 2,
        *[dma((SLOTS,))] * 4,
        *[reg((RECV,))] * 2,
        *[dma((2,))] * 4,
        dma((2,)), dma((hn, 2)), dma((hn, 2)),
        *[dma((2,))] * 8,
        dma((2,)), dma((2,)), dma((2, 2)), dma,
    ]
    return pl.pallas_call(
        functools.partial(backward_body, layers=layers, tokens=tokens, width=width, wide=wide, rows=rows),
        out_shape=outs,
        in_specs=[hbm] * 10,
        out_specs=[hbm] * 6,
        scratch_shapes=scratch,
        compiler_params=pltpu.CompilerParams(collective_id=0, has_side_effects=True, vmem_limit_bytes=VMEM_LIMIT),
        name="backward",
    )(w_one, w_two, *us, *as_, *hs, *dys)


COPY_SLOTS, COPY_LEAD = 24, 10


def assemble_body(tot, one, two, buf, s_in, s_out, *, layers, nu, nm, width):
    items = 4 * nu * layers

    def load(j):
        return pltpu.make_async_copy(tot.at[j // 2, j % 2], buf.at[j % COPY_SLOTS], s_in.at[j % COPY_SLOTS])

    def stores(j, run):
        n, core = j // 2, j % 2
        layer, i, slot = layers - 1 - n // (2 * nu), n % nu, j % COPY_SLOTS
        mid = (n % 3) // 2
        for q in range(4):
            src = (1 - mid) * q + mid * (q % 2 * 2 + q // 2)
            piece = buf.at[slot, pl.ds(src * 2, 2)]

            @pl.when((n // nu) % 2 == 0)
            def _():
                run(pltpu.make_async_copy(piece, two.at[layer, core * nu + i, pl.ds(2 * q, 2)], s_out.at[slot, q]))

            @pl.when((n // nu) % 2 == 1)
            def _():
                cols = pl.ds(pl.multiple_of((core * (nu // nm) + i // nm) * width, 128), width)
                run(pltpu.make_async_copy(piece, one.at[layer, i % nm, pl.ds(2 * q, 2), :, cols], s_out.at[slot, q]))

    def step(j, carry):
        @pl.when(j >= COPY_SLOTS)
        def _():
            stores(j - COPY_SLOTS, lambda c: c.wait())

        @pl.when(j < items)
        def _():
            load(j).start()

        @pl.when(jnp.logical_and(j >= COPY_LEAD, j < items + COPY_LEAD))
        def _():
            load(j - COPY_LEAD).wait()
            stores(j - COPY_LEAD, lambda c: c.start())

        return carry

    lax.fori_loop(0, items + COPY_SLOTS, step, 0)


def assemble(tot, layers, width, wide, rows):
    nu, nm, sub = wide // 2 // rows, width // rows, rows // 8
    shape = jax.ShapeDtypeStruct
    hbm = pl.BlockSpec(memory_space=pl.ANY)
    one, two = pl.pallas_call(
        functools.partial(assemble_body, layers=layers, nu=nu, nm=nm, width=width),
        out_shape=[shape((layers, nm, 8, sub, wide), BF16), shape((layers, 2 * nu, 8, sub, width), BF16)],
        in_specs=[hbm],
        out_specs=[hbm, hbm],
        scratch_shapes=[pltpu.VMEM((COPY_SLOTS, 8, sub, width), BF16), pltpu.SemaphoreType.DMA((COPY_SLOTS,)), pltpu.SemaphoreType.DMA((COPY_SLOTS, 4))],
        compiler_params=pltpu.CompilerParams(vmem_limit_bytes=VMEM_LIMIT),
        name="assemble",
    )(tot)
    return one.reshape(layers, width, wide), two.reshape(layers, wide, width)


def solution(mesh, rows=UNIT_ROWS):
    batch_spec = P(AXES)

    def per_device(w_one, w_two, x_loc, dy_loc):
        layers, width, wide = w_one.shape
        x = x_loc.reshape(-1, width)
        dy = dy_loc.reshape(-1, width)
        swap = [(0, 1), (1, 0)]
        x_nbr = lax.ppermute(x, "replica", swap)
        dy_nbr = lax.ppermute(dy, "replica", swap)
        z = jnp.full((1,), lax.axis_index("replica"), jnp.int32)
        kept = [forward(z, tokens, w_one, w_two, rows) for tokens in (x, x_nbr)]
        us, as_, hs = zip(*kept)
        tot, dx = backward(w_one, w_two, us, as_, hs, (dy, dy_nbr), rows)[:2]
        one, two = assemble(tot, layers, width, wide, rows)
        return one, two, dx.reshape(x_loc.shape)

    return jax.shard_map(per_device, mesh=mesh, in_specs=(P(), P(), batch_spec, batch_spec), out_specs=(P(), P(), batch_spec), check_vma=False)
```

```python
import functools

import jax
import jax.numpy as jnp
from jax import lax
from jax.experimental import pallas as pl
from jax.experimental.pallas import tpu as pltpu
from jax.sharding import PartitionSpec as P

AXES = ("replica", "data")
MESH = pl.DeviceIdType.MESH
BF16, F32 = jnp.bfloat16, jnp.float32
VMEM_LIMIT = 67_043_328
C0, C1 = 0.7978845608028654, 0.044715
UNIT_ROWS = 256
LAG = 3
SLOTS, RECV, PARTS, RECV0 = 12, 8, 2, 4
X, Y, Z = 0, 1, 2


def gelu(v):
    return 0.5 * v * (1.0 + jnp.tanh(C0 * (v + C1 * (v * v * v))))


def gelu_slope(v):
    sq = v * v
    t = jnp.tanh(C0 * (v + C1 * (sq * v)))
    return 0.5 * (1.0 + t) + 0.5 * v * (1.0 - t * t) * (C0 * (1.0 + 3.0 * C1 * sq))


def mm(lhs, rhs, lhs_dim, rhs_dim):
    return lax.dot_general(lhs, rhs, (((lhs_dim,), (rhs_dim,)), ((), ())), preferred_element_type=F32)


def forward_body(z_ref, x_ref, w1_ref, w2_ref, u_ref, a_ref, h_ref, hid, acc, act_s, *, layers, chunks, rows):
    layer, j = pl.program_id(0), pl.program_id(1)
    part = rows // 2
    shift = z_ref[0] * part

    def pick(ref, k):
        return ref[:, pl.ds(pl.multiple_of(k * rows + shift, part), part)]

    @pl.when(jnp.logical_and(layer == 0, j == 0))
    def _():
        hid[...] = x_ref[...]

    @pl.when(j == 0)
    def _():
        for k in range(hid.shape[1] // rows):
            h_ref[0, :, k * part : (k + 1) * part] = pick(hid, k)
        acc[...] = hid[...].astype(F32)

    pre = mm(hid[...], w1_ref[0], 1, 0).astype(BF16)
    u_ref[0] = pre
    act = gelu(pre.astype(F32)).astype(BF16)
    act_s[...] = act

    @pl.when(layer < layers - 1)
    def _():
        acc[...] += mm(act, w2_ref[0], 1, 0)

        @pl.when(j == chunks - 1)
        def _():
            hid[...] = acc[...].astype(BF16)

    for k in range(act_s.shape[1] // rows):
        a_ref[0, :, k * part : (k + 1) * part] = pick(act_s, k)


def forward(z, x, w_one, w_two, rows):
    layers, width, wide = w_one.shape
    tokens = x.shape[0]
    chunk = width
    chunks = wide // chunk
    shape = jax.ShapeDtypeStruct
    return pl.pallas_call(
        functools.partial(forward_body, layers=layers, chunks=chunks, rows=rows),
        grid=(layers, chunks),
        out_shape=[shape((layers, tokens, wide), BF16), shape((layers, tokens, wide // 2), BF16), shape((layers, tokens, width // 2), BF16)],
        in_specs=[
            pl.BlockSpec(memory_space=pltpu.SMEM),
            pl.BlockSpec((tokens, width), lambda l, j: (0, 0)),
            pl.BlockSpec((1, width, chunk), lambda l, j: (l, 0, j)),
            pl.BlockSpec((1, chunk, width), lambda l, j: (l, j, 0)),
        ],
        out_specs=[
            pl.BlockSpec((1, tokens, chunk), lambda l, j: (l, 0, j)),
            pl.BlockSpec((1, tokens, chunk // 2), lambda l, j: (l, 0, j)),
            pl.BlockSpec((1, tokens, width // 2), lambda l, j: (l, 0, 0)),
        ],
        scratch_shapes=[pltpu.VMEM((tokens, width), BF16), pltpu.VMEM((tokens, width), F32), pltpu.VMEM((tokens, chunk), BF16)],
        compiler_params=pltpu.CompilerParams(vmem_limit_bytes=VMEM_LIMIT),
        cost_estimate=pl.CostEstimate(
            flops=(4 * layers - 2) * tokens * width * wide, bytes_accessed=4 * layers * width * wide, transcendentals=layers * tokens * wide
        ),
        name="forward",
    )(z, x, w_one, w_two)


def backward_body(
    w1, w2, u_own, u_nbr, a_own, a_nbr, h_own, h_nbr, dy_own, dy_nbr,
    tot, dx,
    a_cat, du_cat, h_cat, gb_cat, g, w2c, w1c, uc, unit, part0, rcv0, rcv1, rcv2,
    s_rs1, s_rs2, s_ag1, s_ag2, s_ag3, s_fwd, s_own, r_ag1, r_ag2, r_ag3, r_fwd,
    r_rs1, r_rs2, c_rs1, c_rs2, s_rs0, r_rs0, c_rs0,
    l_a, l_gb, l_h, l_w2, l_w1, l_u, l_dx,
    *, layers, tokens, width, wide, rows,
):
    half = wide // 2
    part = rows // 2
    nu = half // rows
    nm = width // rows
    nf = nu // nm
    chunk = wide // nu
    units = 2 * nu * layers
    step = tokens // 2
    z, rest = lax.axis_index("replica"), lax.axis_index("data")
    core, x, y = rest % 2, (rest // 2) % 2, rest // 4

    def choose(axis):
        return (1 - axis) * (2 - axis) // 2, axis * (2 - axis), axis * (axis - 1) // 2

    def peer(axis):
        ex, ey, ez = choose(axis)
        px, py, pz = x + ex * (1 - 2 * x), y + ey * (1 - 2 * y), z + ez * (1 - 2 * z)
        return (pz, (py * 2 + px) * 2 + core)

    sibling = (z, (y * 2 + x) * 2 + 1 - core)

    def send(src, dst, ssem, rsem, to):
        return pltpu.make_async_remote_copy(src_ref=src, dst_ref=dst, send_sem=ssem, recv_sem=rsem, device_id=to, device_id_type=MESH)

    def place(n):
        mid = (n % 3) // 2
        a_axis = (1 - mid) * (n % 3) + mid * ((n // 3) % 2)
        b_axis = 1 - a_axis
        bit_a = x + a_axis * (y - x)
        bit_b = x + b_axis * (y - x)
        own = (1 - mid) * (4 * z + 2 * bit_a + bit_b) + mid * (4 * bit_a + 2 * z + bit_b)
        return mid, a_axis, b_axis, bit_a, bit_b, own

    def rs0(n):
        return send(part0.at[n % PARTS], rcv0.at[n % RECV0], s_rs0.at[n % PARTS], r_rs0.at[n % RECV0], sibling)

    def rs1(n):
        mid, a_axis, b_axis, bit_a, bit_b, own = place(n)
        return send(unit.at[n % SLOTS, pl.ds(2 - 2 * bit_a, 2)], rcv1.at[n % RECV], s_rs1.at[n % SLOTS], r_rs1.at[n % RECV], peer(a_axis))

    def rs2(n):
        mid, a_axis, b_axis, bit_a, bit_b, own = place(n)
        return send(unit.at[n % SLOTS, pl.ds(2 * bit_a + 1 - bit_b, 1)], rcv2.at[n % RECV], s_rs2.at[n % SLOTS], r_rs2.at[n % RECV], peer(b_axis))

    def own_copy(n):
        mid, a_axis, b_axis, bit_a, bit_b, own = place(n)
        return pltpu.make_async_copy(unit.at[n % SLOTS, pl.ds(2 * bit_a + bit_b, 1)], tot.at[n, core, pl.ds(own, 1)], s_own.at[n % SLOTS])

    def ag1(n):
        mid, a_axis, b_axis, bit_a, bit_b, own = place(n)
        return send(
            unit.at[n % SLOTS, pl.ds(2 * bit_a + bit_b, 1)], tot.at[n, core, pl.ds(own, 1)], s_ag1.at[n % SLOTS], r_ag1.at[n % SLOTS], peer(b_axis)
        )

    def ag2(n):
        mid, a_axis, b_axis, bit_a, bit_b, own = place(n)
        piece = tot.at[n, core, pl.ds(own // 2 * 2, 2)]
        return send(piece, piece, s_ag2.at[n % SLOTS], r_ag2.at[n % SLOTS], peer(a_axis + mid * (Z - a_axis)))

    def ag3(n):
        mid, a_axis, b_axis, bit_a, bit_b, own = place(n)
        piece = tot.at[n, core, pl.ds(own // 4 * 4, 4)]
        return send(piece, piece, s_ag3.at[n % SLOTS], r_ag3.at[n % SLOTS], peer(Z + mid * (a_axis - Z)))

    def fwd(n):
        piece = tot.at[n, core]
        return send(piece, piece, s_fwd.at[n % SLOTS], r_fwd.at[n % SLOTS], sibling)

    def add(n, block, rcv, slot, j):
        unit[n % SLOTS, block] = (unit[n % SLOTS, block].astype(F32) + rcv[slot, j].astype(F32)).astype(BF16)

    def credit(sem, n, slots, to):
        @pl.when(n + slots < units)
        def _():
            pl.semaphore_signal(sem.at[n % slots], inc=1, device_id=to, device_id_type=MESH)

    def spend(sem, n, slots):
        @pl.when(n >= slots)
        def _():
            pl.semaphore_wait(sem.at[n % slots], 1)

    def live(n):
        return jnp.logical_and(n >= 0, n < units)

    def comm(t):
        n0, n1, n2, n3, n4, n5 = (t - 1 - k * LAG for k in range(6))
        n6 = n5 - 2

        @pl.when(live(n2))
        def _():
            mid, a_axis, b_axis, bit_a, bit_b, own = place(n2)
            rs2(n2).wait_recv()
            add(n2, 2 * bit_a + bit_b, rcv2, n2 % RECV, 0)
            credit(c_rs2, n2, RECV, peer(b_axis))
            rs1(n2).wait_send()

        @pl.when(live(n1))
        def _():
            mid, a_axis, b_axis, bit_a, bit_b, own = place(n1)
            rs1(n1).wait_recv()
            add(n1, 2 * bit_a + 1 - bit_b, rcv1, n1 % RECV, 1 - bit_b)
            add(n1, 2 * bit_a + bit_b, rcv1, n1 % RECV, bit_b)
            credit(c_rs1, n1, RECV, peer(a_axis))

        @pl.when(live(n0))
        def _():
            mid, a_axis, b_axis, bit_a, bit_b, own = place(n0)
            rs0(n0).wait()
            for first in (2 - 2 * bit_a, 2 * bit_a):
                for j in range(2):
                    add(n0, first + j, rcv0, n0 % RECV0, first + j)
            credit(c_rs0, n0, RECV0, sibling)

        @pl.when(live(n2))
        def _():
            own_copy(n2).start()
            ag1(n2).start()

        @pl.when(live(n1))
        def _():
            spend(c_rs2, n1, RECV)
            rs2(n1).start()

        @pl.when(live(n0))
        def _():
            spend(c_rs1, n0, RECV)
            rs1(n0).start()

        @pl.when(live(n3))
        def _():
            rs2(n3).wait_send()
            own_copy(n3).wait()
            ag1(n3).wait()
            ag2(n3).start()

        @pl.when(live(n4))
        def _():
            ag2(n4).wait()
            ag3(n4).start()

        @pl.when(live(n5))
        def _():
            ag3(n5).wait()
            fwd(n5).start()

        @pl.when(live(n6))
        def _():
            fwd(n6).wait()

    def push_unit(t):
        spend(c_rs0, t, RECV0)
        rs0(t).start()

    sets = (0, 1)
    us, as_, hs, dys = (u_own, u_nbr), (a_own, a_nbr), (h_own, h_nbr), (dy_own, dy_nbr)

    def of(k):
        return pl.ds(k * tokens, tokens)

    def loads(layer, i):
        f0, slot = pl.multiple_of(i * chunk, 128), i % 2
        return (
            pltpu.make_async_copy(w2.at[layer, pl.ds(f0, chunk)], w2c.at[slot], l_w2.at[slot]),
            pltpu.make_async_copy(w1.at[layer, :, pl.ds(f0, chunk)], w1c.at[slot], l_w1.at[slot]),
            *(pltpu.make_async_copy(us[k].at[layer, :, pl.ds(f0, chunk)], uc.at[slot, k], l_u.at[slot, k]) for k in sets),
        )

    def cols(i, size):
        return pl.ds(pl.multiple_of(i * size, 128), size)

    def a_load(layer, k):
        return pltpu.make_async_copy(as_[k].at[layer], a_cat.at[of(k)], l_a.at[k])

    def h_load(layer, k):
        return pltpu.make_async_copy(hs[k].at[layer], h_cat.at[of(k)], l_h.at[k])

    def gb_load(k):
        return pltpu.make_async_copy(dys[k], gb_cat.at[of(k)], l_gb.at[k])

    def dx_store():
        return pltpu.make_async_copy(gb_cat.at[of(0)], dx, l_dx)

    def blocks(out):
        return out.reshape(4, rows // 8, width).astype(BF16)

    barrier = pltpu.get_barrier_semaphore()
    for to in (peer(X), peer(Y), peer(Z), sibling):
        pl.semaphore_signal(barrier, inc=1, device_id=to, device_id_type=MESH)
    for k in sets:
        gb_load(k).start()
        a_load(layers - 1, k).start()
    for load in loads(layers - 1, 0):
        load.start()
    for k in sets:
        gb_load(k).wait()
        g[of(k)] = gb_cat[of(k)].astype(F32)
    pl.semaphore_wait(barrier, 4)

    def layer_step(li, carry):
        layer = layers - 1 - li
        base = li * 2 * nu
        for k in sets:
            a_load(layer, k).wait()
            h_load(layer, k).start()

        def first(i, carry):
            t = base + i
            lhs = jnp.concatenate([a_cat[:, cols((1 - core) * nu + i, part)], a_cat[:, cols(core * nu + i, part)]], axis=1)
            out = mm(lhs, gb_cat[...], 0, 0)
            part0[t % PARTS] = blocks(out[:part])
            unit[t % SLOTS] = blocks(out[part:])

            @pl.when(i < nu - 1)
            def _():
                for load in loads(layer, i + 1):
                    load.start()

            comm(t)
            push_unit(t)

            for load in loads(layer, i):
                load.wait()

            def token_block(b, carry):
                k = b // 2
                at = pl.ds(pl.multiple_of(b % 2 * step, 16), step)
                rows_b = pl.ds(pl.multiple_of(b * step, 16), step)
                d_act = mm(gb_cat[rows_b], w2c[i % 2], 1, 1)
                du = (d_act * gelu_slope(uc[i % 2, k, at].astype(F32))).astype(BF16)
                du_cat[rows_b, cols(i, chunk)] = du

                @pl.when(jnp.logical_or(layer > 0, k == 0))
                def _():
                    g[rows_b] += mm(du, w1c[i % 2], 1, 1)

                return carry

            lax.fori_loop(0, 4, token_block, 0)
            return carry

        lax.fori_loop(0, nu, first, 0)
        for k in sets:
            gb_cat[of(k)] = g[of(k)].astype(BF16)
        for k in sets:
            h_load(layer, k).wait()

        @pl.when(layer > 0)
        def _():
            for load in loads(layer - 1, 0):
                load.start()
            for k in sets:
                a_load(layer - 1, k).start()

        @pl.when(layer == 0)
        def _():
            dx_store().start()

        def second(i, carry):
            t = base + nu + i
            mi, fi = i % nm, i // nm
            lhs = h_cat[:, cols(mi, part)]
            part0[t % PARTS] = blocks(mm(lhs, du_cat[:, cols((1 - core) * nf + fi, width)], 0, 0))
            unit[t % SLOTS] = blocks(mm(lhs, du_cat[:, cols(core * nf + fi, width)], 0, 0))
            comm(t)
            push_unit(t)
            return carry

        lax.fori_loop(0, nu, second, 0)
        return carry

    lax.fori_loop(0, layers, layer_step, 0)

    def drain(t, carry):
        comm(t)
        return carry

    lax.fori_loop(units, units + 1 + 5 * LAG + 2, drain, 0)
    dx_store().wait()


def backward(w_one, w_two, us, as_, hs, dys, rows):
    layers, width, wide = w_one.shape
    tokens = dys[0].shape[0]
    half = wide // 2
    nu = half // rows
    chunk = wide // nu
    units = 2 * nu * layers
    dma, reg = pltpu.SemaphoreType.DMA, pltpu.SemaphoreType.REGULAR
    hbm = pl.BlockSpec(memory_space=pl.ANY)
    sub = rows // 8
    shape = jax.ShapeDtypeStruct
    scratch = [
        pltpu.VMEM((2 * tokens, half), BF16),
        pltpu.VMEM((2 * tokens, wide), BF16),
        pltpu.VMEM((2 * tokens, width // 2), BF16),
        pltpu.VMEM((2 * tokens, width), BF16),
        pltpu.VMEM((2 * tokens, width), F32),
        pltpu.VMEM((2, chunk, width), BF16),
        pltpu.VMEM((2, width, chunk), BF16),
        pltpu.VMEM((2, 2, tokens, chunk), BF16),
        pltpu.VMEM((SLOTS, 4, sub, width), BF16),
        pltpu.VMEM((PARTS, 4, sub, width), BF16),
        pltpu.VMEM((RECV0, 4, sub, width), BF16),
        pltpu.VMEM((RECV, 2, sub, width), BF16),
        pltpu.VMEM((RECV, 1, sub, width), BF16),
        *[dma((SLOTS,))] * 11,
        *[dma((RECV,))] * 2,
        *[reg((RECV,))] * 2,
        dma((PARTS,)), dma((RECV0,)), reg((RECV0,)),
        dma((2,)), dma((2,)), dma((2,)), dma((2,)), dma((2,)), dma((2, 2)), dma,
    ]
    return pl.pallas_call(
        functools.partial(backward_body, layers=layers, tokens=tokens, width=width, wide=wide, rows=rows),
        out_shape=[shape((units, 2, 8, sub, width), BF16), shape((tokens, width), BF16)],
        in_specs=[hbm] * 10,
        out_specs=[hbm] * 2,
        scratch_shapes=scratch,
        compiler_params=pltpu.CompilerParams(collective_id=0, has_side_effects=True, vmem_limit_bytes=VMEM_LIMIT),
        name="backward",
    )(w_one, w_two, *us, *as_, *hs, *dys)


COPY_SLOTS, COPY_LEAD = 24, 10


def assemble_body(tot, one, two, buf, s_in, s_out, *, layers, nu, nm, width):
    items = 4 * nu * layers

    def load(j):
        return pltpu.make_async_copy(tot.at[j // 2, j % 2], buf.at[j % COPY_SLOTS], s_in.at[j % COPY_SLOTS])

    def stores(j, run):
        n, core = j // 2, j % 2
        layer, i, slot = layers - 1 - n // (2 * nu), n % nu, j % COPY_SLOTS
        mid = (n % 3) // 2
        for q in range(4):
            src = (1 - mid) * q + mid * (q % 2 * 2 + q // 2)
            piece = buf.at[slot, pl.ds(src * 2, 2)]

            @pl.when((n // nu) % 2 == 0)
            def _():
                run(pltpu.make_async_copy(piece, two.at[layer, core * nu + i, pl.ds(2 * q, 2)], s_out.at[slot, q]))

            @pl.when((n // nu) % 2 == 1)
            def _():
                cols = pl.ds(pl.multiple_of((core * (nu // nm) + i // nm) * width, 128), width)
                run(pltpu.make_async_copy(piece, one.at[layer, i % nm, pl.ds(2 * q, 2), :, cols], s_out.at[slot, q]))

    def step(j, carry):
        @pl.when(j >= COPY_SLOTS)
        def _():
            stores(j - COPY_SLOTS, lambda c: c.wait())

        @pl.when(j < items)
        def _():
            load(j).start()

        @pl.when(jnp.logical_and(j >= COPY_LEAD, j < items + COPY_LEAD))
        def _():
            load(j - COPY_LEAD).wait()
            stores(j - COPY_LEAD, lambda c: c.start())

        return carry

    lax.fori_loop(0, items + COPY_SLOTS, step, 0)


def assemble(tot, layers, width, wide, rows):
    nu, nm, sub = wide // 2 // rows, width // rows, rows // 8
    shape = jax.ShapeDtypeStruct
    hbm = pl.BlockSpec(memory_space=pl.ANY)
    one, two = pl.pallas_call(
        functools.partial(assemble_body, layers=layers, nu=nu, nm=nm, width=width),
        out_shape=[shape((layers, nm, 8, sub, wide), BF16), shape((layers, 2 * nu, 8, sub, width), BF16)],
        in_specs=[hbm],
        out_specs=[hbm, hbm],
        scratch_shapes=[pltpu.VMEM((COPY_SLOTS, 8, sub, width), BF16), pltpu.SemaphoreType.DMA((COPY_SLOTS,)), pltpu.SemaphoreType.DMA((COPY_SLOTS, 4))],
        compiler_params=pltpu.CompilerParams(vmem_limit_bytes=VMEM_LIMIT),
        name="assemble",
    )(tot)
    return one.reshape(layers, width, wide), two.reshape(layers, wide, width)


def solution(mesh, rows=UNIT_ROWS):
    batch_spec = P(AXES)

    def per_device(w_one, w_two, x_loc, dy_loc):
        layers, width, wide = w_one.shape
        x = x_loc.reshape(-1, width)
        dy = dy_loc.reshape(-1, width)
        swap = [(0, 1), (1, 0)]
        x_nbr = lax.ppermute(x, "replica", swap)
        dy_nbr = lax.ppermute(dy, "replica", swap)
        z = jnp.full((1,), lax.axis_index("replica"), jnp.int32)
        kept = [forward(z, tokens, w_one, w_two, rows) for tokens in (x, x_nbr)]
        us, as_, hs = zip(*kept)
        tot, dx = backward(w_one, w_two, us, as_, hs, (dy, dy_nbr), rows)
        one, two = assemble(tot, layers, width, wide, rows)
        return one, two, dx.reshape(x_loc.shape)

    return jax.shard_map(per_device, mesh=mesh, in_specs=(P(), P(), batch_spec, batch_spec), out_specs=(P(), P(), batch_spec), check_vma=False)
```

```python
import functools

import jax
import jax.numpy as jnp
from jax import lax
from jax.experimental import pallas as pl
from jax.experimental.pallas import tpu as pltpu
from jax.sharding import PartitionSpec as P

AXES = ("replica", "data")
MESH = pl.DeviceIdType.MESH
BF16, F32 = jnp.bfloat16, jnp.float32
VMEM_LIMIT = 67_043_328
C0, C1 = 0.7978845608028654, 0.044715
UNIT_ROWS = 256
LAG = 3
SLOTS, SEMS, RECV, PARTS, RECV0 = 44, 12, 10, 3, 4
PACE = 7
X, Y, Z = 0, 1, 2


def gelu(v):
    return 0.5 * v * (1.0 + jnp.tanh(C0 * (v + C1 * (v * v * v))))


def gelu_slope(v):
    sq = v * v
    t = jnp.tanh(v * (C0 + C0 * C1 * sq))
    return 0.5 + 0.5 * t + v * (1.0 - t * t) * (0.5 * C0 + 1.5 * C0 * C1 * sq)


def mm(lhs, rhs, lhs_dim, rhs_dim):
    return lax.dot_general(lhs, rhs, (((lhs_dim,), (rhs_dim,)), ((), ())), preferred_element_type=F32)


def forward_body(z_ref, x_ref, w1_ref, w2_ref, u_ref, a_ref, h_ref, hid, acc, act_s, *, layers, chunks, rows):
    layer, j = pl.program_id(0), pl.program_id(1)
    part = rows // 2
    shift = z_ref[0] * part

    def pick(ref, k):
        return ref[:, pl.ds(pl.multiple_of(k * rows + shift, part), part)]

    @pl.when(jnp.logical_and(layer == 0, j == 0))
    def _():
        hid[...] = x_ref[...]

    @pl.when(j == 0)
    def _():
        for k in range(hid.shape[1] // rows):
            h_ref[0, :, k * part : (k + 1) * part] = pick(hid, k)
        acc[...] = hid[...].astype(F32)

    pre = mm(hid[...], w1_ref[0], 1, 0).astype(BF16)
    u_ref[0] = pre
    act = gelu(pre.astype(F32)).astype(BF16)
    act_s[...] = act

    @pl.when(layer < layers - 1)
    def _():
        acc[...] += mm(act, w2_ref[0], 1, 0)

        @pl.when(j == chunks - 1)
        def _():
            hid[...] = acc[...].astype(BF16)

    for k in range(act_s.shape[1] // rows):
        a_ref[0, :, k * part : (k + 1) * part] = pick(act_s, k)


def forward(z, x, w_one, w_two, rows):
    layers, width, wide = w_one.shape
    tokens = x.shape[0]
    chunk = width
    chunks = wide // chunk
    shape = jax.ShapeDtypeStruct
    return pl.pallas_call(
        functools.partial(forward_body, layers=layers, chunks=chunks, rows=rows),
        grid=(layers, chunks),
        out_shape=[shape((layers, tokens, wide), BF16), shape((layers, tokens, wide // 2), BF16), shape((layers, tokens, width // 2), BF16)],
        in_specs=[
            pl.BlockSpec(memory_space=pltpu.SMEM),
            pl.BlockSpec((tokens, width), lambda l, j: (0, 0)),
            pl.BlockSpec((1, width, chunk), lambda l, j: (l, 0, j)),
            pl.BlockSpec((1, chunk, width), lambda l, j: (l, j, 0)),
        ],
        out_specs=[
            pl.BlockSpec((1, tokens, chunk), lambda l, j: (l, 0, j)),
            pl.BlockSpec((1, tokens, chunk // 2), lambda l, j: (l, 0, j)),
            pl.BlockSpec((1, tokens, width // 2), lambda l, j: (l, 0, 0)),
        ],
        scratch_shapes=[pltpu.VMEM((tokens, width), BF16), pltpu.VMEM((tokens, width), F32), pltpu.VMEM((tokens, chunk), BF16)],
        compiler_params=pltpu.CompilerParams(vmem_limit_bytes=VMEM_LIMIT),
        cost_estimate=pl.CostEstimate(
            flops=(4 * layers - 2) * tokens * width * wide, bytes_accessed=4 * layers * width * wide, transcendentals=layers * tokens * wide
        ),
        name="forward",
    )(z, x, w_one, w_two)


def backward_body(
    w1, w2, u_own, u_nbr, a_own, a_nbr, h_own, h_nbr, dy_own, dy_nbr,
    tot, dx,
    a_cat, du_cat, h_cat, gb_cat, g, w2c, w1c, uc, unit, part0, rcv0, rcv1, rcv2,
    s_rs1, s_rs2, s_ag1, s_ag2, s_ag3, s_fwd, s_own, r_ag1, r_ag2, r_ag3, r_fwd,
    r_rs1, r_rs2, c_rs1, c_rs2, s_rs0, r_rs0, c_rs0,
    l_a, l_gb, l_h, l_w2, l_w1, l_u, l_dx,
    *, layers, tokens, width, wide, rows,
):
    half = wide // 2
    part = rows // 2
    nu = half // rows
    nm = width // rows
    nf = nu // nm
    chunk = wide // nu
    units = 2 * nu * layers
    pieces = 2 * units
    narrow = width // 2
    step = tokens // 2
    z, rest = lax.axis_index("replica"), lax.axis_index("data")
    core, x, y = rest % 2, (rest // 2) % 2, rest // 4

    def choose(axis):
        return (1 - axis) * (2 - axis) // 2, axis * (2 - axis), axis * (axis - 1) // 2

    def peer(axis):
        ex, ey, ez = choose(axis)
        px, py, pz = x + ex * (1 - 2 * x), y + ey * (1 - 2 * y), z + ez * (1 - 2 * z)
        return (pz, (py * 2 + px) * 2 + core)

    sibling = (z, (y * 2 + x) * 2 + 1 - core)

    def send(src, dst, ssem, rsem, to):
        return pltpu.make_async_remote_copy(src_ref=src, dst_ref=dst, send_sem=ssem, recv_sem=rsem, device_id=to, device_id_type=MESH)

    def place(m):
        mid = (m % 3) // 2
        a_axis = (1 - mid) * (m % 3) + mid * ((m // 3) % 2)
        b_axis = 1 - a_axis
        bit_a = x + a_axis * (y - x)
        bit_b = x + b_axis * (y - x)
        own = (1 - mid) * (4 * z + 2 * bit_a + bit_b) + mid * (4 * bit_a + 2 * z + bit_b)
        return mid, a_axis, b_axis, bit_a, bit_b, own

    def rs0(n):
        return send(part0.at[n % PARTS], rcv0.at[n % RECV0], s_rs0.at[n % PARTS], r_rs0.at[n % RECV0], sibling)

    def rs1(m):
        mid, a_axis, b_axis, bit_a, bit_b, own = place(m)
        return send(unit.at[m % SLOTS, pl.ds(2 - 2 * bit_a, 2)], rcv1.at[m % RECV], s_rs1.at[m % SEMS], r_rs1.at[m % RECV], peer(a_axis))

    def rs2(m):
        mid, a_axis, b_axis, bit_a, bit_b, own = place(m)
        return send(unit.at[m % SLOTS, pl.ds(2 * bit_a + 1 - bit_b, 1)], rcv2.at[m % RECV], s_rs2.at[m % SEMS], r_rs2.at[m % RECV], peer(b_axis))

    def own_copy(m):
        mid, a_axis, b_axis, bit_a, bit_b, own = place(m)
        return pltpu.make_async_copy(unit.at[m % SLOTS, pl.ds(2 * bit_a + bit_b, 1)], tot.at[m, core, pl.ds(own, 1)], s_own.at[m % SEMS])

    def ag1(m):
        mid, a_axis, b_axis, bit_a, bit_b, own = place(m)
        return send(
            unit.at[m % SLOTS, pl.ds(2 * bit_a + bit_b, 1)], tot.at[m, core, pl.ds(own, 1)], s_ag1.at[m % SEMS], r_ag1.at[m % SEMS], peer(b_axis)
        )

    def ag2(m):
        mid, a_axis, b_axis, bit_a, bit_b, own = place(m)
        span = tot.at[m, core, pl.ds(own // 2 * 2, 2)]
        return send(span, span, s_ag2.at[m % SEMS], r_ag2.at[m % SEMS], peer(a_axis + mid * (Z - a_axis)))

    def ag3(m):
        mid, a_axis, b_axis, bit_a, bit_b, own = place(m)
        span = tot.at[m, core, pl.ds(own // 4 * 4, 4)]
        return send(span, span, s_ag3.at[m % SEMS], r_ag3.at[m % SEMS], peer(Z + mid * (a_axis - Z)))

    def fwd(m):
        span = tot.at[m, core]
        return send(span, span, s_fwd.at[m % SEMS], r_fwd.at[m % SEMS], sibling)

    def add(m, block, other):
        unit[m % SLOTS, block] = (unit[m % SLOTS, block].astype(F32) + other.astype(F32)).astype(BF16)

    def credit(sem, n, slots, count, to):
        @pl.when(n + slots < count)
        def _():
            pl.semaphore_signal(sem.at[n % slots], inc=1, device_id=to, device_id_type=MESH)

    def spend(sem, n, slots):
        @pl.when(n >= slots)
        def _():
            pl.semaphore_wait(sem.at[n % slots], 1)

    def live(m):
        return jnp.logical_and(m >= 0, m < pieces)

    def make(n, theirs, mine):
        part0[n % PARTS] = theirs.reshape(4, rows // 8, width).astype(BF16)
        kept = mine.reshape(4, rows // 8, width).astype(BF16)
        for c in range(2):
            unit[(2 * n + c) % SLOTS] = kept[:, :, c * narrow : (c + 1) * narrow]

    def push(n):
        spend(c_rs0, n, RECV0)
        rs0(n).start()

    def pair_sum(n):
        rs0(n).wait()
        for c in range(2):
            for block in range(4):
                add(2 * n + c, block, rcv0[n % RECV0, block, :, c * narrow : (c + 1) * narrow])
        credit(c_rs0, n, RECV0, units, sibling)

    def comm(r, carry):
        m0, m1, m2, m3, m4, m5 = (r - k * LAG for k in range(6))
        m6 = m5 - LAG

        @pl.when(live(m2))
        def _():
            mid, a_axis, b_axis, bit_a, bit_b, own = place(m2)
            rs2(m2).wait_recv()
            add(m2, 2 * bit_a + bit_b, rcv2[m2 % RECV, 0])
            credit(c_rs2, m2, RECV, pieces, peer(b_axis))
            rs1(m2).wait_send()

        @pl.when(live(m1))
        def _():
            mid, a_axis, b_axis, bit_a, bit_b, own = place(m1)
            rs1(m1).wait_recv()
            add(m1, 2 * bit_a + 1 - bit_b, rcv1[m1 % RECV, 1 - bit_b])
            add(m1, 2 * bit_a + bit_b, rcv1[m1 % RECV, bit_b])
            credit(c_rs1, m1, RECV, pieces, peer(a_axis))

        @pl.when(live(m0))
        def _():
            spend(c_rs1, m0, RECV)
            rs1(m0).start()

        @pl.when(live(m2))
        def _():
            own_copy(m2).start()
            ag1(m2).start()

        @pl.when(live(m1))
        def _():
            spend(c_rs2, m1, RECV)
            rs2(m1).start()

        @pl.when(live(m3))
        def _():
            rs2(m3).wait_send()
            own_copy(m3).wait()
            ag1(m3).wait()
            ag2(m3).start()

        @pl.when(live(m4))
        def _():
            ag2(m4).wait()
            ag3(m4).start()

        @pl.when(live(m5))
        def _():
            ag3(m5).wait()
            fwd(m5).start()

        @pl.when(live(m6))
        def _():
            fwd(m6).wait()

        return carry

    def rounds(lo, hi):
        lax.fori_loop(lo, hi, comm, 0)

    def spread(i):
        return PACE * i * i // (nu * nu)

    sets = (0, 1)
    us, as_, hs, dys = (u_own, u_nbr), (a_own, a_nbr), (h_own, h_nbr), (dy_own, dy_nbr)

    def of(k):
        return pl.ds(k * tokens, tokens)

    def loads(layer, i):
        f0, slot = pl.multiple_of(i * chunk, 128), i % 2
        return (
            pltpu.make_async_copy(w2.at[layer, pl.ds(f0, chunk)], w2c.at[slot], l_w2.at[slot]),
            pltpu.make_async_copy(w1.at[layer, :, pl.ds(f0, chunk)], w1c.at[slot], l_w1.at[slot]),
            *(pltpu.make_async_copy(us[k].at[layer, :, pl.ds(f0, chunk)], uc.at[slot, k], l_u.at[slot, k]) for k in sets),
        )

    def cols(i, size):
        return pl.ds(pl.multiple_of(i * size, 128), size)

    def a_load(layer, k):
        return pltpu.make_async_copy(as_[k].at[layer], a_cat.at[of(k)], l_a.at[k])

    def h_load(layer, k):
        return pltpu.make_async_copy(hs[k].at[layer], h_cat.at[of(k)], l_h.at[k])

    def gb_load(k):
        return pltpu.make_async_copy(dys[k], gb_cat.at[of(k)], l_gb.at[k])

    def dx_store():
        return pltpu.make_async_copy(gb_cat.at[of(0)], dx, l_dx)

    barrier = pltpu.get_barrier_semaphore()
    for to in (peer(X), peer(Y), peer(Z), sibling):
        pl.semaphore_signal(barrier, inc=1, device_id=to, device_id_type=MESH)
    for k in sets:
        gb_load(k).start()
        a_load(layers - 1, k).start()
    for load in loads(layers - 1, 0):
        load.start()
    for k in sets:
        gb_load(k).wait()
        g[of(k)] = gb_cat[of(k)].astype(F32)
    pl.semaphore_wait(barrier, 4)

    def layer_step(li, carry):
        layer = layers - 1 - li
        base = li * 2 * nu
        late = jnp.minimum(li, 1)
        r0 = (4 * nu * li - 2 * nu + PACE) * late
        r1 = r0 + PACE
        r2 = 4 * nu * li + 2 * nu
        for k in sets:
            a_load(layer, k).wait()

        def second_weight(i, carry):
            n = base + i
            lhs = jnp.concatenate([a_cat[:, cols((1 - core) * nu + i, part)], a_cat[:, cols(core * nu + i, part)]], axis=1)
            out = mm(lhs, gb_cat[...], 0, 0)
            make(n, out[:part], out[part:])

            @pl.when(n >= 2)
            def _():
                pair_sum(n - 2)

            push(n)
            rounds(r0 + spread(i), r0 + spread(i + 1))
            return carry

        lax.fori_loop(0, nu, second_weight, 0)
        pair_sum(base + nu - 2)
        pair_sum(base + nu - 1)
        for k in sets:
            h_load(layer, k).start()

        @pl.when(layer > 0)
        def _():
            for k in sets:
                a_load(layer - 1, k).start()

        def hidden_chunk(i, carry):
            for load in loads(layer, i):
                load.wait()

            @pl.when(i < nu - 1)
            def _():
                for load in loads(layer, i + 1):
                    load.start()

            def token_set(k, carry):
                at = [pl.ds(q * step, step) for q in range(2)]
                rows_q = [pl.ds(pl.multiple_of(k * tokens + q * step, 16), step) for q in range(2)]
                d_act = [mm(gb_cat[r], w2c[i % 2], 1, 1) for r in rows_q]
                for q in range(2):
                    du = (d_act[q] * gelu_slope(uc[i % 2, k, at[q]].astype(F32))).astype(BF16)
                    du_cat[rows_q[q], cols(i, chunk)] = du
                    g[rows_q[q]] += mm(du, w1c[i % 2], 1, 1)
                s = 2 * i + k
                rounds(r1 + (r2 - r1) * s // (2 * nu), r1 + (r2 - r1) * (s + 1) // (2 * nu))
                return carry

            lax.fori_loop(0, 2, token_set, 0)
            return carry

        lax.fori_loop(0, nu, hidden_chunk, 0)
        for k in sets:
            gb_cat[of(k)] = g[of(k)].astype(BF16)
        for k in sets:
            h_load(layer, k).wait()

        @pl.when(layer > 0)
        def _():
            for load in loads(layer - 1, 0):
                load.start()

        @pl.when(layer == 0)
        def _():
            dx_store().start()

        def first_weight(i, carry):
            n = base + nu + i
            mi, fi = i % nm, i // nm
            lhs = h_cat[:, cols(mi, part)]
            make(
                n,
                mm(lhs, du_cat[:, cols((1 - core) * nf + fi, width)], 0, 0),
                mm(lhs, du_cat[:, cols(core * nf + fi, width)], 0, 0),
            )

            @pl.when(i >= 2)
            def _():
                pair_sum(n - 2)

            push(n)
            rounds(r2 + spread(i), r2 + spread(i + 1))
            return carry

        lax.fori_loop(0, nu, first_weight, 0)
        return carry

    lax.fori_loop(0, layers, layer_step, 0)
    pair_sum(units - 2)
    pair_sum(units - 1)
    rounds(4 * nu * layers - 2 * nu + PACE, pieces + 6 * LAG)
    dx_store().wait()


def backward(w_one, w_two, us, as_, hs, dys, rows):
    layers, width, wide = w_one.shape
    tokens = dys[0].shape[0]
    half = wide // 2
    nu = half // rows
    chunk = wide // nu
    units = 2 * nu * layers
    dma, reg = pltpu.SemaphoreType.DMA, pltpu.SemaphoreType.REGULAR
    hbm = pl.BlockSpec(memory_space=pl.ANY)
    sub, narrow = rows // 8, width // 2
    shape = jax.ShapeDtypeStruct
    scratch = [
        pltpu.VMEM((2 * tokens, half), BF16),
        pltpu.VMEM((2 * tokens, wide), BF16),
        pltpu.VMEM((2 * tokens, width // 2), BF16),
        pltpu.VMEM((2 * tokens, width), BF16),
        pltpu.VMEM((2 * tokens, width), F32),
        pltpu.VMEM((2, chunk, width), BF16),
        pltpu.VMEM((2, width, chunk), BF16),
        pltpu.VMEM((2, 2, tokens, chunk), BF16),
        pltpu.VMEM((SLOTS, 4, sub, narrow), BF16),
        pltpu.VMEM((PARTS, 4, sub, width), BF16),
        pltpu.VMEM((RECV0, 4, sub, width), BF16),
        pltpu.VMEM((RECV, 2, sub, narrow), BF16),
        pltpu.VMEM((RECV, 1, sub, narrow), BF16),
        *[dma((SEMS,))] * 11,
        *[dma((RECV,))] * 2,
        *[reg((RECV,))] * 2,
        dma((PARTS,)), dma((RECV0,)), reg((RECV0,)),
        dma((2,)), dma((2,)), dma((2,)), dma((2,)), dma((2,)), dma((2, 2)), dma,
    ]
    return pl.pallas_call(
        functools.partial(backward_body, layers=layers, tokens=tokens, width=width, wide=wide, rows=rows),
        out_shape=[shape((2 * units, 2, 8, sub, narrow), BF16), shape((tokens, width), BF16)],
        in_specs=[hbm] * 10,
        out_specs=[hbm] * 2,
        scratch_shapes=scratch,
        compiler_params=pltpu.CompilerParams(collective_id=0, has_side_effects=True, vmem_limit_bytes=VMEM_LIMIT),
        name="backward",
    )(w_one, w_two, *us, *as_, *hs, *dys)


COPY_SLOTS, COPY_LEAD = 40, 16


def assemble_body(tot, one, two, buf, s_in, s_out, *, layers, nu, nm, width):
    items = 8 * nu * layers
    narrow = width // 2

    def load(j):
        return pltpu.make_async_copy(tot.at[j // 2, j % 2], buf.at[j % COPY_SLOTS], s_in.at[j % COPY_SLOTS])

    def stores(j, run):
        m, core, slot = j // 2, j % 2, j % COPY_SLOTS
        n, side = m // 2, m % 2
        layer, i = layers - 1 - n // (2 * nu), n % nu
        mid = (m % 3) // 2
        for q in range(4):
            src = (1 - mid) * q + mid * (q % 2 * 2 + q // 2)
            span = buf.at[slot, pl.ds(src * 2, 2)]

            @pl.when((n // nu) % 2 == 0)
            def _():
                cols = pl.ds(pl.multiple_of(side * narrow, 128), narrow)
                run(pltpu.make_async_copy(span, two.at[layer, core * nu + i, pl.ds(2 * q, 2), :, cols], s_out.at[slot, q]))

            @pl.when((n // nu) % 2 == 1)
            def _():
                cols = pl.ds(pl.multiple_of((core * (nu // nm) + i // nm) * width + side * narrow, 128), narrow)
                run(pltpu.make_async_copy(span, one.at[layer, i % nm, pl.ds(2 * q, 2), :, cols], s_out.at[slot, q]))

    def step(j, carry):
        @pl.when(j >= COPY_SLOTS)
        def _():
            stores(j - COPY_SLOTS, lambda c: c.wait())

        @pl.when(j < items)
        def _():
            load(j).start()

        @pl.when(jnp.logical_and(j >= COPY_LEAD, j < items + COPY_LEAD))
        def _():
            load(j - COPY_LEAD).wait()
            stores(j - COPY_LEAD, lambda c: c.start())

        return carry

    lax.fori_loop(0, items + COPY_SLOTS, step, 0)


def assemble(tot, layers, width, wide, rows):
    nu, nm, sub = wide // 2 // rows, width // rows, rows // 8
    shape = jax.ShapeDtypeStruct
    hbm = pl.BlockSpec(memory_space=pl.ANY)
    one, two = pl.pallas_call(
        functools.partial(assemble_body, layers=layers, nu=nu, nm=nm, width=width),
        out_shape=[shape((layers, nm, 8, sub, wide), BF16), shape((layers, 2 * nu, 8, sub, width), BF16)],
        in_specs=[hbm],
        out_specs=[hbm, hbm],
        scratch_shapes=[pltpu.VMEM((COPY_SLOTS, 8, sub, width // 2), BF16), pltpu.SemaphoreType.DMA((COPY_SLOTS,)), pltpu.SemaphoreType.DMA((COPY_SLOTS, 4))],
        compiler_params=pltpu.CompilerParams(vmem_limit_bytes=VMEM_LIMIT),
        name="assemble",
    )(tot)
    return one.reshape(layers, width, wide), two.reshape(layers, wide, width)


def solution(mesh, rows=UNIT_ROWS):
    batch_spec = P(AXES)

    def per_device(w_one, w_two, x_loc, dy_loc):
        layers, width, wide = w_one.shape
        x = x_loc.reshape(-1, width)
        dy = dy_loc.reshape(-1, width)
        swap = [(0, 1), (1, 0)]
        x_nbr = lax.ppermute(x, "replica", swap)
        dy_nbr = lax.ppermute(dy, "replica", swap)
        z = jnp.full((1,), lax.axis_index("replica"), jnp.int32)
        kept = [forward(z, tokens, w_one, w_two, rows) for tokens in (x, x_nbr)]
        us, as_, hs = zip(*kept)
        tot, dx = backward(w_one, w_two, us, as_, hs, (dy, dy_nbr), rows)
        one, two = assemble(tot, layers, width, wide, rows)
        return one, two, dx.reshape(x_loc.shape)

    return jax.shard_map(per_device, mesh=mesh, in_specs=(P(), P(), batch_spec, batch_spec), out_specs=(P(), P(), batch_spec), check_vma=False)
```

```python
import functools

import jax
import jax.numpy as jnp
from jax import lax
from jax.experimental import pallas as pl
from jax.experimental.pallas import tpu as pltpu
from jax.sharding import PartitionSpec as P

AXES = ("replica", "data")
MESH = pl.DeviceIdType.MESH
BF16, F32 = jnp.bfloat16, jnp.float32
VMEM_LIMIT = 67_043_328
C0, C1 = 0.7978845608028654, 0.044715
UNIT_ROWS = 256
LAG = 3
SLOTS, SEMS, RECV, PARTS, RECV0 = 44, 12, 10, 3, 4
PACE_FIRST, PACE = (6, 16, 19, 26, 30), (-2, 12, 16, 26, 30)
X, Y, Z = 0, 1, 2


def gelu(v):
    half = 0.5 * v
    return half + half * jnp.tanh(v * (C0 + C0 * C1 * (v * v)))


def gelu_slope(v):
    sq = v * v
    t = jnp.tanh(v * (C0 + C0 * C1 * sq))
    return 0.5 + 0.5 * t + v * (1.0 - t * t) * (0.5 * C0 + 1.5 * C0 * C1 * sq)


def mm(lhs, rhs, lhs_dim, rhs_dim):
    return lax.dot_general(lhs, rhs, (((lhs_dim,), (rhs_dim,)), ((), ())), preferred_element_type=F32)


def forward_body(z_ref, x_ref, w1_ref, w2_ref, u_ref, a_ref, h_ref, hid, acc, act_s, *, layers, chunks, rows):
    layer, j = pl.program_id(0), pl.program_id(1)
    part = rows // 2
    shift = z_ref[0] * part

    def keep(dst, src):
        for k in range(src.shape[1] // rows):
            dst[0, :, k * part : (k + 1) * part] = src[:, pl.ds(pl.multiple_of(k * rows + shift, part), part)]

    @pl.when(jnp.logical_and(layer == 0, j == 0))
    def _():
        hid[...] = x_ref[...]

    @pl.when(j == 0)
    def _():
        keep(h_ref, hid)
        acc[...] = hid[...].astype(F32)

    def up():
        pre = mm(hid[...], w1_ref[0], 1, 0).astype(BF16)
        u_ref[0] = pre
        act = gelu(pre.astype(F32)).astype(BF16)
        act_s[...] = act
        keep(a_ref, act_s)
        return act

    @pl.when(layer < layers - 1)
    def _():
        acc[...] += mm(up(), w2_ref[0], 1, 0)

        @pl.when(j == chunks - 1)
        def _():
            hid[...] = acc[...].astype(BF16)

    @pl.when(layer == layers - 1)
    def _():
        up()


def forward(z, x, w_one, w_two, rows):
    layers, width, wide = w_one.shape
    tokens = x.shape[0]
    chunk = width
    chunks = wide // chunk
    shape = jax.ShapeDtypeStruct
    return pl.pallas_call(
        functools.partial(forward_body, layers=layers, chunks=chunks, rows=rows),
        grid=(layers, chunks),
        out_shape=[shape((layers, tokens, wide), BF16), shape((layers, tokens, wide // 2), BF16), shape((layers, tokens, width // 2), BF16)],
        in_specs=[
            pl.BlockSpec(memory_space=pltpu.SMEM),
            pl.BlockSpec((tokens, width), lambda l, j: (0, 0)),
            pl.BlockSpec((1, width, chunk), lambda l, j: (l, 0, j)),
            pl.BlockSpec((1, chunk, width), lambda l, j: (l, j, 0)),
        ],
        out_specs=[
            pl.BlockSpec((1, tokens, chunk), lambda l, j: (l, 0, j)),
            pl.BlockSpec((1, tokens, chunk // 2), lambda l, j: (l, 0, j)),
            pl.BlockSpec((1, tokens, width // 2), lambda l, j: (l, 0, 0)),
        ],
        scratch_shapes=[pltpu.VMEM((tokens, width), BF16), pltpu.VMEM((tokens, width), F32), pltpu.VMEM((tokens, chunk), BF16)],
        compiler_params=pltpu.CompilerParams(vmem_limit_bytes=VMEM_LIMIT),
        cost_estimate=pl.CostEstimate(
            flops=(4 * layers - 2) * tokens * width * wide, bytes_accessed=4 * layers * width * wide, transcendentals=layers * tokens * wide
        ),
        name="forward",
    )(z, x, w_one, w_two)


def backward_body(
    w1, w2, u_own, u_nbr, a_own, a_nbr, h_own, h_nbr, dy_own, dy_nbr,
    tot, dx, last,
    a_cat, du_cat, h_cat, gb_cat, g, w2c, w1c, uc, unit, part0, rcv0, rcv1, rcv2,
    s_rs1, s_rs2, s_ag1, s_ag2, s_ag3, s_fwd, s_own, r_ag1, r_ag2, r_ag3, r_fwd,
    r_rs1, r_rs2, c_rs1, c_rs2, s_rs0, r_rs0, c_rs0,
    l_a, l_gb, l_h, l_w2, l_w1, l_u, l_dx,
    *, layers, tokens, width, wide, rows,
):
    half = wide // 2
    part = rows // 2
    nu = half // rows
    hn = nu // 2
    nm = width // rows
    nf = nu // nm
    chunk = wide // nu
    units = 2 * nu * layers
    pieces = 2 * units
    whole = pieces - 2 * nu
    early = (hn + 1) // 2
    narrow = width // 2
    step = tokens // 2
    z, rest = lax.axis_index("replica"), lax.axis_index("data")
    core, x, y = rest % 2, (rest // 2) % 2, rest // 4

    def choose(axis):
        return (1 - axis) * (2 - axis) // 2, axis * (2 - axis), axis * (axis - 1) // 2

    def peer(axis):
        ex, ey, ez = choose(axis)
        px, py, pz = x + ex * (1 - 2 * x), y + ey * (1 - 2 * y), z + ez * (1 - 2 * z)
        return (pz, (py * 2 + px) * 2 + core)

    sibling = (z, (y * 2 + x) * 2 + 1 - core)

    def send(src, dst, ssem, rsem, to):
        return pltpu.make_async_remote_copy(src_ref=src, dst_ref=dst, send_sem=ssem, recv_sem=rsem, device_id=to, device_id_type=MESH)

    def place(m):
        mid = (m % 3) // 2
        a_axis = (1 - mid) * (m % 3) + mid * ((m // 3) % 2)
        b_axis = 1 - a_axis
        bit_a = x + a_axis * (y - x)
        bit_b = x + b_axis * (y - x)
        own = (1 - mid) * (4 * z + 2 * bit_a + bit_b) + mid * (4 * bit_a + 2 * z + bit_b)
        return mid, a_axis, b_axis, bit_a, bit_b, own

    def rs0(n):
        return send(part0.at[n % PARTS], rcv0.at[n % RECV0], s_rs0.at[n % PARTS], r_rs0.at[n % RECV0], sibling)

    def rs1(m):
        mid, a_axis, b_axis, bit_a, bit_b, own = place(m)
        return send(unit.at[m % SLOTS, pl.ds(2 - 2 * bit_a, 2)], rcv1.at[m % RECV], s_rs1.at[m % SEMS], r_rs1.at[m % RECV], peer(a_axis))

    def rs2(m):
        mid, a_axis, b_axis, bit_a, bit_b, own = place(m)
        return send(unit.at[m % SLOTS, pl.ds(2 * bit_a + 1 - bit_b, 1)], rcv2.at[m % RECV], s_rs2.at[m % SEMS], r_rs2.at[m % RECV], peer(b_axis))

    def own_copy(m):
        mid, a_axis, b_axis, bit_a, bit_b, own = place(m)
        return pltpu.make_async_copy(unit.at[m % SLOTS, pl.ds(2 * bit_a + bit_b, 1)], tot.at[m, core, pl.ds(own, 1)], s_own.at[m % SEMS])

    def last_copy(m):
        mid, a_axis, b_axis, bit_a, bit_b, own = place(m)
        return pltpu.make_async_copy(unit.at[m % SLOTS, pl.ds(2 * bit_a + bit_b, 1)], last.at[pl.ds(m - whole, 1)], s_own.at[m % SEMS])

    def ag1(m):
        mid, a_axis, b_axis, bit_a, bit_b, own = place(m)
        return send(
            unit.at[m % SLOTS, pl.ds(2 * bit_a + bit_b, 1)], tot.at[m, core, pl.ds(own, 1)], s_ag1.at[m % SEMS], r_ag1.at[m % SEMS], peer(b_axis)
        )

    def ag2(m):
        mid, a_axis, b_axis, bit_a, bit_b, own = place(m)
        span = tot.at[m, core, pl.ds(own // 2 * 2, 2)]
        return send(span, span, s_ag2.at[m % SEMS], r_ag2.at[m % SEMS], peer(a_axis + mid * (Z - a_axis)))

    def ag3(m):
        mid, a_axis, b_axis, bit_a, bit_b, own = place(m)
        span = tot.at[m, core, pl.ds(own // 4 * 4, 4)]
        return send(span, span, s_ag3.at[m % SEMS], r_ag3.at[m % SEMS], peer(Z + mid * (a_axis - Z)))

    def fwd(m):
        span = tot.at[m, core]
        return send(span, span, s_fwd.at[m % SEMS], r_fwd.at[m % SEMS], sibling)

    def add(m, block, other):
        unit[m % SLOTS, block] = (unit[m % SLOTS, block].astype(F32) + other.astype(F32)).astype(BF16)

    def credit(sem, n, slots, count, to):
        @pl.when(n + slots < count)
        def _():
            pl.semaphore_signal(sem.at[n % slots], inc=1, device_id=to, device_id_type=MESH)

    def spend(sem, n, slots):
        @pl.when(n >= slots)
        def _():
            pl.semaphore_wait(sem.at[n % slots], 1)

    def live(m):
        return jnp.logical_and(m >= 0, m < pieces)

    def spread_out(m):
        return jnp.logical_and(m >= 0, m < whole)

    def left(m):
        return jnp.logical_and(m >= whole, m < pieces)

    def make(n, theirs, mine):
        part0[n % PARTS] = theirs.reshape(4, rows // 8, width).astype(BF16)
        kept = mine.reshape(4, rows // 8, width).astype(BF16)
        for c in range(2):
            unit[(2 * n + c) % SLOTS] = kept[:, :, c * narrow : (c + 1) * narrow]

    def push(n):
        spend(c_rs0, n, RECV0)
        rs0(n).start()

    def pair_sum(n):
        rs0(n).wait()
        for c in range(2):
            for block in range(4):
                add(2 * n + c, block, rcv0[n % RECV0, block, :, c * narrow : (c + 1) * narrow])
        credit(c_rs0, n, RECV0, units, sibling)

    def comm(r, carry):
        m0, m1, m2, m3, m4, m5 = (r - k * LAG for k in range(6))
        m6 = m5 - LAG

        @pl.when(live(m2))
        def _():
            mid, a_axis, b_axis, bit_a, bit_b, own = place(m2)
            rs2(m2).wait_recv()
            add(m2, 2 * bit_a + bit_b, rcv2[m2 % RECV, 0])
            credit(c_rs2, m2, RECV, pieces, peer(b_axis))
            rs1(m2).wait_send()

        @pl.when(live(m1))
        def _():
            mid, a_axis, b_axis, bit_a, bit_b, own = place(m1)
            rs1(m1).wait_recv()
            add(m1, 2 * bit_a + 1 - bit_b, rcv1[m1 % RECV, 1 - bit_b])
            add(m1, 2 * bit_a + bit_b, rcv1[m1 % RECV, bit_b])
            credit(c_rs1, m1, RECV, pieces, peer(a_axis))

        @pl.when(live(m0))
        def _():
            spend(c_rs1, m0, RECV)
            rs1(m0).start()

        @pl.when(spread_out(m2))
        def _():
            own_copy(m2).start()
            ag1(m2).start()

        @pl.when(left(m2))
        def _():
            last_copy(m2).start()

        @pl.when(live(m1))
        def _():
            spend(c_rs2, m1, RECV)
            rs2(m1).start()

        @pl.when(live(m3))
        def _():
            rs2(m3).wait_send()

        @pl.when(left(m3))
        def _():
            last_copy(m3).wait()

        @pl.when(spread_out(m3))
        def _():
            own_copy(m3).wait()
            ag1(m3).wait()
            ag2(m3).start()

        @pl.when(spread_out(m4))
        def _():
            ag2(m4).wait()
            ag3(m4).start()

        @pl.when(spread_out(m5))
        def _():
            ag3(m5).wait()
            fwd(m5).start()

        @pl.when(spread_out(m6))
        def _():
            fwd(m6).wait()

        return carry

    def rounds(lo, hi):
        lax.fori_loop(lo, hi, comm, 0)

    def ramp(lo, hi, i, n):
        return lo + (hi - lo) * i * i // (n * n)

    sets = (0, 1)
    us, as_, hs, dys = (u_own, u_nbr), (a_own, a_nbr), (h_own, h_nbr), (dy_own, dy_nbr)

    def of(k):
        return pl.ds(k * tokens, tokens)

    def chunk_at(i):
        late, wait = hn - early, i // (2 * early)
        first = i // early * hn + i % early
        second = early + (i - 2 * early) // late * hn + (i - 2 * early) % late
        return first + wait * (second - first)

    def loads(layer, i):
        f0, slot = pl.multiple_of(chunk_at(i) * chunk, 128), i % 2
        return (
            pltpu.make_async_copy(w2.at[layer, pl.ds(f0, chunk)], w2c.at[slot], l_w2.at[slot]),
            pltpu.make_async_copy(w1.at[layer, :, pl.ds(f0, chunk)], w1c.at[slot], l_w1.at[slot]),
            *(pltpu.make_async_copy(us[k].at[layer, :, pl.ds(f0, chunk)], uc.at[slot, k], l_u.at[slot, k]) for k in sets),
        )

    def cols(i, size):
        return pl.ds(pl.multiple_of(i * size, 128), size)

    def a_load(layer, k):
        return pltpu.make_async_copy(as_[k].at[layer], a_cat.at[of(k)], l_a.at[k])

    def h_load(layer, k):
        return pltpu.make_async_copy(hs[k].at[layer], h_cat.at[of(k)], l_h.at[k])

    def gb_load(k):
        return pltpu.make_async_copy(dys[k], gb_cat.at[of(k)], l_gb.at[k])

    def dx_store():
        return pltpu.make_async_copy(gb_cat.at[of(0)], dx, l_dx)

    barrier = pltpu.get_barrier_semaphore()
    for to in (peer(X), peer(Y), peer(Z), sibling):
        pl.semaphore_signal(barrier, inc=1, device_id=to, device_id_type=MESH)
    for k in sets:
        gb_load(k).start()
        a_load(layers - 1, k).start()
    for load in loads(layers - 1, 0):
        load.start()
    for k in sets:
        gb_load(k).wait()
    pl.semaphore_wait(barrier, 4)

    def layer_step(li, carry):
        layer = layers - 1 - li
        base = li * 2 * nu
        late = jnp.minimum(li, 1)
        due = [late * (4 * nu * (li - 1) + PACE[4] * nu // 10)]
        for p, q in zip(PACE_FIRST, PACE):
            due.append(4 * nu * li + p * nu // 10 + late * (q * nu // 10 - p * nu // 10))
        for k in sets:
            a_load(layer, k).wait()

        def second_weight(i, carry):
            n = base + i
            lhs = jnp.concatenate([a_cat[:, cols((1 - core) * nu + i, part)], a_cat[:, cols(core * nu + i, part)]], axis=1)
            out = mm(lhs, gb_cat[...], 0, 0)
            make(n, out[:part], out[part:])

            @pl.when(i >= 2)
            def _():
                pair_sum(n - 2)

            push(n)
            rounds(ramp(due[0], due[1], i, nu), ramp(due[0], due[1], i + 1, nu))
            return carry

        lax.fori_loop(0, nu, second_weight, 0)
        pair_sum(base + nu - 2)
        pair_sum(base + nu - 1)
        for k in sets:
            h_load(layer, k).start()

        @pl.when(li == 0)
        def _():
            for k in sets:
                g[of(k)] = gb_cat[of(k)].astype(F32)

        @pl.when(layer > 0)
        def _():
            for k in sets:
                a_load(layer - 1, k).start()

        def hidden_chunk(from_i, to_i, start, stop, i, carry):
            for load in loads(layer, i):
                load.wait()

            @pl.when(i < nu - 1)
            def _():
                for load in loads(layer, i + 1):
                    load.start()

            def token_set(k, carry):
                at = [pl.ds(q * step, step) for q in range(2)]
                rows_q = [pl.ds(pl.multiple_of(k * tokens + q * step, 16), step) for q in range(2)]
                d_act = [mm(gb_cat[r], w2c[i % 2], 1, 1) for r in rows_q]
                for q in range(2):
                    du = (d_act[q] * gelu_slope(uc[i % 2, k, at[q]].astype(F32))).astype(BF16)
                    du_cat[rows_q[q], cols(chunk_at(i), chunk)] = du
                    g[rows_q[q]] += mm(du, w1c[i % 2], 1, 1)
                s = 2 * (i - from_i) + k
                rounds(start + (stop - start) * s // (4 * early), start + (stop - start) * (s + 1) // (4 * early))
                return carry

            lax.fori_loop(0, 2, token_set, 0)
            return carry

        def first_weight(fi, start, stop, mi, carry):
            n = base + nu + fi * nm + mi
            lhs = h_cat[:, cols(mi, part)]
            make(
                n,
                mm(lhs, du_cat[:, cols((1 - core) * nf + fi, width)], 0, 0),
                mm(lhs, du_cat[:, cols(core * nf + fi, width)], 0, 0),
            )

            @pl.when(mi >= 2)
            def _():
                pair_sum(n - 2)

            push(n)
            rounds(ramp(start, stop, mi, nm), ramp(start, stop, mi + 1, nm))
            return carry

        def half_step(fi, carry):
            d0, d1, d2 = (due[k] + fi * (due[k + 2] - due[k]) for k in (1, 2, 3))
            from_i, to_i = fi * 2 * early, 2 * early + fi * (nu - 2 * early)
            lax.fori_loop(from_i, to_i, functools.partial(hidden_chunk, from_i, to_i, d0, d1), 0)
            rounds(d0 + (d1 - d0) * (to_i - from_i) // (2 * early), d1)

            @pl.when(fi == 0)
            def _():
                for k in sets:
                    h_load(layer, k).wait()

            @pl.when(fi == 1)
            def _():
                for k in sets:
                    gb_cat[of(k)] = g[of(k)].astype(BF16)

                @pl.when(layer > 0)
                def _():
                    for load in loads(layer - 1, 0):
                        load.start()

                @pl.when(layer == 0)
                def _():
                    dx_store().start()

            lax.fori_loop(0, nm, functools.partial(first_weight, fi, d1, d2), 0)
            pair_sum(base + nu + fi * nm + nm - 2)
            pair_sum(base + nu + fi * nm + nm - 1)
            return carry

        lax.fori_loop(0, nf, half_step, 0)
        return carry

    lax.fori_loop(0, layers, layer_step, 0)
    rounds(4 * nu * (layers - 1) + PACE[4] * nu // 10, pieces + 4 * LAG)
    dx_store().wait()


def backward(w_one, w_two, us, as_, hs, dys, rows):
    layers, width, wide = w_one.shape
    tokens = dys[0].shape[0]
    half = wide // 2
    nu = half // rows
    chunk = wide // nu
    units = 2 * nu * layers
    dma, reg = pltpu.SemaphoreType.DMA, pltpu.SemaphoreType.REGULAR
    hbm = pl.BlockSpec(memory_space=pl.ANY)
    sub, narrow = rows // 8, width // 2
    shape = jax.ShapeDtypeStruct
    scratch = [
        pltpu.VMEM((2 * tokens, half), BF16),
        pltpu.VMEM((2 * tokens, wide), BF16),
        pltpu.VMEM((2 * tokens, width // 2), BF16),
        pltpu.VMEM((2 * tokens, width), BF16),
        pltpu.VMEM((2 * tokens, width), F32),
        pltpu.VMEM((2, chunk, width), BF16),
        pltpu.VMEM((2, width, chunk), BF16),
        pltpu.VMEM((2, 2, tokens, chunk), BF16),
        pltpu.VMEM((SLOTS, 4, sub, narrow), BF16),
        pltpu.VMEM((PARTS, 4, sub, width), BF16),
        pltpu.VMEM((RECV0, 4, sub, width), BF16),
        pltpu.VMEM((RECV, 2, sub, narrow), BF16),
        pltpu.VMEM((RECV, 1, sub, narrow), BF16),
        *[dma((SEMS,))] * 11,
        *[dma((RECV,))] * 2,
        *[reg((RECV,))] * 2,
        dma((PARTS,)), dma((RECV0,)), reg((RECV0,)),
        dma((2,)), dma((2,)), dma((2,)), dma((2,)), dma((2,)), dma((2, 2)), dma,
    ]
    return pl.pallas_call(
        functools.partial(backward_body, layers=layers, tokens=tokens, width=width, wide=wide, rows=rows),
        out_shape=[
            shape((2 * units - 2 * nu, 2, 8, sub, narrow), BF16),
            shape((tokens, width), BF16),
            shape((2 * nu, sub, narrow), BF16),
        ],
        in_specs=[hbm] * 10,
        out_specs=[hbm] * 3,
        scratch_shapes=scratch,
        compiler_params=pltpu.CompilerParams(collective_id=0, has_side_effects=True, vmem_limit_bytes=VMEM_LIMIT),
        name="backward",
    )(w_one, w_two, *us, *as_, *hs, *dys)


COPY_SLOTS, COPY_LEAD = 40, 16


def assemble_body(tot, dx_in, one, two, dx, buf, dx_buf, s_in, s_out, s_dx, *, layers, nu, nm, width):
    items = 2 * tot.shape[0]
    narrow = width // 2

    def load(j):
        return pltpu.make_async_copy(tot.at[j // 2, j % 2], buf.at[j % COPY_SLOTS], s_in.at[j % COPY_SLOTS])

    def stores(j, run):
        m, core, slot = j // 2, j % 2, j % COPY_SLOTS
        n, side = m // 2, m % 2
        layer, i = layers - 1 - n // (2 * nu), n % nu
        mid = (m % 3) // 2
        for q in range(4):
            src = (1 - mid) * q + mid * (q % 2 * 2 + q // 2)
            span = buf.at[slot, pl.ds(src * 2, 2)]

            @pl.when((n // nu) % 2 == 0)
            def _():
                cols = pl.ds(pl.multiple_of(side * narrow, 128), narrow)
                run(pltpu.make_async_copy(span, two.at[layer, core * nu + i, pl.ds(2 * q, 2), :, cols], s_out.at[slot, q]))

            @pl.when((n // nu) % 2 == 1)
            def _():
                cols = pl.ds(pl.multiple_of((core * (nu // nm) + i // nm) * width + side * narrow, 128), narrow)
                run(pltpu.make_async_copy(span, one.at[layer, i % nm, pl.ds(2 * q, 2), :, cols], s_out.at[slot, q]))

    def step(j, carry):
        @pl.when(j >= COPY_SLOTS)
        def _():
            stores(j - COPY_SLOTS, lambda c: c.wait())

        @pl.when(j < items)
        def _():
            load(j).start()

        @pl.when(jnp.logical_and(j >= COPY_LEAD, j < items + COPY_LEAD))
        def _():
            load(j - COPY_LEAD).wait()
            stores(j - COPY_LEAD, lambda c: c.start())

        return carry

    dx_load = pltpu.make_async_copy(dx_in, dx_buf, s_dx.at[0])
    dx_store = pltpu.make_async_copy(dx_buf, dx, s_dx.at[1])
    dx_load.start()
    lax.fori_loop(0, COPY_SLOTS, step, 0)
    dx_load.wait()
    dx_store.start()
    lax.fori_loop(COPY_SLOTS, items + COPY_SLOTS, step, 0)
    dx_store.wait()


def finish_body(last, one_in, one, buf, s_in, s_out, *, nm, width, first):
    devices, count = last.shape[:2]
    narrow = width // 2

    def load(d):
        return pltpu.make_async_copy(last.at[d], buf.at[d], s_in.at[d])

    def store(d, p):
        m = first + p
        z, y, x, core = d // 8, d // 4 % 2, d // 2 % 2, d % 2
        mid = (m % 3) // 2
        a_axis = (1 - mid) * (m % 3) + mid * ((m // 3) % 2)
        row = 4 * z + 2 * (x + a_axis * (y - x)) + y + a_axis * (x - y)
        i, side = p // 2, p % 2
        cols = pl.ds(pl.multiple_of((core * 2 + i // nm) * width + side * narrow, 128), narrow)
        return pltpu.make_async_copy(buf.at[d, p], one.at[0, i % nm, row, :, cols], s_out)

    for d in range(devices):
        load(d).start()

    def out(d, carry):
        load(d).wait()
        for p in range(count):
            store(d, p).start()
        return carry

    lax.fori_loop(0, devices, out, 0)

    def done(d, carry):
        for p in range(count):
            store(d, p).wait()
        return carry

    lax.fori_loop(0, devices, done, 0)


def assemble(tot, dx, layers, width, wide, rows):
    nu, nm, sub = wide // 2 // rows, width // rows, rows // 8
    shape = jax.ShapeDtypeStruct
    hbm = pl.BlockSpec(memory_space=pl.ANY)
    return pl.pallas_call(
        functools.partial(assemble_body, layers=layers, nu=nu, nm=nm, width=width),
        out_shape=[shape((layers, nm, 8, sub, wide), BF16), shape((layers, 2 * nu, 8, sub, width), BF16), shape(dx.shape, BF16)],
        in_specs=[hbm] * 2,
        out_specs=[hbm] * 3,
        scratch_shapes=[
            pltpu.VMEM((COPY_SLOTS, 8, sub, width // 2), BF16),
            pltpu.VMEM(dx.shape, BF16),
            pltpu.SemaphoreType.DMA((COPY_SLOTS,)),
            pltpu.SemaphoreType.DMA((COPY_SLOTS, 4)),
            pltpu.SemaphoreType.DMA((2,)),
        ],
        compiler_params=pltpu.CompilerParams(vmem_limit_bytes=VMEM_LIMIT),
        cost_estimate=pl.CostEstimate(flops=400 * tot.size, bytes_accessed=4 * tot.size, transcendentals=0),
        name="assemble",
    )(tot, dx)


def finish(last, one, first, nm, width):
    hbm = pl.BlockSpec(memory_space=pl.ANY)
    return pl.pallas_call(
        functools.partial(finish_body, nm=nm, width=width, first=first),
        out_shape=jax.ShapeDtypeStruct(one.shape, BF16),
        in_specs=[hbm] * 2,
        out_specs=hbm,
        scratch_shapes=[pltpu.VMEM(last.shape, BF16), pltpu.SemaphoreType.DMA((last.shape[0],)), pltpu.SemaphoreType.DMA],
        input_output_aliases={1: 0},
        compiler_params=pltpu.CompilerParams(vmem_limit_bytes=VMEM_LIMIT),
        cost_estimate=pl.CostEstimate(flops=400 * last.size, bytes_accessed=4 * last.size, transcendentals=0),
        name="finish",
    )(last, one)


def solution(mesh, rows=UNIT_ROWS):
    batch_spec = P(AXES)

    def per_device(w_one, w_two, x_loc, dy_loc):
        layers, width, wide = w_one.shape
        x = x_loc.reshape(-1, width)
        dy = dy_loc.reshape(-1, width)
        swap = [(0, 1), (1, 0)]
        x_nbr = lax.ppermute(x, "replica", swap)
        dy_nbr = lax.ppermute(dy, "replica", swap)
        z = jnp.full((1,), lax.axis_index("replica"), jnp.int32)
        kept = [forward(z, tokens, w_one, w_two, rows) for tokens in (x, x_nbr)]
        us, as_, hs = zip(*kept)
        tot, dx, last = backward(w_one, w_two, us, as_, hs, (dy, dy_nbr), rows)
        everyone = lax.all_gather(last, AXES)
        one, two, dx = assemble(tot, dx, layers, width, wide, rows)
        one = finish(everyone, one, tot.shape[0], width // rows, width)
        return one.reshape(w_one.shape), two.reshape(w_two.shape), dx.reshape(x_loc.shape)

    return jax.shard_map(per_device, mesh=mesh, in_specs=(P(), P(), batch_spec, batch_spec), out_specs=(P(), P(), batch_spec), check_vma=False)
```

```python
import functools

import jax
import jax.numpy as jnp
from jax import lax
from jax.experimental import pallas as pl
from jax.experimental.pallas import tpu as pltpu
from jax.sharding import PartitionSpec as P

AXES = ("replica", "data")
MESH = pl.DeviceIdType.MESH
BF16, F32 = jnp.bfloat16, jnp.float32
VMEM_LIMIT = 67_043_328
C0, C1 = 0.7978845608028654, 0.044715
UNIT_ROWS = 256
LAG = 3
SLOTS, SEMS, RECV, PARTS, RECV0 = 44, 12, 10, 3, 4
PACE_FIRST, PACE = (6, 18, 20, 28, 30), (-2, 12, 16, 26, 30)
X, Y, Z = 0, 1, 2


def gelu(v):
    half = 0.5 * v
    return half + half * jnp.tanh(v * (C0 + C0 * C1 * (v * v)))


def gelu_slope(v):
    sq = v * v
    t = jnp.tanh(v * (C0 + C0 * C1 * sq))
    return 0.5 + 0.5 * t + v * (1.0 - t * t) * (0.5 * C0 + 1.5 * C0 * C1 * sq)


def mm(lhs, rhs, lhs_dim, rhs_dim):
    return lax.dot_general(lhs, rhs, (((lhs_dim,), (rhs_dim,)), ((), ())), preferred_element_type=F32)


def forward_body(
    x_ref, x, dy, w1_ref, w2_ref, u_ref, a_ref, h_ref, x_nbr, dy_nbr, hid, acc, act_s, nxt, s_send, s_recv, s_load, *, layers, chunks, rows
):
    tokens_of, layer, j = pl.program_id(0), pl.program_id(1), pl.program_id(2)
    z = lax.axis_index("replica")
    part = rows // 2
    shift = z * part
    other = (1 - z, lax.axis_index("data"))

    def swap(k):
        src, dst = ((x, x_nbr), (dy, dy_nbr))[k]
        return pltpu.make_async_remote_copy(
            src_ref=src, dst_ref=dst, send_sem=s_send.at[k], recv_sem=s_recv.at[k], device_id=other, device_id_type=MESH
        )

    next_load = pltpu.make_async_copy(x_nbr, nxt, s_load)
    begins = jnp.logical_and(layer == 0, j == 0)

    @pl.when(jnp.logical_and(tokens_of == 0, begins))
    def _():
        barrier = pltpu.get_barrier_semaphore()
        pl.semaphore_signal(barrier, inc=1, device_id=other, device_id_type=MESH)
        hid[...] = x_ref[...]
        pl.semaphore_wait(barrier, 1)
        for k in range(2):
            swap(k).start()

    @pl.when(jnp.logical_and(tokens_of == 0, jnp.logical_and(layer == layers - 1, j == 0)))
    def _():
        swap(0).wait()
        next_load.start()

    @pl.when(jnp.logical_and(tokens_of == 1, begins))
    def _():
        next_load.wait()
        hid[...] = nxt[...]

    @pl.when(jnp.logical_and(tokens_of == 1, jnp.logical_and(layer == layers - 1, j == chunks - 1)))
    def _():
        swap(1).wait()

    def keep(dst, src):
        for k in range(src.shape[1] // rows):
            dst[0, 0, :, k * part : (k + 1) * part] = src[:, pl.ds(pl.multiple_of(k * rows + shift, part), part)]

    @pl.when(j == 0)
    def _():
        keep(h_ref, hid)
        acc[...] = hid[...].astype(F32)

    def up():
        pre = mm(hid[...], w1_ref[0], 1, 0).astype(BF16)
        u_ref[0, 0] = pre
        act = gelu(pre.astype(F32)).astype(BF16)
        act_s[...] = act
        keep(a_ref, act_s)
        return act

    @pl.when(layer < layers - 1)
    def _():
        acc[...] += mm(up(), w2_ref[0], 1, 0)

        @pl.when(j == chunks - 1)
        def _():
            hid[...] = acc[...].astype(BF16)

    @pl.when(layer == layers - 1)
    def _():
        up()


def forward(x, dy, w_one, w_two, rows):
    layers, width, wide = w_one.shape
    tokens = x.shape[0]
    chunk = width
    chunks = wide // chunk
    shape = jax.ShapeDtypeStruct
    hbm = pl.BlockSpec(memory_space=pl.ANY)
    dma = pltpu.SemaphoreType.DMA
    return pl.pallas_call(
        functools.partial(forward_body, layers=layers, chunks=chunks, rows=rows),
        grid=(2, layers, chunks),
        out_shape=[
            shape((2, layers, tokens, wide), BF16),
            shape((2, layers, tokens, wide // 2), BF16),
            shape((2, layers, tokens, width // 2), BF16),
            shape(x.shape, BF16),
            shape(x.shape, BF16),
        ],
        in_specs=[
            pl.BlockSpec((tokens, width), lambda s, l, j: (0, 0)),
            hbm,
            hbm,
            pl.BlockSpec((1, width, chunk), lambda s, l, j: (l, 0, j)),
            pl.BlockSpec((1, chunk, width), lambda s, l, j: (l, j, 0)),
        ],
        out_specs=[
            pl.BlockSpec((1, 1, tokens, chunk), lambda s, l, j: (s, l, 0, j)),
            pl.BlockSpec((1, 1, tokens, chunk // 2), lambda s, l, j: (s, l, 0, j)),
            pl.BlockSpec((1, 1, tokens, width // 2), lambda s, l, j: (s, l, 0, 0)),
            hbm,
            hbm,
        ],
        scratch_shapes=[
            pltpu.VMEM((tokens, width), BF16),
            pltpu.VMEM((tokens, width), F32),
            pltpu.VMEM((tokens, chunk), BF16),
            pltpu.VMEM((tokens, width), BF16),
            dma((2,)),
            dma((2,)),
            dma,
        ],
        compiler_params=pltpu.CompilerParams(
            collective_id=1, has_side_effects=True, vmem_limit_bytes=VMEM_LIMIT
        ),
        name="forward",
    )(x, x, dy, w_one, w_two)


def backward_body(
    w1, w2, u, a, h, dy_own, dy_nbr,
    tot, dx, last,
    a_cat, du_cat, h_cat, gb_cat, g, w2c, w1c, uc, unit, part0, rcv0, rcv1, rcv2,
    s_rs1, s_rs2, s_ag1, s_ag2, s_ag3, s_fwd, s_own, r_ag1, r_ag2, r_ag3, r_fwd,
    r_rs1, r_rs2, c_rs1, c_rs2, s_rs0, r_rs0, c_rs0,
    l_a, l_gb, l_h, l_w2, l_w1, l_u, l_dx,
    *, layers, tokens, width, wide, rows,
):
    half = wide // 2
    part = rows // 2
    nu = half // rows
    hn = nu // 2
    nm = width // rows
    nf = nu // nm
    chunk = wide // nu
    units = 2 * nu * layers
    pieces = 2 * units
    whole = pieces - 2 * nu
    early = (hn + 1) // 2
    narrow = width // 2
    step = tokens // 2
    z, rest = lax.axis_index("replica"), lax.axis_index("data")
    core, x, y = rest % 2, (rest // 2) % 2, rest // 4

    def choose(axis):
        return (1 - axis) * (2 - axis) // 2, axis * (2 - axis), axis * (axis - 1) // 2

    def peer(axis):
        ex, ey, ez = choose(axis)
        px, py, pz = x + ex * (1 - 2 * x), y + ey * (1 - 2 * y), z + ez * (1 - 2 * z)
        return (pz, (py * 2 + px) * 2 + core)

    sibling = (z, (y * 2 + x) * 2 + 1 - core)

    def send(src, dst, ssem, rsem, to):
        return pltpu.make_async_remote_copy(src_ref=src, dst_ref=dst, send_sem=ssem, recv_sem=rsem, device_id=to, device_id_type=MESH)

    def place(m):
        mid = (m % 3) // 2
        a_axis = (1 - mid) * (m % 3) + mid * ((m // 3) % 2)
        b_axis = 1 - a_axis
        bit_a = x + a_axis * (y - x)
        bit_b = x + b_axis * (y - x)
        own = (1 - mid) * (4 * z + 2 * bit_a + bit_b) + mid * (4 * bit_a + 2 * z + bit_b)
        return mid, a_axis, b_axis, bit_a, bit_b, own

    def rs0(n):
        return send(part0.at[n % PARTS], rcv0.at[n % RECV0], s_rs0.at[n % PARTS], r_rs0.at[n % RECV0], sibling)

    def rs1(m):
        mid, a_axis, b_axis, bit_a, bit_b, own = place(m)
        return send(unit.at[m % SLOTS, pl.ds(2 - 2 * bit_a, 2)], rcv1.at[m % RECV], s_rs1.at[m % SEMS], r_rs1.at[m % RECV], peer(a_axis))

    def rs2(m):
        mid, a_axis, b_axis, bit_a, bit_b, own = place(m)
        return send(unit.at[m % SLOTS, pl.ds(2 * bit_a + 1 - bit_b, 1)], rcv2.at[m % RECV], s_rs2.at[m % SEMS], r_rs2.at[m % RECV], peer(b_axis))

    def own_copy(m):
        mid, a_axis, b_axis, bit_a, bit_b, own = place(m)
        return pltpu.make_async_copy(unit.at[m % SLOTS, pl.ds(2 * bit_a + bit_b, 1)], tot.at[m, core, pl.ds(own, 1)], s_own.at[m % SEMS])

    def last_copy(m):
        mid, a_axis, b_axis, bit_a, bit_b, own = place(m)
        return pltpu.make_async_copy(unit.at[m % SLOTS, pl.ds(2 * bit_a + bit_b, 1)], last.at[pl.ds(m - whole, 1)], s_own.at[m % SEMS])

    def ag1(m):
        mid, a_axis, b_axis, bit_a, bit_b, own = place(m)
        return send(
            unit.at[m % SLOTS, pl.ds(2 * bit_a + bit_b, 1)], tot.at[m, core, pl.ds(own, 1)], s_ag1.at[m % SEMS], r_ag1.at[m % SEMS], peer(b_axis)
        )

    def ag2(m):
        mid, a_axis, b_axis, bit_a, bit_b, own = place(m)
        span = tot.at[m, core, pl.ds(own // 2 * 2, 2)]
        return send(span, span, s_ag2.at[m % SEMS], r_ag2.at[m % SEMS], peer(a_axis + mid * (Z - a_axis)))

    def ag3(m):
        mid, a_axis, b_axis, bit_a, bit_b, own = place(m)
        span = tot.at[m, core, pl.ds(own // 4 * 4, 4)]
        return send(span, span, s_ag3.at[m % SEMS], r_ag3.at[m % SEMS], peer(Z + mid * (a_axis - Z)))

    def fwd(m):
        span = tot.at[m, core]
        return send(span, span, s_fwd.at[m % SEMS], r_fwd.at[m % SEMS], sibling)

    def add(m, block, other):
        unit[m % SLOTS, block] = (unit[m % SLOTS, block].astype(F32) + other.astype(F32)).astype(BF16)

    def credit(sem, n, slots, count, to):
        @pl.when(n + slots < count)
        def _():
            pl.semaphore_signal(sem.at[n % slots], inc=1, device_id=to, device_id_type=MESH)

    def spend(sem, n, slots):
        @pl.when(n >= slots)
        def _():
            pl.semaphore_wait(sem.at[n % slots], 1)

    def live(m):
        return jnp.logical_and(m >= 0, m < pieces)

    def spread_out(m):
        return jnp.logical_and(m >= 0, m < whole)

    def left(m):
        return jnp.logical_and(m >= whole, m < pieces)

    def make(n, theirs, mine):
        part0[n % PARTS] = theirs.reshape(4, rows // 8, width).astype(BF16)
        kept = mine.reshape(4, rows // 8, width).astype(BF16)
        for c in range(2):
            unit[(2 * n + c) % SLOTS] = kept[:, :, c * narrow : (c + 1) * narrow]

    def push(n):
        spend(c_rs0, n, RECV0)
        rs0(n).start()

    def pair_sum(n):
        rs0(n).wait()
        for c in range(2):
            for block in range(4):
                add(2 * n + c, block, rcv0[n % RECV0, block, :, c * narrow : (c + 1) * narrow])
        credit(c_rs0, n, RECV0, units, sibling)

    def comm(r, carry):
        m0, m1, m2, m3, m4, m5 = (r - k * LAG for k in range(6))
        m6 = m5 - LAG

        @pl.when(live(m2))
        def _():
            mid, a_axis, b_axis, bit_a, bit_b, own = place(m2)
            rs2(m2).wait_recv()
            add(m2, 2 * bit_a + bit_b, rcv2[m2 % RECV, 0])
            credit(c_rs2, m2, RECV, pieces, peer(b_axis))
            rs1(m2).wait_send()

        @pl.when(live(m1))
        def _():
            mid, a_axis, b_axis, bit_a, bit_b, own = place(m1)
            rs1(m1).wait_recv()
            add(m1, 2 * bit_a + 1 - bit_b, rcv1[m1 % RECV, 1 - bit_b])
            add(m1, 2 * bit_a + bit_b, rcv1[m1 % RECV, bit_b])
            credit(c_rs1, m1, RECV, pieces, peer(a_axis))

        @pl.when(live(m0))
        def _():
            spend(c_rs1, m0, RECV)
            rs1(m0).start()

        @pl.when(spread_out(m2))
        def _():
            own_copy(m2).start()
            ag1(m2).start()

        @pl.when(left(m2))
        def _():
            last_copy(m2).start()

        @pl.when(live(m1))
        def _():
            spend(c_rs2, m1, RECV)
            rs2(m1).start()

        @pl.when(live(m3))
        def _():
            rs2(m3).wait_send()

        @pl.when(left(m3))
        def _():
            last_copy(m3).wait()

        @pl.when(spread_out(m3))
        def _():
            own_copy(m3).wait()
            ag1(m3).wait()
            ag2(m3).start()

        @pl.when(spread_out(m4))
        def _():
            ag2(m4).wait()
            ag3(m4).start()

        @pl.when(spread_out(m5))
        def _():
            ag3(m5).wait()
            fwd(m5).start()

        @pl.when(spread_out(m6))
        def _():
            fwd(m6).wait()

        return carry

    def rounds(lo, hi):
        lax.fori_loop(lo, hi, comm, 0)

    def ramp(lo, hi, i, n):
        return lo + (hi - lo) * i * i // (n * n)

    sets = (0, 1)
    dys = (dy_own, dy_nbr)

    def of(k):
        return pl.ds(k * tokens, tokens)

    def chunk_at(i):
        late, wait = hn - early, i // (2 * early)
        first = i // early * hn + i % early
        second = early + (i - 2 * early) // late * hn + (i - 2 * early) % late
        return first + wait * (second - first)

    def loads(layer, i):
        f0, slot = pl.multiple_of(chunk_at(i) * chunk, 128), i % 2
        return (
            pltpu.make_async_copy(w2.at[layer, pl.ds(f0, chunk)], w2c.at[slot], l_w2.at[slot]),
            pltpu.make_async_copy(w1.at[layer, :, pl.ds(f0, chunk)], w1c.at[slot], l_w1.at[slot]),
            *(pltpu.make_async_copy(u.at[k, layer, :, pl.ds(f0, chunk)], uc.at[slot, k], l_u.at[slot, k]) for k in sets),
        )

    def cols(i, size):
        return pl.ds(pl.multiple_of(i * size, 128), size)

    def a_load(layer, k):
        return pltpu.make_async_copy(a.at[k, layer], a_cat.at[of(k)], l_a.at[k])

    def h_load(layer, k):
        return pltpu.make_async_copy(h.at[k, layer], h_cat.at[of(k)], l_h.at[k])

    def gb_load(k):
        return pltpu.make_async_copy(dys[k], gb_cat.at[of(k)], l_gb.at[k])

    def dx_store():
        return pltpu.make_async_copy(gb_cat.at[of(0)], dx, l_dx)

    barrier = pltpu.get_barrier_semaphore()
    for to in (peer(X), peer(Y), peer(Z), sibling):
        pl.semaphore_signal(barrier, inc=1, device_id=to, device_id_type=MESH)
    for k in sets:
        gb_load(k).start()
        a_load(layers - 1, k).start()
    for k in sets:
        gb_load(k).wait()
    pl.semaphore_wait(barrier, 4)

    def layer_step(li, carry):
        layer = layers - 1 - li
        base = li * 2 * nu
        late = jnp.minimum(li, 1)
        due = [late * (4 * nu * (li - 1) + PACE[4] * nu // 10)]
        for p, q in zip(PACE_FIRST, PACE):
            due.append(4 * nu * li + p * nu // 10 + late * (q * nu // 10 - p * nu // 10))
        for k in sets:
            a_load(layer, k).wait()

        def second_weight(i, carry):
            n = base + i
            lhs = jnp.concatenate([a_cat[:, cols((1 - core) * nu + i, part)], a_cat[:, cols(core * nu + i, part)]], axis=1)
            out = mm(lhs, gb_cat[...], 0, 0)
            make(n, out[:part], out[part:])

            @pl.when(i >= 2)
            def _():
                pair_sum(n - 2)

            push(n)
            rounds(ramp(due[0], due[1], i, nu), ramp(due[0], due[1], i + 1, nu))
            return carry

        lax.fori_loop(0, nu, second_weight, 0)
        pair_sum(base + nu - 2)
        pair_sum(base + nu - 1)
        for k in sets:
            h_load(layer, k).start()

        @pl.when(li == 0)
        def _():
            for load in loads(layer, 0):
                load.start()
            for k in sets:
                g[of(k)] = gb_cat[of(k)].astype(F32)

        @pl.when(layer > 0)
        def _():
            for k in sets:
                a_load(layer - 1, k).start()

        def hidden_chunk(from_i, to_i, start, stop, i, carry):
            for load in loads(layer, i):
                load.wait()

            @pl.when(i < nu - 1)
            def _():
                for load in loads(layer, i + 1):
                    load.start()

            def token_set(k, carry):
                at = [pl.ds(q * step, step) for q in range(2)]
                rows_q = [pl.ds(pl.multiple_of(k * tokens + q * step, 16), step) for q in range(2)]
                d_act = [mm(gb_cat[r], w2c[i % 2], 1, 1) for r in rows_q]
                for q in range(2):
                    du = (d_act[q] * gelu_slope(uc[i % 2, k, at[q]].astype(F32))).astype(BF16)
                    du_cat[rows_q[q], cols(chunk_at(i), chunk)] = du
                    g[rows_q[q]] += mm(du, w1c[i % 2], 1, 1)
                s = 2 * (i - from_i) + k
                rounds(start + (stop - start) * s // (4 * early), start + (stop - start) * (s + 1) // (4 * early))
                return carry

            lax.fori_loop(0, 2, token_set, 0)
            return carry

        def first_weight(fi, start, stop, mi, carry):
            n = base + nu + fi * nm + mi
            lhs = h_cat[:, cols(mi, part)]
            make(
                n,
                mm(lhs, du_cat[:, cols((1 - core) * nf + fi, width)], 0, 0),
                mm(lhs, du_cat[:, cols(core * nf + fi, width)], 0, 0),
            )

            @pl.when(mi >= 2)
            def _():
                pair_sum(n - 2)

            push(n)
            rounds(ramp(start, stop, mi, nm), ramp(start, stop, mi + 1, nm))
            return carry

        def half_step(fi, carry):
            d0, d1, d2 = (due[k] + fi * (due[k + 2] - due[k]) for k in (1, 2, 3))
            from_i, to_i = fi * 2 * early, 2 * early + fi * (nu - 2 * early)
            lax.fori_loop(from_i, to_i, functools.partial(hidden_chunk, from_i, to_i, d0, d1), 0)
            rounds(d0 + (d1 - d0) * (to_i - from_i) // (2 * early), d1)

            @pl.when(fi == 0)
            def _():
                for k in sets:
                    h_load(layer, k).wait()

            @pl.when(fi == 1)
            def _():
                for k in sets:
                    gb_cat[of(k)] = g[of(k)].astype(BF16)

                @pl.when(layer > 0)
                def _():
                    for load in loads(layer - 1, 0):
                        load.start()

                @pl.when(layer == 0)
                def _():
                    dx_store().start()

            lax.fori_loop(0, nm, functools.partial(first_weight, fi, d1, d2), 0)
            pair_sum(base + nu + fi * nm + nm - 2)
            pair_sum(base + nu + fi * nm + nm - 1)
            return carry

        lax.fori_loop(0, nf, half_step, 0)
        return carry

    lax.fori_loop(0, layers, layer_step, 0)
    rounds(4 * nu * (layers - 1) + PACE[4] * nu // 10, pieces + 4 * LAG)
    dx_store().wait()


def backward(w_one, w_two, u, a, h, dy, dy_nbr, rows):
    layers, width, wide = w_one.shape
    tokens = dy.shape[0]
    half = wide // 2
    nu = half // rows
    chunk = wide // nu
    units = 2 * nu * layers
    dma, reg = pltpu.SemaphoreType.DMA, pltpu.SemaphoreType.REGULAR
    hbm = pl.BlockSpec(memory_space=pl.ANY)
    sub, narrow = rows // 8, width // 2
    shape = jax.ShapeDtypeStruct
    scratch = [
        pltpu.VMEM((2 * tokens, half), BF16),
        pltpu.VMEM((2 * tokens, wide), BF16),
        pltpu.VMEM((2 * tokens, width // 2), BF16),
        pltpu.VMEM((2 * tokens, width), BF16),
        pltpu.VMEM((2 * tokens, width), F32),
        pltpu.VMEM((2, chunk, width), BF16),
        pltpu.VMEM((2, width, chunk), BF16),
        pltpu.VMEM((2, 2, tokens, chunk), BF16),
        pltpu.VMEM((SLOTS, 4, sub, narrow), BF16),
        pltpu.VMEM((PARTS, 4, sub, width), BF16),
        pltpu.VMEM((RECV0, 4, sub, width), BF16),
        pltpu.VMEM((RECV, 2, sub, narrow), BF16),
        pltpu.VMEM((RECV, 1, sub, narrow), BF16),
        *[dma((SEMS,))] * 11,
        *[dma((RECV,))] * 2,
        *[reg((RECV,))] * 2,
        dma((PARTS,)), dma((RECV0,)), reg((RECV0,)),
        dma((2,)), dma((2,)), dma((2,)), dma((2,)), dma((2,)), dma((2, 2)), dma,
    ]
    return pl.pallas_call(
        functools.partial(backward_body, layers=layers, tokens=tokens, width=width, wide=wide, rows=rows),
        out_shape=[
            shape((2 * units - 2 * nu, 2, 8, sub, narrow), BF16),
            shape((tokens, width), BF16),
            shape((2 * nu, sub, narrow), BF16),
        ],
        in_specs=[hbm] * 7,
        out_specs=[hbm] * 3,
        scratch_shapes=scratch,
        compiler_params=pltpu.CompilerParams(collective_id=0, has_side_effects=True, vmem_limit_bytes=VMEM_LIMIT),
        name="backward",
    )(w_one, w_two, u, a, h, dy, dy_nbr)


COPY_SLOTS, COPY_LEAD = 40, 16


def assemble_body(tot, dx_in, one, two, dx, buf, dx_buf, s_in, s_out, s_dx, *, layers, nu, nm, width):
    items = 2 * tot.shape[0]
    narrow = width // 2

    def load(j):
        return pltpu.make_async_copy(tot.at[j // 2, j % 2], buf.at[j % COPY_SLOTS], s_in.at[j % COPY_SLOTS])

    def stores(j, run):
        m, core, slot = j // 2, j % 2, j % COPY_SLOTS
        n, side = m // 2, m % 2
        layer, i = layers - 1 - n // (2 * nu), n % nu
        mid = (m % 3) // 2
        for q in range(4):
            src = (1 - mid) * q + mid * (q % 2 * 2 + q // 2)
            span = buf.at[slot, pl.ds(src * 2, 2)]

            @pl.when((n // nu) % 2 == 0)
            def _():
                cols = pl.ds(pl.multiple_of(side * narrow, 128), narrow)
                run(pltpu.make_async_copy(span, two.at[layer, core * nu + i, pl.ds(2 * q, 2), :, cols], s_out.at[slot, q]))

            @pl.when((n // nu) % 2 == 1)
            def _():
                cols = pl.ds(pl.multiple_of((core * (nu // nm) + i // nm) * width + side * narrow, 128), narrow)
                run(pltpu.make_async_copy(span, one.at[layer, i % nm, pl.ds(2 * q, 2), :, cols], s_out.at[slot, q]))

    def step(j, carry):
        @pl.when(j >= COPY_SLOTS)
        def _():
            stores(j - COPY_SLOTS, lambda c: c.wait())

        @pl.when(j < items)
        def _():
            load(j).start()

        @pl.when(jnp.logical_and(j >= COPY_LEAD, j < items + COPY_LEAD))
        def _():
            load(j - COPY_LEAD).wait()
            stores(j - COPY_LEAD, lambda c: c.start())

        return carry

    dx_load = pltpu.make_async_copy(dx_in, dx_buf, s_dx.at[0])
    dx_store = pltpu.make_async_copy(dx_buf, dx, s_dx.at[1])
    dx_load.start()
    lax.fori_loop(0, COPY_SLOTS, step, 0)
    dx_load.wait()
    dx_store.start()
    lax.fori_loop(COPY_SLOTS, items + COPY_SLOTS, step, 0)
    dx_store.wait()


def finish_body(last, one_in, one, buf, s_in, s_out, *, nm, width, first):
    devices, count = last.shape[:2]
    narrow = width // 2

    def load(d):
        return pltpu.make_async_copy(last.at[d], buf.at[d], s_in.at[d])

    def store(d, p):
        m = first + p
        z, y, x, core = d // 8, d // 4 % 2, d // 2 % 2, d % 2
        mid = (m % 3) // 2
        a_axis = (1 - mid) * (m % 3) + mid * ((m // 3) % 2)
        row = 4 * z + 2 * (x + a_axis * (y - x)) + y + a_axis * (x - y)
        i, side = p // 2, p % 2
        cols = pl.ds(pl.multiple_of((core * 2 + i // nm) * width + side * narrow, 128), narrow)
        return pltpu.make_async_copy(buf.at[d, p], one.at[0, i % nm, row, :, cols], s_out)

    for d in range(devices):
        load(d).start()

    def out(d, carry):
        load(d).wait()
        for p in range(count):
            store(d, p).start()
        return carry

    lax.fori_loop(0, devices, out, 0)

    def done(d, carry):
        for p in range(count):
            store(d, p).wait()
        return carry

    lax.fori_loop(0, devices, done, 0)


def assemble(tot, dx, layers, width, wide, rows):
    nu, nm, sub = wide // 2 // rows, width // rows, rows // 8
    shape = jax.ShapeDtypeStruct
    hbm = pl.BlockSpec(memory_space=pl.ANY)
    return pl.pallas_call(
        functools.partial(assemble_body, layers=layers, nu=nu, nm=nm, width=width),
        out_shape=[shape((layers, nm, 8, sub, wide), BF16), shape((layers, 2 * nu, 8, sub, width), BF16), shape(dx.shape, BF16)],
        in_specs=[hbm] * 2,
        out_specs=[hbm] * 3,
        scratch_shapes=[
            pltpu.VMEM((COPY_SLOTS, 8, sub, width // 2), BF16),
            pltpu.VMEM(dx.shape, BF16),
            pltpu.SemaphoreType.DMA((COPY_SLOTS,)),
            pltpu.SemaphoreType.DMA((COPY_SLOTS, 4)),
            pltpu.SemaphoreType.DMA((2,)),
        ],
        compiler_params=pltpu.CompilerParams(vmem_limit_bytes=VMEM_LIMIT),
        cost_estimate=pl.CostEstimate(flops=400 * tot.size, bytes_accessed=4 * tot.size, transcendentals=0),
        name="assemble",
    )(tot, dx)


def finish(last, one, first, nm, width):
    hbm = pl.BlockSpec(memory_space=pl.ANY)
    return pl.pallas_call(
        functools.partial(finish_body, nm=nm, width=width, first=first),
        out_shape=jax.ShapeDtypeStruct(one.shape, BF16),
        in_specs=[hbm] * 2,
        out_specs=hbm,
        scratch_shapes=[pltpu.VMEM(last.shape, BF16), pltpu.SemaphoreType.DMA((last.shape[0],)), pltpu.SemaphoreType.DMA],
        input_output_aliases={1: 0},
        compiler_params=pltpu.CompilerParams(vmem_limit_bytes=VMEM_LIMIT),
        cost_estimate=pl.CostEstimate(flops=400 * last.size, bytes_accessed=4 * last.size, transcendentals=0),
        name="finish",
    )(last, one)


def solution(mesh, rows=UNIT_ROWS):
    batch_spec = P(AXES)

    def per_device(w_one, w_two, x_loc, dy_loc):
        layers, width, wide = w_one.shape
        x = x_loc.reshape(-1, width)
        dy = dy_loc.reshape(-1, width)
        u, a, h, _, dy_nbr = forward(x, dy, w_one, w_two, rows)
        tot, dx, last = backward(w_one, w_two, u, a, h, dy, dy_nbr, rows)
        everyone = lax.all_gather(last, AXES)
        one, two, dx = assemble(tot, dx, layers, width, wide, rows)
        one = finish(everyone, one, tot.shape[0], width // rows, width)
        return one.reshape(w_one.shape), two.reshape(w_two.shape), dx.reshape(x_loc.shape)

    return jax.shard_map(per_device, mesh=mesh, in_specs=(P(), P(), batch_spec, batch_spec), out_specs=(P(), P(), batch_spec), check_vma=False)
```

```python
import functools

import jax
import jax.numpy as jnp
from jax import lax
from jax.experimental import pallas as pl
from jax.experimental.pallas import tpu as pltpu
from jax.sharding import PartitionSpec as P

AXES = ("replica", "data")
MESH = pl.DeviceIdType.MESH
BF16, F32 = jnp.bfloat16, jnp.float32
VMEM_LIMIT = 67_043_328
C0, C1 = 0.7978845608028654, 0.044715
UNIT_ROWS = 256
LAG = 3
SLOTS, SEMS, RECV, PARTS, RECV0 = 44, 12, 10, 3, 4
PACE_FIRST, PACE = (6, 18, 20, 28, 30), (-2, 12, 16, 26, 30)
X, Y, Z = 0, 1, 2


def gelu(v):
    half = 0.5 * v
    return half + half * jnp.tanh(v * (C0 + C0 * C1 * (v * v)))


def gelu_slope(v):
    sq = v * v
    t = jnp.tanh(v * (C0 + C0 * C1 * sq))
    return 0.5 + 0.5 * t + v * (1.0 - t * t) * (0.5 * C0 + 1.5 * C0 * C1 * sq)


def mm(lhs, rhs, lhs_dim, rhs_dim):
    return lax.dot_general(lhs, rhs, (((lhs_dim,), (rhs_dim,)), ((), ())), preferred_element_type=F32)


def forward_body(
    x_ref, x, dy, w1_ref, w2_ref, u_ref, a_ref, h_ref, x_nbr, dy_nbr, h_nbr,
    hid, acc, act_s, nxt, made, s_send, s_recv, s_load,
    *, layers, chunks, rows,
):
    tokens_of, layer, j = pl.program_id(0), pl.program_id(1), pl.program_id(2)
    z = lax.axis_index("replica")
    part = rows // 2
    shift = z * part
    other = (1 - z, lax.axis_index("data"))
    third = x.shape[0] // 3
    given = layers - 2

    def swap(src, dst, k):
        return pltpu.make_async_remote_copy(
            src_ref=src, dst_ref=dst, send_sem=s_send.at[k], recv_sem=s_recv.at[k], device_id=other, device_id_type=MESH
        )

    x_swap = swap(x, x_nbr, 0)
    dy_swap = [swap(dy.at[pl.ds(k * third, third)], dy_nbr.at[pl.ds(k * third, third)], 1 + k) for k in range(3)]
    h_swap = [swap(made.at[k], h_nbr.at[k], 4 + k) for k in range(given)]
    x_load = pltpu.make_async_copy(x_nbr, nxt, s_load)
    h_load = [pltpu.make_async_copy(h_nbr.at[k], nxt, s_load) for k in range(given)]

    def at(s, l, c):
        return pl.when(jnp.logical_and(tokens_of == s, jnp.logical_and(layer == l, j == c)))

    @at(0, 0, 0)
    def _():
        barrier = pltpu.get_barrier_semaphore()
        pl.semaphore_signal(barrier, inc=1, device_id=other, device_id_type=MESH)
        hid[...] = x_ref[...]
        pl.semaphore_wait(barrier, 1)
        x_swap.start()
        dy_swap[0].start()

    for k in range(given):

        @at(0, k + 2, 0)
        def _(k=k):
            h_swap[k].start()

        @at(1, k + 1, chunks - 1)
        def _(k=k):
            h_swap[k].wait_recv()
            h_load[k].start()

        @at(1, k + 2, 0)
        def _(k=k):
            h_load[k].wait()
            hid[...] = nxt[...]

    @at(0, layers - 1, 0)
    def _():
        dy_swap[1].start()
        dy_swap[2].start()
        x_swap.wait()
        x_load.start()

    @at(1, 0, 0)
    def _():
        x_load.wait()
        hid[...] = nxt[...]

    @at(1, layers - 1, chunks - 1)
    def _():
        for copy in h_swap:
            copy.wait_send()
        for copy in dy_swap:
            copy.wait()

    def keep(dst, src):
        for k in range(src.shape[1] // rows):
            dst[0, 0, :, k * part : (k + 1) * part] = src[:, pl.ds(pl.multiple_of(k * rows + shift, part), part)]

    @pl.when(j == 0)
    def _():
        keep(h_ref, hid)
        acc[...] = hid[...].astype(F32)

    def up():
        pre = mm(hid[...], w1_ref[0], 1, 0).astype(BF16)
        u_ref[0, 0] = pre
        act = gelu(pre.astype(F32)).astype(BF16)
        act_s[...] = act
        keep(a_ref, act_s)
        return act

    full = layer < layers - 1 - tokens_of * given

    @pl.when(full)
    def _():
        acc[...] += mm(up(), w2_ref[0], 1, 0)

        @pl.when(j == chunks - 1)
        def _():
            hid[...] = acc[...].astype(BF16)

    @pl.when(jnp.logical_not(full))
    def _():
        up()

    for k in range(given):

        @at(0, k + 1, chunks - 1)
        def _(k=k):
            made[k] = hid[...]


def forward(x, dy, w_one, w_two, rows):
    layers, width, wide = w_one.shape
    tokens = x.shape[0]
    chunk = width
    chunks = wide // chunk
    shape = jax.ShapeDtypeStruct
    hbm = pl.BlockSpec(memory_space=pl.ANY)
    dma = pltpu.SemaphoreType.DMA
    return pl.pallas_call(
        functools.partial(forward_body, layers=layers, chunks=chunks, rows=rows),
        grid=(2, layers, chunks),
        out_shape=[
            shape((2, layers, tokens, wide), BF16),
            shape((2, layers, tokens, wide // 2), BF16),
            shape((2, layers, tokens, width // 2), BF16),
            shape(x.shape, BF16),
            shape(x.shape, BF16),
            shape((max(layers - 2, 1), tokens, width), BF16),
        ],
        in_specs=[
            pl.BlockSpec((tokens, width), lambda s, l, j: (0, 0)),
            hbm,
            hbm,
            pl.BlockSpec((1, width, chunk), lambda s, l, j: (l, 0, j)),
            pl.BlockSpec((1, chunk, width), lambda s, l, j: (l, j, 0)),
        ],
        out_specs=[
            pl.BlockSpec((1, 1, tokens, chunk), lambda s, l, j: (s, l, 0, j)),
            pl.BlockSpec((1, 1, tokens, chunk // 2), lambda s, l, j: (s, l, 0, j)),
            pl.BlockSpec((1, 1, tokens, width // 2), lambda s, l, j: (s, l, 0, 0)),
            hbm,
            hbm,
            hbm,
        ],
        scratch_shapes=[
            pltpu.VMEM((tokens, width), BF16),
            pltpu.VMEM((tokens, width), F32),
            pltpu.VMEM((tokens, chunk), BF16),
            pltpu.VMEM((tokens, width), BF16),
            pltpu.VMEM((max(layers - 2, 1), tokens, width), BF16),
            dma((2 + layers,)),
            dma((2 + layers,)),
            dma,
        ],
        compiler_params=pltpu.CompilerParams(
            collective_id=1, has_side_effects=True, vmem_limit_bytes=VMEM_LIMIT
        ),
        name="forward",
    )(x, x, dy, w_one, w_two)


def backward_body(
    w1, w2, u, a, h, dy_own, dy_nbr,
    tot, dx, last,
    a_cat, du_cat, h_cat, gb_cat, g, w2c, w1c, uc, unit, part0, rcv0, rcv1, rcv2,
    s_rs1, s_rs2, s_ag1, s_ag2, s_ag3, s_fwd, s_own, r_ag1, r_ag2, r_ag3, r_fwd,
    r_rs1, r_rs2, c_rs1, c_rs2, s_rs0, r_rs0, c_rs0,
    l_a, l_gb, l_h, l_w2, l_w1, l_u, l_dx,
    *, layers, tokens, width, wide, rows,
):
    half = wide // 2
    part = rows // 2
    nu = half // rows
    hn = nu // 2
    nm = width // rows
    nf = nu // nm
    chunk = wide // nu
    units = 2 * nu * layers
    pieces = 2 * units
    whole = pieces - 2 * nu
    early = (hn + 1) // 2
    narrow = width // 2
    step = tokens // 2
    z, rest = lax.axis_index("replica"), lax.axis_index("data")
    core, x, y = rest % 2, (rest // 2) % 2, rest // 4

    def choose(axis):
        return (1 - axis) * (2 - axis) // 2, axis * (2 - axis), axis * (axis - 1) // 2

    def peer(axis):
        ex, ey, ez = choose(axis)
        px, py, pz = x + ex * (1 - 2 * x), y + ey * (1 - 2 * y), z + ez * (1 - 2 * z)
        return (pz, (py * 2 + px) * 2 + core)

    sibling = (z, (y * 2 + x) * 2 + 1 - core)

    def send(src, dst, ssem, rsem, to):
        return pltpu.make_async_remote_copy(src_ref=src, dst_ref=dst, send_sem=ssem, recv_sem=rsem, device_id=to, device_id_type=MESH)

    def place(m):
        mid = (m % 3) // 2
        a_axis = (1 - mid) * (m % 3) + mid * ((m // 3) % 2)
        b_axis = 1 - a_axis
        bit_a = x + a_axis * (y - x)
        bit_b = x + b_axis * (y - x)
        own = (1 - mid) * (4 * z + 2 * bit_a + bit_b) + mid * (4 * bit_a + 2 * z + bit_b)
        return mid, a_axis, b_axis, bit_a, bit_b, own

    def rs0(n):
        return send(part0.at[n % PARTS], rcv0.at[n % RECV0], s_rs0.at[n % PARTS], r_rs0.at[n % RECV0], sibling)

    def rs1(m):
        mid, a_axis, b_axis, bit_a, bit_b, own = place(m)
        return send(unit.at[m % SLOTS, pl.ds(2 - 2 * bit_a, 2)], rcv1.at[m % RECV], s_rs1.at[m % SEMS], r_rs1.at[m % RECV], peer(a_axis))

    def rs2(m):
        mid, a_axis, b_axis, bit_a, bit_b, own = place(m)
        return send(unit.at[m % SLOTS, pl.ds(2 * bit_a + 1 - bit_b, 1)], rcv2.at[m % RECV], s_rs2.at[m % SEMS], r_rs2.at[m % RECV], peer(b_axis))

    def own_copy(m):
        mid, a_axis, b_axis, bit_a, bit_b, own = place(m)
        return pltpu.make_async_copy(unit.at[m % SLOTS, pl.ds(2 * bit_a + bit_b, 1)], tot.at[m, core, pl.ds(own, 1)], s_own.at[m % SEMS])

    def last_copy(m):
        mid, a_axis, b_axis, bit_a, bit_b, own = place(m)
        return pltpu.make_async_copy(unit.at[m % SLOTS, pl.ds(2 * bit_a + bit_b, 1)], last.at[pl.ds(m - whole, 1)], s_own.at[m % SEMS])

    def ag1(m):
        mid, a_axis, b_axis, bit_a, bit_b, own = place(m)
        return send(
            unit.at[m % SLOTS, pl.ds(2 * bit_a + bit_b, 1)], tot.at[m, core, pl.ds(own, 1)], s_ag1.at[m % SEMS], r_ag1.at[m % SEMS], peer(b_axis)
        )

    def ag2(m):
        mid, a_axis, b_axis, bit_a, bit_b, own = place(m)
        span = tot.at[m, core, pl.ds(own // 2 * 2, 2)]
        return send(span, span, s_ag2.at[m % SEMS], r_ag2.at[m % SEMS], peer(a_axis + mid * (Z - a_axis)))

    def ag3(m):
        mid, a_axis, b_axis, bit_a, bit_b, own = place(m)
        span = tot.at[m, core, pl.ds(own // 4 * 4, 4)]
        return send(span, span, s_ag3.at[m % SEMS], r_ag3.at[m % SEMS], peer(Z + mid * (a_axis - Z)))

    def fwd(m):
        span = tot.at[m, core]
        return send(span, span, s_fwd.at[m % SEMS], r_fwd.at[m % SEMS], sibling)

    def add(m, block, other):
        unit[m % SLOTS, block] = (unit[m % SLOTS, block].astype(F32) + other.astype(F32)).astype(BF16)

    def credit(sem, n, slots, count, to):
        @pl.when(n + slots < count)
        def _():
            pl.semaphore_signal(sem.at[n % slots], inc=1, device_id=to, device_id_type=MESH)

    def spend(sem, n, slots):
        @pl.when(n >= slots)
        def _():
            pl.semaphore_wait(sem.at[n % slots], 1)

    def live(m):
        return jnp.logical_and(m >= 0, m < pieces)

    def spread_out(m):
        return jnp.logical_and(m >= 0, m < whole)

    def left(m):
        return jnp.logical_and(m >= whole, m < pieces)

    def make(n, theirs, mine):
        part0[n % PARTS] = theirs.reshape(4, rows // 8, width).astype(BF16)
        kept = mine.reshape(4, rows // 8, width).astype(BF16)
        for c in range(2):
            unit[(2 * n + c) % SLOTS] = kept[:, :, c * narrow : (c + 1) * narrow]

    def push(n):
        spend(c_rs0, n, RECV0)
        rs0(n).start()

    def pair_sum(n):
        rs0(n).wait()
        for c in range(2):
            for block in range(4):
                add(2 * n + c, block, rcv0[n % RECV0, block, :, c * narrow : (c + 1) * narrow])
        credit(c_rs0, n, RECV0, units, sibling)

    def comm(r, carry):
        m0, m1, m2, m3, m4, m5 = (r - k * LAG for k in range(6))
        m6 = m5 - LAG

        @pl.when(live(m2))
        def _():
            mid, a_axis, b_axis, bit_a, bit_b, own = place(m2)
            rs2(m2).wait_recv()
            add(m2, 2 * bit_a + bit_b, rcv2[m2 % RECV, 0])
            credit(c_rs2, m2, RECV, pieces, peer(b_axis))
            rs1(m2).wait_send()

        @pl.when(live(m1))
        def _():
            mid, a_axis, b_axis, bit_a, bit_b, own = place(m1)
            rs1(m1).wait_recv()
            add(m1, 2 * bit_a + 1 - bit_b, rcv1[m1 % RECV, 1 - bit_b])
            add(m1, 2 * bit_a + bit_b, rcv1[m1 % RECV, bit_b])
            credit(c_rs1, m1, RECV, pieces, peer(a_axis))

        @pl.when(live(m0))
        def _():
            spend(c_rs1, m0, RECV)
            rs1(m0).start()

        @pl.when(spread_out(m2))
        def _():
            own_copy(m2).start()
            ag1(m2).start()

        @pl.when(left(m2))
        def _():
            last_copy(m2).start()

        @pl.when(live(m1))
        def _():
            spend(c_rs2, m1, RECV)
            rs2(m1).start()

        @pl.when(live(m3))
        def _():
            rs2(m3).wait_send()

        @pl.when(left(m3))
        def _():
            last_copy(m3).wait()

        @pl.when(spread_out(m3))
        def _():
            own_copy(m3).wait()
            ag1(m3).wait()
            ag2(m3).start()

        @pl.when(spread_out(m4))
        def _():
            ag2(m4).wait()
            ag3(m4).start()

        @pl.when(spread_out(m5))
        def _():
            ag3(m5).wait()
            fwd(m5).start()

        @pl.when(spread_out(m6))
        def _():
            fwd(m6).wait()

        return carry

    def rounds(lo, hi):
        lax.fori_loop(lo, hi, comm, 0)

    def ramp(lo, hi, i, n):
        return lo + (hi - lo) * i * i // (n * n)

    sets = (0, 1)
    dys = (dy_own, dy_nbr)

    def of(k):
        return pl.ds(k * tokens, tokens)

    def chunk_at(i):
        late, wait = hn - early, i // (2 * early)
        first = i // early * hn + i % early
        second = early + (i - 2 * early) // late * hn + (i - 2 * early) % late
        return first + wait * (second - first)

    def loads(layer, i):
        f0, slot = pl.multiple_of(chunk_at(i) * chunk, 128), i % 2
        return (
            pltpu.make_async_copy(w2.at[layer, pl.ds(f0, chunk)], w2c.at[slot], l_w2.at[slot]),
            pltpu.make_async_copy(w1.at[layer, :, pl.ds(f0, chunk)], w1c.at[slot], l_w1.at[slot]),
            *(pltpu.make_async_copy(u.at[k, layer, :, pl.ds(f0, chunk)], uc.at[slot, k], l_u.at[slot, k]) for k in sets),
        )

    def cols(i, size):
        return pl.ds(pl.multiple_of(i * size, 128), size)

    def a_load(layer, k):
        return pltpu.make_async_copy(a.at[k, layer], a_cat.at[of(k)], l_a.at[k])

    def h_load(layer, k):
        return pltpu.make_async_copy(h.at[k, layer], h_cat.at[of(k)], l_h.at[k])

    def gb_load(k):
        return pltpu.make_async_copy(dys[k], gb_cat.at[of(k)], l_gb.at[k])

    def dx_store():
        return pltpu.make_async_copy(gb_cat.at[of(0)], dx, l_dx)

    barrier = pltpu.get_barrier_semaphore()
    for to in (peer(X), peer(Y), peer(Z), sibling):
        pl.semaphore_signal(barrier, inc=1, device_id=to, device_id_type=MESH)
    for k in sets:
        gb_load(k).start()
        a_load(layers - 1, k).start()
    for k in sets:
        gb_load(k).wait()
    pl.semaphore_wait(barrier, 4)

    def layer_step(li, carry):
        layer = layers - 1 - li
        base = li * 2 * nu
        late = jnp.minimum(li, 1)
        due = [late * (4 * nu * (li - 1) + PACE[4] * nu // 10)]
        for p, q in zip(PACE_FIRST, PACE):
            due.append(4 * nu * li + p * nu // 10 + late * (q * nu // 10 - p * nu // 10))
        for k in sets:
            a_load(layer, k).wait()

        def second_weight(i, carry):
            n = base + i
            lhs = jnp.concatenate([a_cat[:, cols((1 - core) * nu + i, part)], a_cat[:, cols(core * nu + i, part)]], axis=1)
            out = mm(lhs, gb_cat[...], 0, 0)
            make(n, out[:part], out[part:])

            @pl.when(i >= 2)
            def _():
                pair_sum(n - 2)

            push(n)
            rounds(ramp(due[0], due[1], i, nu), ramp(due[0], due[1], i + 1, nu))
            return carry

        lax.fori_loop(0, nu, second_weight, 0)
        pair_sum(base + nu - 2)
        pair_sum(base + nu - 1)
        for k in sets:
            h_load(layer, k).start()

        @pl.when(li == 0)
        def _():
            for load in loads(layer, 0):
                load.start()
            for k in sets:
                g[of(k)] = gb_cat[of(k)].astype(F32)

        @pl.when(layer > 0)
        def _():
            for k in sets:
                a_load(layer - 1, k).start()

        def hidden_chunk(from_i, to_i, start, stop, i, carry):
            for load in loads(layer, i):
                load.wait()

            @pl.when(i < nu - 1)
            def _():
                for load in loads(layer, i + 1):
                    load.start()

            def token_set(k, carry):
                at = [pl.ds(q * step, step) for q in range(2)]
                rows_q = [pl.ds(pl.multiple_of(k * tokens + q * step, 16), step) for q in range(2)]
                d_act = [mm(gb_cat[r], w2c[i % 2], 1, 1) for r in rows_q]
                for q in range(2):
                    du = (d_act[q] * gelu_slope(uc[i % 2, k, at[q]].astype(F32))).astype(BF16)
                    du_cat[rows_q[q], cols(chunk_at(i), chunk)] = du
                    g[rows_q[q]] += mm(du, w1c[i % 2], 1, 1)
                s = 2 * (i - from_i) + k
                rounds(start + (stop - start) * s // (4 * early), start + (stop - start) * (s + 1) // (4 * early))
                return carry

            lax.fori_loop(0, 2, token_set, 0)
            return carry

        def first_weight(fi, start, stop, mi, carry):
            n = base + nu + fi * nm + mi
            lhs = h_cat[:, cols(mi, part)]
            make(
                n,
                mm(lhs, du_cat[:, cols((1 - core) * nf + fi, width)], 0, 0),
                mm(lhs, du_cat[:, cols(core * nf + fi, width)], 0, 0),
            )

            @pl.when(mi >= 2)
            def _():
                pair_sum(n - 2)

            push(n)
            rounds(ramp(start, stop, mi, nm), ramp(start, stop, mi + 1, nm))
            return carry

        def half_step(fi, carry):
            d0, d1, d2 = (due[k] + fi * (due[k + 2] - due[k]) for k in (1, 2, 3))
            from_i, to_i = fi * 2 * early, 2 * early + fi * (nu - 2 * early)
            lax.fori_loop(from_i, to_i, functools.partial(hidden_chunk, from_i, to_i, d0, d1), 0)
            rounds(d0 + (d1 - d0) * (to_i - from_i) // (2 * early), d1)

            @pl.when(fi == 0)
            def _():
                for k in sets:
                    h_load(layer, k).wait()

            @pl.when(fi == 1)
            def _():
                for k in sets:
                    gb_cat[of(k)] = g[of(k)].astype(BF16)

                @pl.when(layer > 0)
                def _():
                    for load in loads(layer - 1, 0):
                        load.start()

                @pl.when(layer == 0)
                def _():
                    dx_store().start()

            lax.fori_loop(0, nm, functools.partial(first_weight, fi, d1, d2), 0)
            pair_sum(base + nu + fi * nm + nm - 2)
            pair_sum(base + nu + fi * nm + nm - 1)
            return carry

        lax.fori_loop(0, nf, half_step, 0)
        return carry

    lax.fori_loop(0, layers, layer_step, 0)
    rounds(4 * nu * (layers - 1) + PACE[4] * nu // 10, pieces + 4 * LAG)
    dx_store().wait()


def backward(w_one, w_two, u, a, h, dy, dy_nbr, rows):
    layers, width, wide = w_one.shape
    tokens = dy.shape[0]
    half = wide // 2
    nu = half // rows
    chunk = wide // nu
    units = 2 * nu * layers
    dma, reg = pltpu.SemaphoreType.DMA, pltpu.SemaphoreType.REGULAR
    hbm = pl.BlockSpec(memory_space=pl.ANY)
    sub, narrow = rows // 8, width // 2
    shape = jax.ShapeDtypeStruct
    scratch = [
        pltpu.VMEM((2 * tokens, half), BF16),
        pltpu.VMEM((2 * tokens, wide), BF16),
        pltpu.VMEM((2 * tokens, width // 2), BF16),
        pltpu.VMEM((2 * tokens, width), BF16),
        pltpu.VMEM((2 * tokens, width), F32),
        pltpu.VMEM((2, chunk, width), BF16),
        pltpu.VMEM((2, width, chunk), BF16),
        pltpu.VMEM((2, 2, tokens, chunk), BF16),
        pltpu.VMEM((SLOTS, 4, sub, narrow), BF16),
        pltpu.VMEM((PARTS, 4, sub, width), BF16),
        pltpu.VMEM((RECV0, 4, sub, width), BF16),
        pltpu.VMEM((RECV, 2, sub, narrow), BF16),
        pltpu.VMEM((RECV, 1, sub, narrow), BF16),
        *[dma((SEMS,))] * 11,
        *[dma((RECV,))] * 2,
        *[reg((RECV,))] * 2,
        dma((PARTS,)), dma((RECV0,)), reg((RECV0,)),
        dma((2,)), dma((2,)), dma((2,)), dma((2,)), dma((2,)), dma((2, 2)), dma,
    ]
    return pl.pallas_call(
        functools.partial(backward_body, layers=layers, tokens=tokens, width=width, wide=wide, rows=rows),
        out_shape=[
            shape((2 * units - 2 * nu, 2, 8, sub, narrow), BF16),
            shape((tokens, width), BF16),
            shape((2 * nu, sub, narrow), BF16),
        ],
        in_specs=[hbm] * 7,
        out_specs=[hbm] * 3,
        scratch_shapes=scratch,
        compiler_params=pltpu.CompilerParams(collective_id=0, has_side_effects=True, vmem_limit_bytes=VMEM_LIMIT),
        name="backward",
    )(w_one, w_two, u, a, h, dy, dy_nbr)


COPY_SLOTS, COPY_LEAD = 40, 16


def assemble_body(tot, dx_in, one, two, dx, buf, dx_buf, s_in, s_out, s_dx, *, layers, nu, nm, width):
    items = 2 * tot.shape[0]
    narrow = width // 2

    def load(j):
        return pltpu.make_async_copy(tot.at[j // 2, j % 2], buf.at[j % COPY_SLOTS], s_in.at[j % COPY_SLOTS])

    def stores(j, run):
        m, core, slot = j // 2, j % 2, j % COPY_SLOTS
        n, side = m // 2, m % 2
        layer, i = layers - 1 - n // (2 * nu), n % nu
        mid = (m % 3) // 2
        for q in range(4):
            src = (1 - mid) * q + mid * (q % 2 * 2 + q // 2)
            span = buf.at[slot, pl.ds(src * 2, 2)]

            @pl.when((n // nu) % 2 == 0)
            def _():
                cols = pl.ds(pl.multiple_of(side * narrow, 128), narrow)
                run(pltpu.make_async_copy(span, two.at[layer, core * nu + i, pl.ds(2 * q, 2), :, cols], s_out.at[slot, q]))

            @pl.when((n // nu) % 2 == 1)
            def _():
                cols = pl.ds(pl.multiple_of((core * (nu // nm) + i // nm) * width + side * narrow, 128), narrow)
                run(pltpu.make_async_copy(span, one.at[layer, i % nm, pl.ds(2 * q, 2), :, cols], s_out.at[slot, q]))

    def step(j, carry):
        @pl.when(j >= COPY_SLOTS)
        def _():
            stores(j - COPY_SLOTS, lambda c: c.wait())

        @pl.when(j < items)
        def _():
            load(j).start()

        @pl.when(jnp.logical_and(j >= COPY_LEAD, j < items + COPY_LEAD))
        def _():
            load(j - COPY_LEAD).wait()
            stores(j - COPY_LEAD, lambda c: c.start())

        return carry

    dx_load = pltpu.make_async_copy(dx_in, dx_buf, s_dx.at[0])
    dx_store = pltpu.make_async_copy(dx_buf, dx, s_dx.at[1])
    dx_load.start()
    lax.fori_loop(0, COPY_SLOTS, step, 0)
    dx_load.wait()
    dx_store.start()
    lax.fori_loop(COPY_SLOTS, items + COPY_SLOTS, step, 0)
    dx_store.wait()


def finish_body(last, one_in, one, buf, s_in, s_out, *, nm, width, first):
    devices, count = last.shape[:2]
    narrow = width // 2

    def load(d):
        return pltpu.make_async_copy(last.at[d], buf.at[d], s_in.at[d])

    def store(d, p):
        m = first + p
        z, y, x, core = d // 8, d // 4 % 2, d // 2 % 2, d % 2
        mid = (m % 3) // 2
        a_axis = (1 - mid) * (m % 3) + mid * ((m // 3) % 2)
        row = 4 * z + 2 * (x + a_axis * (y - x)) + y + a_axis * (x - y)
        i, side = p // 2, p % 2
        cols = pl.ds(pl.multiple_of((core * 2 + i // nm) * width + side * narrow, 128), narrow)
        return pltpu.make_async_copy(buf.at[d, p], one.at[0, i % nm, row, :, cols], s_out)

    for d in range(devices):
        load(d).start()

    def out(d, carry):
        load(d).wait()
        for p in range(count):
            store(d, p).start()
        return carry

    lax.fori_loop(0, devices, out, 0)

    def done(d, carry):
        for p in range(count):
            store(d, p).wait()
        return carry

    lax.fori_loop(0, devices, done, 0)


def assemble(tot, dx, layers, width, wide, rows):
    nu, nm, sub = wide // 2 // rows, width // rows, rows // 8
    shape = jax.ShapeDtypeStruct
    hbm = pl.BlockSpec(memory_space=pl.ANY)
    return pl.pallas_call(
        functools.partial(assemble_body, layers=layers, nu=nu, nm=nm, width=width),
        out_shape=[shape((layers, nm, 8, sub, wide), BF16), shape((layers, 2 * nu, 8, sub, width), BF16), shape(dx.shape, BF16)],
        in_specs=[hbm] * 2,
        out_specs=[hbm] * 3,
        scratch_shapes=[
            pltpu.VMEM((COPY_SLOTS, 8, sub, width // 2), BF16),
            pltpu.VMEM(dx.shape, BF16),
            pltpu.SemaphoreType.DMA((COPY_SLOTS,)),
            pltpu.SemaphoreType.DMA((COPY_SLOTS, 4)),
            pltpu.SemaphoreType.DMA((2,)),
        ],
        compiler_params=pltpu.CompilerParams(vmem_limit_bytes=VMEM_LIMIT),
        cost_estimate=pl.CostEstimate(flops=400 * tot.size, bytes_accessed=4 * tot.size, transcendentals=0),
        name="assemble",
    )(tot, dx)


def finish(last, one, first, nm, width):
    hbm = pl.BlockSpec(memory_space=pl.ANY)
    return pl.pallas_call(
        functools.partial(finish_body, nm=nm, width=width, first=first),
        out_shape=jax.ShapeDtypeStruct(one.shape, BF16),
        in_specs=[hbm] * 2,
        out_specs=hbm,
        scratch_shapes=[pltpu.VMEM(last.shape, BF16), pltpu.SemaphoreType.DMA((last.shape[0],)), pltpu.SemaphoreType.DMA],
        input_output_aliases={1: 0},
        compiler_params=pltpu.CompilerParams(vmem_limit_bytes=VMEM_LIMIT),
        cost_estimate=pl.CostEstimate(flops=400 * last.size, bytes_accessed=4 * last.size, transcendentals=0),
        name="finish",
    )(last, one)


def solution(mesh, rows=UNIT_ROWS):
    batch_spec = P(AXES)

    def per_device(w_one, w_two, x_loc, dy_loc):
        layers, width, wide = w_one.shape
        x = x_loc.reshape(-1, width)
        dy = dy_loc.reshape(-1, width)
        u, a, h, _, dy_nbr, _ = forward(x, dy, w_one, w_two, rows)
        tot, dx, last = backward(w_one, w_two, u, a, h, dy, dy_nbr, rows)
        everyone = lax.all_gather(last, AXES)
        one, two, dx = assemble(tot, dx, layers, width, wide, rows)
        one = finish(everyone, one, tot.shape[0], width // rows, width)
        return one.reshape(w_one.shape), two.reshape(w_two.shape), dx.reshape(x_loc.shape)

    return jax.shard_map(per_device, mesh=mesh, in_specs=(P(), P(), batch_spec, batch_spec), out_specs=(P(), P(), batch_spec), check_vma=False)
```

```python
import functools

import jax
import jax.numpy as jnp
from jax import lax
from jax.experimental import pallas as pl
from jax.experimental.pallas import tpu as pltpu
from jax.sharding import PartitionSpec as P

AXES = ("replica", "data")
MESH = pl.DeviceIdType.MESH
BF16, F32 = jnp.bfloat16, jnp.float32
VMEM_LIMIT = 67_043_328
C0, C1 = 0.7978845608028654, 0.044715
UNIT_ROWS = 256
LAG = 4
SLOTS, SEMS, RECV, PARTS, RECV0 = 44, 12, 10, 3, 4
PACE_FIRST, PACE = (6, 18, 20, 28, 30), (-2, 12, 16, 26, 30)
X, Y, Z = 0, 1, 2
UP_BLOCKS = 4


def gelu(v):
    half = 0.5 * v
    return half + half * jnp.tanh(v * (C0 + C0 * C1 * (v * v)))


def gelu_slope(v):
    sq = v * v
    t = jnp.tanh(v * (C0 + C0 * C1 * sq))
    return 0.5 + 0.5 * t + v * (1.0 - t * t) * (0.5 * C0 + 1.5 * C0 * C1 * sq)


def mm(lhs, rhs, lhs_dim, rhs_dim):
    return lax.dot_general(lhs, rhs, (((lhs_dim,), (rhs_dim,)), ((), ())), preferred_element_type=F32)


def forward_body(
    x_ref, x, dy, w1_ref, w2_ref, u_ref, a_ref, h_ref, x_nbr, dy_nbr, h_nbr,
    hid, acc, act_s, nxt, made, s_send, s_recv, s_load,
    *, layers, chunks, rows,
):
    tokens_of, layer, j = pl.program_id(0), pl.program_id(1), pl.program_id(2)
    z = lax.axis_index("replica")
    part = rows // 2
    shift = z * part
    other = (1 - z, lax.axis_index("data"))
    third = x.shape[0] // 3
    given = layers - 2

    def swap(src, dst, k):
        return pltpu.make_async_remote_copy(
            src_ref=src, dst_ref=dst, send_sem=s_send.at[k], recv_sem=s_recv.at[k], device_id=other, device_id_type=MESH
        )

    x_swap = swap(x, x_nbr, 0)
    dy_swap = [swap(dy.at[pl.ds(k * third, third)], dy_nbr.at[pl.ds(k * third, third)], 1 + k) for k in range(3)]
    h_swap = [swap(made.at[k], h_nbr.at[k], 4 + k) for k in range(given)]
    x_load = pltpu.make_async_copy(x_nbr, nxt, s_load)
    h_load = [pltpu.make_async_copy(h_nbr.at[k], nxt, s_load) for k in range(given)]

    def at(s, l, c):
        return pl.when(jnp.logical_and(tokens_of == s, jnp.logical_and(layer == l, j == c)))

    @at(0, 0, 0)
    def _():
        barrier = pltpu.get_barrier_semaphore()
        pl.semaphore_signal(barrier, inc=1, device_id=other, device_id_type=MESH)
        hid[...] = x_ref[...]
        pl.semaphore_wait(barrier, 1)
        x_swap.start()
        dy_swap[0].start()

    for k in range(given):

        @at(0, k + 2, 0)
        def _(k=k):
            h_swap[k].start()

        @at(1, k + 1, chunks - 1)
        def _(k=k):
            h_swap[k].wait_recv()
            h_load[k].start()

        @at(1, k + 2, 0)
        def _(k=k):
            h_load[k].wait()
            hid[...] = nxt[...]

    @at(0, layers - 1, 0)
    def _():
        dy_swap[1].start()
        dy_swap[2].start()
        x_swap.wait()
        x_load.start()

    @at(1, 0, 0)
    def _():
        x_load.wait()
        hid[...] = nxt[...]

    @at(1, layers - 1, chunks - 1)
    def _():
        for copy in h_swap:
            copy.wait_send()
        for copy in dy_swap:
            copy.wait()

    def keep(dst, src):
        for k in range(src.shape[1] // rows):
            dst[0, 0, :, k * part : (k + 1) * part] = src[:, pl.ds(pl.multiple_of(k * rows + shift, part), part)]

    @pl.when(j == 0)
    def _():
        keep(h_ref, hid)
        acc[...] = hid[...].astype(F32)

    def up():
        pre = mm(hid[...], w1_ref[0], 1, 0).astype(BF16)
        u_ref[0, 0] = pre
        act = gelu(pre.astype(F32)).astype(BF16)
        act_s[...] = act
        keep(a_ref, act_s)
        return act

    def up_only():
        step = hid.shape[0] // UP_BLOCKS
        spans = [slice(k * step, (k + 1) * step) for k in range(UP_BLOCKS)]
        pre = [mm(hid[span], w1_ref[0], 1, 0).astype(BF16) for span in spans]
        for span, p in zip(spans, pre):
            u_ref[0, 0, span] = p
            act_s[span] = gelu(p.astype(F32)).astype(BF16)
        keep(a_ref, act_s)

    full = layer < layers - 1 - tokens_of * given

    @pl.when(full)
    def _():
        acc[...] += mm(up(), w2_ref[0], 1, 0)

        @pl.when(j == chunks - 1)
        def _():
            hid[...] = acc[...].astype(BF16)

    @pl.when(jnp.logical_not(full))
    def _():
        up_only()

    for k in range(given):

        @at(0, k + 1, chunks - 1)
        def _(k=k):
            made[k] = hid[...]


def forward(x, dy, w_one, w_two, rows):
    layers, width, wide = w_one.shape
    tokens = x.shape[0]
    chunk = width
    chunks = wide // chunk
    shape = jax.ShapeDtypeStruct
    hbm = pl.BlockSpec(memory_space=pl.ANY)
    dma = pltpu.SemaphoreType.DMA
    return pl.pallas_call(
        functools.partial(forward_body, layers=layers, chunks=chunks, rows=rows),
        grid=(2, layers, chunks),
        out_shape=[
            shape((2, layers, tokens, wide), BF16),
            shape((2, layers, tokens, wide // 2), BF16),
            shape((2, layers, tokens, width // 2), BF16),
            shape(x.shape, BF16),
            shape(x.shape, BF16),
            shape((max(layers - 2, 1), tokens, width), BF16),
        ],
        in_specs=[
            pl.BlockSpec((tokens, width), lambda s, l, j: (0, 0)),
            hbm,
            hbm,
            pl.BlockSpec((1, width, chunk), lambda s, l, j: (l, 0, j)),
            pl.BlockSpec((1, chunk, width), lambda s, l, j: (l, j, 0)),
        ],
        out_specs=[
            pl.BlockSpec((1, 1, tokens, chunk), lambda s, l, j: (s, l, 0, j)),
            pl.BlockSpec((1, 1, tokens, chunk // 2), lambda s, l, j: (s, l, 0, j)),
            pl.BlockSpec((1, 1, tokens, width // 2), lambda s, l, j: (s, l, 0, 0)),
            hbm,
            hbm,
            hbm,
        ],
        scratch_shapes=[
            pltpu.VMEM((tokens, width), BF16),
            pltpu.VMEM((tokens, width), F32),
            pltpu.VMEM((tokens, chunk), BF16),
            pltpu.VMEM((tokens, width), BF16),
            pltpu.VMEM((max(layers - 2, 1), tokens, width), BF16),
            dma((2 + layers,)),
            dma((2 + layers,)),
            dma,
        ],
        compiler_params=pltpu.CompilerParams(
            collective_id=1, has_side_effects=True, vmem_limit_bytes=VMEM_LIMIT
        ),
        name="forward",
    )(x, x, dy, w_one, w_two)


def backward_body(
    w1, w2, u, a, h, dy_own, dy_nbr,
    tot, dx, last,
    a_cat, du_cat, h_cat, gb_cat, g, w2c, w1c, uc, unit, part0, rcv0, rcv1, rcv2,
    s_rs1, s_rs2, s_ag1, s_ag2, s_ag3, s_fwd, s_own, r_ag1, r_ag2, r_ag3, r_fwd,
    r_rs1, r_rs2, c_rs1, c_rs2, s_rs0, r_rs0, c_rs0,
    l_a, l_gb, l_h, l_w2, l_w1, l_u, l_dx,
    *, layers, tokens, width, wide, rows,
):
    half = wide // 2
    part = rows // 2
    nu = half // rows
    hn = nu // 2
    nm = width // rows
    nf = nu // nm
    chunk = wide // nu
    units = 2 * nu * layers
    pieces = 2 * units
    whole = pieces - 2 * nu
    early = (hn + 1) // 2
    narrow = width // 2
    step = tokens // 2
    z, rest = lax.axis_index("replica"), lax.axis_index("data")
    core, x, y = rest % 2, (rest // 2) % 2, rest // 4

    def choose(axis):
        return (1 - axis) * (2 - axis) // 2, axis * (2 - axis), axis * (axis - 1) // 2

    def peer(axis):
        ex, ey, ez = choose(axis)
        px, py, pz = x + ex * (1 - 2 * x), y + ey * (1 - 2 * y), z + ez * (1 - 2 * z)
        return (pz, (py * 2 + px) * 2 + core)

    sibling = (z, (y * 2 + x) * 2 + 1 - core)

    def send(src, dst, ssem, rsem, to):
        return pltpu.make_async_remote_copy(src_ref=src, dst_ref=dst, send_sem=ssem, recv_sem=rsem, device_id=to, device_id_type=MESH)

    def place(m):
        mid = (m % 3) // 2
        a_axis = (1 - mid) * (m % 3) + mid * ((m // 3) % 2)
        b_axis = 1 - a_axis
        bit_a = x + a_axis * (y - x)
        bit_b = x + b_axis * (y - x)
        own = (1 - mid) * (4 * z + 2 * bit_a + bit_b) + mid * (4 * bit_a + 2 * z + bit_b)
        return mid, a_axis, b_axis, bit_a, bit_b, own

    def rs0(n):
        return send(part0.at[n % PARTS], rcv0.at[n % RECV0], s_rs0.at[n % PARTS], r_rs0.at[n % RECV0], sibling)

    def rs1(m):
        mid, a_axis, b_axis, bit_a, bit_b, own = place(m)
        return send(unit.at[m % SLOTS, pl.ds(2 - 2 * bit_a, 2)], rcv1.at[m % RECV], s_rs1.at[m % SEMS], r_rs1.at[m % RECV], peer(a_axis))

    def rs2(m):
        mid, a_axis, b_axis, bit_a, bit_b, own = place(m)
        return send(unit.at[m % SLOTS, pl.ds(2 * bit_a + 1 - bit_b, 1)], rcv2.at[m % RECV], s_rs2.at[m % SEMS], r_rs2.at[m % RECV], peer(b_axis))

    def own_copy(m):
        mid, a_axis, b_axis, bit_a, bit_b, own = place(m)
        return pltpu.make_async_copy(unit.at[m % SLOTS, pl.ds(2 * bit_a + bit_b, 1)], tot.at[m, core, pl.ds(own, 1)], s_own.at[m % SEMS])

    def last_copy(m):
        mid, a_axis, b_axis, bit_a, bit_b, own = place(m)
        return pltpu.make_async_copy(unit.at[m % SLOTS, pl.ds(2 * bit_a + bit_b, 1)], last.at[pl.ds(m - whole, 1)], s_own.at[m % SEMS])

    def ag1(m):
        mid, a_axis, b_axis, bit_a, bit_b, own = place(m)
        return send(
            unit.at[m % SLOTS, pl.ds(2 * bit_a + bit_b, 1)], tot.at[m, core, pl.ds(own, 1)], s_ag1.at[m % SEMS], r_ag1.at[m % SEMS], peer(b_axis)
        )

    def ag2(m):
        mid, a_axis, b_axis, bit_a, bit_b, own = place(m)
        span = tot.at[m, core, pl.ds(own // 2 * 2, 2)]
        return send(span, span, s_ag2.at[m % SEMS], r_ag2.at[m % SEMS], peer(a_axis + mid * (Z - a_axis)))

    def ag3(m):
        mid, a_axis, b_axis, bit_a, bit_b, own = place(m)
        span = tot.at[m, core, pl.ds(own // 4 * 4, 4)]
        return send(span, span, s_ag3.at[m % SEMS], r_ag3.at[m % SEMS], peer(Z + mid * (a_axis - Z)))

    def fwd(m):
        span = tot.at[m, core]
        return send(span, span, s_fwd.at[m % SEMS], r_fwd.at[m % SEMS], sibling)

    def add(m, block, other):
        unit[m % SLOTS, block] = (unit[m % SLOTS, block].astype(F32) + other.astype(F32)).astype(BF16)

    def credit(sem, n, slots, count, to):
        @pl.when(n + slots < count)
        def _():
            pl.semaphore_signal(sem.at[n % slots], inc=1, device_id=to, device_id_type=MESH)

    def spend(sem, n, slots):
        @pl.when(n >= slots)
        def _():
            pl.semaphore_wait(sem.at[n % slots], 1)

    def live(m):
        return jnp.logical_and(m >= 0, m < pieces)

    def spread_out(m):
        return jnp.logical_and(m >= 0, m < whole)

    def left(m):
        return jnp.logical_and(m >= whole, m < pieces)

    def make(n, theirs, mine):
        part0[n % PARTS] = theirs.reshape(4, rows // 8, width).astype(BF16)
        kept = mine.reshape(4, rows // 8, width).astype(BF16)
        for c in range(2):
            unit[(2 * n + c) % SLOTS] = kept[:, :, c * narrow : (c + 1) * narrow]

    def push(n):
        spend(c_rs0, n, RECV0)
        rs0(n).start()

    def pair_sum(n):
        rs0(n).wait()
        for c in range(2):
            for block in range(4):
                add(2 * n + c, block, rcv0[n % RECV0, block, :, c * narrow : (c + 1) * narrow])
        credit(c_rs0, n, RECV0, units, sibling)

    def comm(r, carry):
        m0, m1, m2, m3, m4, m5 = (r - k * LAG for k in range(6))
        m6 = m5 - LAG

        @pl.when(live(m2))
        def _():
            mid, a_axis, b_axis, bit_a, bit_b, own = place(m2)
            rs2(m2).wait_recv()
            add(m2, 2 * bit_a + bit_b, rcv2[m2 % RECV, 0])
            credit(c_rs2, m2, RECV, pieces, peer(b_axis))
            rs1(m2).wait_send()

        @pl.when(live(m1))
        def _():
            mid, a_axis, b_axis, bit_a, bit_b, own = place(m1)
            rs1(m1).wait_recv()
            add(m1, 2 * bit_a + 1 - bit_b, rcv1[m1 % RECV, 1 - bit_b])
            add(m1, 2 * bit_a + bit_b, rcv1[m1 % RECV, bit_b])
            credit(c_rs1, m1, RECV, pieces, peer(a_axis))

        @pl.when(live(m0))
        def _():
            spend(c_rs1, m0, RECV)
            rs1(m0).start()

        @pl.when(spread_out(m2))
        def _():
            own_copy(m2).start()
            ag1(m2).start()

        @pl.when(left(m2))
        def _():
            last_copy(m2).start()

        @pl.when(live(m1))
        def _():
            spend(c_rs2, m1, RECV)
            rs2(m1).start()

        @pl.when(live(m3))
        def _():
            rs2(m3).wait_send()

        @pl.when(left(m3))
        def _():
            last_copy(m3).wait()

        @pl.when(spread_out(m3))
        def _():
            own_copy(m3).wait()
            ag1(m3).wait()
            ag2(m3).start()

        @pl.when(spread_out(m4))
        def _():
            ag2(m4).wait()
            ag3(m4).start()

        @pl.when(spread_out(m5))
        def _():
            ag3(m5).wait()
            fwd(m5).start()

        @pl.when(spread_out(m6))
        def _():
            fwd(m6).wait()

        return carry

    def rounds(lo, hi):
        lax.fori_loop(lo, hi, comm, 0)

    def ramp(lo, hi, i, n):
        return lo + (hi - lo) * i * i // (n * n)

    sets = (0, 1)
    dys = (dy_own, dy_nbr)

    def of(k):
        return pl.ds(k * tokens, tokens)

    def chunk_at(i):
        late, wait = hn - early, i // (2 * early)
        first = i // early * hn + i % early
        second = early + (i - 2 * early) // late * hn + (i - 2 * early) % late
        return first + wait * (second - first)

    def loads(layer, i):
        f0, slot = pl.multiple_of(chunk_at(i) * chunk, 128), i % 2
        return (
            pltpu.make_async_copy(w2.at[layer, pl.ds(f0, chunk)], w2c.at[slot], l_w2.at[slot]),
            pltpu.make_async_copy(w1.at[layer, :, pl.ds(f0, chunk)], w1c.at[slot], l_w1.at[slot]),
            *(pltpu.make_async_copy(u.at[k, layer, :, pl.ds(f0, chunk)], uc.at[slot, k], l_u.at[slot, k]) for k in sets),
        )

    def cols(i, size):
        return pl.ds(pl.multiple_of(i * size, 128), size)

    def a_load(layer, k):
        return pltpu.make_async_copy(a.at[k, layer], a_cat.at[of(k)], l_a.at[k])

    def h_load(layer, k):
        return pltpu.make_async_copy(h.at[k, layer], h_cat.at[of(k)], l_h.at[k])

    def gb_load(k):
        return pltpu.make_async_copy(dys[k], gb_cat.at[of(k)], l_gb.at[k])

    def dx_store():
        return pltpu.make_async_copy(gb_cat.at[of(0)], dx, l_dx)

    barrier = pltpu.get_barrier_semaphore()
    for to in (peer(X), peer(Y), peer(Z), sibling):
        pl.semaphore_signal(barrier, inc=1, device_id=to, device_id_type=MESH)
    for k in sets:
        gb_load(k).start()
        a_load(layers - 1, k).start()
    for k in sets:
        gb_load(k).wait()
    pl.semaphore_wait(barrier, 4)

    def layer_step(li, carry):
        layer = layers - 1 - li
        base = li * 2 * nu
        late = jnp.minimum(li, 1)
        due = [late * (4 * nu * (li - 1) + PACE[4] * nu // 10)]
        for p, q in zip(PACE_FIRST, PACE):
            due.append(4 * nu * li + p * nu // 10 + late * (q * nu // 10 - p * nu // 10))
        for k in sets:
            a_load(layer, k).wait()

        def second_weight(i, carry):
            n = base + i
            lhs = jnp.concatenate([a_cat[:, cols((1 - core) * nu + i, part)], a_cat[:, cols(core * nu + i, part)]], axis=1)
            out = mm(lhs, gb_cat[...], 0, 0)
            make(n, out[:part], out[part:])

            @pl.when(i >= 2)
            def _():
                pair_sum(n - 2)

            push(n)
            rounds(ramp(due[0], due[1], i, nu), ramp(due[0], due[1], i + 1, nu))
            return carry

        lax.fori_loop(0, nu, second_weight, 0)
        pair_sum(base + nu - 2)
        pair_sum(base + nu - 1)
        for k in sets:
            h_load(layer, k).start()

        @pl.when(li == 0)
        def _():
            for load in loads(layer, 0):
                load.start()
            for k in sets:
                g[of(k)] = gb_cat[of(k)].astype(F32)

        @pl.when(layer > 0)
        def _():
            for k in sets:
                a_load(layer - 1, k).start()

        def hidden_chunk(from_i, to_i, start, stop, i, carry):
            for load in loads(layer, i):
                load.wait()

            @pl.when(i < nu - 1)
            def _():
                for load in loads(layer, i + 1):
                    load.start()

            def token_set(k, carry):
                at = [pl.ds(q * step, step) for q in range(2)]
                rows_q = [pl.ds(pl.multiple_of(k * tokens + q * step, 16), step) for q in range(2)]
                d_act = [mm(gb_cat[r], w2c[i % 2], 1, 1) for r in rows_q]
                for q in range(2):
                    du = (d_act[q] * gelu_slope(uc[i % 2, k, at[q]].astype(F32))).astype(BF16)
                    du_cat[rows_q[q], cols(chunk_at(i), chunk)] = du
                    g[rows_q[q]] += mm(du, w1c[i % 2], 1, 1)
                s = 2 * (i - from_i) + k
                rounds(start + (stop - start) * s // (4 * early), start + (stop - start) * (s + 1) // (4 * early))
                return carry

            lax.fori_loop(0, 2, token_set, 0)
            return carry

        def first_weight(fi, start, stop, mi, carry):
            n = base + nu + fi * nm + mi
            lhs = h_cat[:, cols(mi, part)]
            make(
                n,
                mm(lhs, du_cat[:, cols((1 - core) * nf + fi, width)], 0, 0),
                mm(lhs, du_cat[:, cols(core * nf + fi, width)], 0, 0),
            )

            @pl.when(mi >= 2)
            def _():
                pair_sum(n - 2)

            push(n)
            rounds(ramp(start, stop, mi, nm), ramp(start, stop, mi + 1, nm))
            return carry

        def half_step(fi, carry):
            d0, d1, d2 = (due[k] + fi * (due[k + 2] - due[k]) for k in (1, 2, 3))
            from_i, to_i = fi * 2 * early, 2 * early + fi * (nu - 2 * early)
            lax.fori_loop(from_i, to_i, functools.partial(hidden_chunk, from_i, to_i, d0, d1), 0)
            rounds(d0 + (d1 - d0) * (to_i - from_i) // (2 * early), d1)

            @pl.when(fi == 0)
            def _():
                for k in sets:
                    h_load(layer, k).wait()

            @pl.when(fi == 1)
            def _():
                for k in sets:
                    gb_cat[of(k)] = g[of(k)].astype(BF16)

                @pl.when(layer > 0)
                def _():
                    for load in loads(layer - 1, 0):
                        load.start()

                @pl.when(layer == 0)
                def _():
                    dx_store().start()

            lax.fori_loop(0, nm, functools.partial(first_weight, fi, d1, d2), 0)
            pair_sum(base + nu + fi * nm + nm - 2)
            pair_sum(base + nu + fi * nm + nm - 1)
            return carry

        lax.fori_loop(0, nf, half_step, 0)
        return carry

    lax.fori_loop(0, layers, layer_step, 0)
    rounds(4 * nu * (layers - 1) + PACE[4] * nu // 10, pieces + 4 * LAG)
    dx_store().wait()


def backward(w_one, w_two, u, a, h, dy, dy_nbr, rows):
    layers, width, wide = w_one.shape
    tokens = dy.shape[0]
    half = wide // 2
    nu = half // rows
    chunk = wide // nu
    units = 2 * nu * layers
    dma, reg = pltpu.SemaphoreType.DMA, pltpu.SemaphoreType.REGULAR
    hbm = pl.BlockSpec(memory_space=pl.ANY)
    sub, narrow = rows // 8, width // 2
    shape = jax.ShapeDtypeStruct
    scratch = [
        pltpu.VMEM((2 * tokens, half), BF16),
        pltpu.VMEM((2 * tokens, wide), BF16),
        pltpu.VMEM((2 * tokens, width // 2), BF16),
        pltpu.VMEM((2 * tokens, width), BF16),
        pltpu.VMEM((2 * tokens, width), F32),
        pltpu.VMEM((2, chunk, width), BF16),
        pltpu.VMEM((2, width, chunk), BF16),
        pltpu.VMEM((2, 2, tokens, chunk), BF16),
        pltpu.VMEM((SLOTS, 4, sub, narrow), BF16),
        pltpu.VMEM((PARTS, 4, sub, width), BF16),
        pltpu.VMEM((RECV0, 4, sub, width), BF16),
        pltpu.VMEM((RECV, 2, sub, narrow), BF16),
        pltpu.VMEM((RECV, 1, sub, narrow), BF16),
        *[dma((SEMS,))] * 11,
        *[dma((RECV,))] * 2,
        *[reg((RECV,))] * 2,
        dma((PARTS,)), dma((RECV0,)), reg((RECV0,)),
        dma((2,)), dma((2,)), dma((2,)), dma((2,)), dma((2,)), dma((2, 2)), dma,
    ]
    return pl.pallas_call(
        functools.partial(backward_body, layers=layers, tokens=tokens, width=width, wide=wide, rows=rows),
        out_shape=[
            shape((2 * units - 2 * nu, 2, 8, sub, narrow), BF16),
            shape((tokens, width), BF16),
            shape((2 * nu, sub, narrow), BF16),
        ],
        in_specs=[hbm] * 7,
        out_specs=[hbm] * 3,
        scratch_shapes=scratch,
        compiler_params=pltpu.CompilerParams(collective_id=0, has_side_effects=True, vmem_limit_bytes=VMEM_LIMIT),
        name="backward",
    )(w_one, w_two, u, a, h, dy, dy_nbr)


COPY_SLOTS, COPY_LEAD = 40, 16


def assemble_body(tot, dx_in, one, two, dx, buf, dx_buf, s_in, s_out, s_dx, *, layers, nu, nm, width):
    items = 2 * tot.shape[0]
    narrow = width // 2

    def load(j):
        return pltpu.make_async_copy(tot.at[j // 2, j % 2], buf.at[j % COPY_SLOTS], s_in.at[j % COPY_SLOTS])

    def stores(j, run):
        m, core, slot = j // 2, j % 2, j % COPY_SLOTS
        n, side = m // 2, m % 2
        layer, i = layers - 1 - n // (2 * nu), n % nu
        mid = (m % 3) // 2
        for q in range(4):
            src = (1 - mid) * q + mid * (q % 2 * 2 + q // 2)
            span = buf.at[slot, pl.ds(src * 2, 2)]

            @pl.when((n // nu) % 2 == 0)
            def _():
                cols = pl.ds(pl.multiple_of(side * narrow, 128), narrow)
                run(pltpu.make_async_copy(span, two.at[layer, core * nu + i, pl.ds(2 * q, 2), :, cols], s_out.at[slot, q]))

            @pl.when((n // nu) % 2 == 1)
            def _():
                cols = pl.ds(pl.multiple_of((core * (nu // nm) + i // nm) * width + side * narrow, 128), narrow)
                run(pltpu.make_async_copy(span, one.at[layer, i % nm, pl.ds(2 * q, 2), :, cols], s_out.at[slot, q]))

    def step(j, carry):
        @pl.when(j >= COPY_SLOTS)
        def _():
            stores(j - COPY_SLOTS, lambda c: c.wait())

        @pl.when(j < items)
        def _():
            load(j).start()

        @pl.when(jnp.logical_and(j >= COPY_LEAD, j < items + COPY_LEAD))
        def _():
            load(j - COPY_LEAD).wait()
            stores(j - COPY_LEAD, lambda c: c.start())

        return carry

    dx_load = pltpu.make_async_copy(dx_in, dx_buf, s_dx.at[0])
    dx_store = pltpu.make_async_copy(dx_buf, dx, s_dx.at[1])
    dx_load.start()
    lax.fori_loop(0, COPY_SLOTS, step, 0)
    dx_load.wait()
    dx_store.start()
    lax.fori_loop(COPY_SLOTS, items + COPY_SLOTS, step, 0)
    dx_store.wait()


def finish_body(last, one_in, one, buf, s_in, s_out, *, nm, width, first):
    devices, count = last.shape[:2]
    narrow = width // 2

    def load(d):
        return pltpu.make_async_copy(last.at[d], buf.at[d], s_in.at[d])

    def store(d, p):
        m = first + p
        z, y, x, core = d // 8, d // 4 % 2, d // 2 % 2, d % 2
        mid = (m % 3) // 2
        a_axis = (1 - mid) * (m % 3) + mid * ((m // 3) % 2)
        row = 4 * z + 2 * (x + a_axis * (y - x)) + y + a_axis * (x - y)
        i, side = p // 2, p % 2
        cols = pl.ds(pl.multiple_of((core * 2 + i // nm) * width + side * narrow, 128), narrow)
        return pltpu.make_async_copy(buf.at[d, p], one.at[0, i % nm, row, :, cols], s_out)

    for d in range(devices):
        load(d).start()

    def out(d, carry):
        load(d).wait()
        for p in range(count):
            store(d, p).start()
        return carry

    lax.fori_loop(0, devices, out, 0)

    def done(d, carry):
        for p in range(count):
            store(d, p).wait()
        return carry

    lax.fori_loop(0, devices, done, 0)


def assemble(tot, dx, layers, width, wide, rows):
    nu, nm, sub = wide // 2 // rows, width // rows, rows // 8
    shape = jax.ShapeDtypeStruct
    hbm = pl.BlockSpec(memory_space=pl.ANY)
    return pl.pallas_call(
        functools.partial(assemble_body, layers=layers, nu=nu, nm=nm, width=width),
        out_shape=[shape((layers, nm, 8, sub, wide), BF16), shape((layers, 2 * nu, 8, sub, width), BF16), shape(dx.shape, BF16)],
        in_specs=[hbm] * 2,
        out_specs=[hbm] * 3,
        scratch_shapes=[
            pltpu.VMEM((COPY_SLOTS, 8, sub, width // 2), BF16),
            pltpu.VMEM(dx.shape, BF16),
            pltpu.SemaphoreType.DMA((COPY_SLOTS,)),
            pltpu.SemaphoreType.DMA((COPY_SLOTS, 4)),
            pltpu.SemaphoreType.DMA((2,)),
        ],
        compiler_params=pltpu.CompilerParams(vmem_limit_bytes=VMEM_LIMIT),
        cost_estimate=pl.CostEstimate(flops=400 * tot.size, bytes_accessed=4 * tot.size, transcendentals=0),
        name="assemble",
    )(tot, dx)


def finish(last, one, first, nm, width):
    hbm = pl.BlockSpec(memory_space=pl.ANY)
    return pl.pallas_call(
        functools.partial(finish_body, nm=nm, width=width, first=first),
        out_shape=jax.ShapeDtypeStruct(one.shape, BF16),
        in_specs=[hbm] * 2,
        out_specs=hbm,
        scratch_shapes=[pltpu.VMEM(last.shape, BF16), pltpu.SemaphoreType.DMA((last.shape[0],)), pltpu.SemaphoreType.DMA],
        input_output_aliases={1: 0},
        compiler_params=pltpu.CompilerParams(vmem_limit_bytes=VMEM_LIMIT),
        cost_estimate=pl.CostEstimate(flops=400 * last.size, bytes_accessed=4 * last.size, transcendentals=0),
        name="finish",
    )(last, one)


def solution(mesh, rows=UNIT_ROWS):
    batch_spec = P(AXES)

    def per_device(w_one, w_two, x_loc, dy_loc):
        layers, width, wide = w_one.shape
        x = x_loc.reshape(-1, width)
        dy = dy_loc.reshape(-1, width)
        u, a, h, _, dy_nbr, _ = forward(x, dy, w_one, w_two, rows)
        tot, dx, last = backward(w_one, w_two, u, a, h, dy, dy_nbr, rows)
        everyone = lax.all_gather(last, AXES)
        one, two, dx = assemble(tot, dx, layers, width, wide, rows)
        one = finish(everyone, one, tot.shape[0], width // rows, width)
        return one.reshape(w_one.shape), two.reshape(w_two.shape), dx.reshape(x_loc.shape)

    return jax.shard_map(per_device, mesh=mesh, in_specs=(P(), P(), batch_spec, batch_spec), out_specs=(P(), P(), batch_spec), check_vma=False)
```

```python
import functools

import jax
import jax.numpy as jnp
from jax import lax
from jax.experimental import pallas as pl
from jax.experimental.pallas import tpu as pltpu
from jax.sharding import PartitionSpec as P

AXES = ("replica", "data")
MESH = pl.DeviceIdType.MESH
BF16, F32 = jnp.bfloat16, jnp.float32
VMEM_LIMIT = 67_043_328
C0, C1 = 0.7978845608028654, 0.044715
UNIT_ROWS = 256
LAG = 4
SLOTS, SEMS, RECV, PARTS, RECV0 = 44, 12, 10, 3, 4
PACE_FIRST, PACE = (6, 18, 20, 28, 30), (-2, 12, 16, 26, 30)
X, Y, Z = 0, 1, 2
GIVEN = 1
UP_BLOCKS = 4


def gelu(v):
    half = 0.5 * v
    return half + half * jnp.tanh(v * (C0 + C0 * C1 * (v * v)))


def gelu_slope(v):
    sq = v * v
    t = jnp.tanh(v * (C0 + C0 * C1 * sq))
    return 0.5 + 0.5 * t + v * (1.0 - t * t) * (0.5 * C0 + 1.5 * C0 * C1 * sq)


def mm(lhs, rhs, lhs_dim, rhs_dim):
    return lax.dot_general(lhs, rhs, (((lhs_dim,), (rhs_dim,)), ((), ())), preferred_element_type=F32)


def forward_body(
    x_ref, x, dy, w1_ref, w2_ref, u_ref, a_ref, h_ref, x_nbr, dy_nbr, h_nbr,
    hid, acc, act_s, nxt, made, s_send, s_recv, s_load,
    *, layers, chunks, rows,
):
    tokens_of, layer, j = pl.program_id(0), pl.program_id(1), pl.program_id(2)
    z = lax.axis_index("replica")
    part = rows // 2
    shift = z * part
    other = (1 - z, lax.axis_index("data"))
    first_given = layers - GIVEN

    def swap(src, dst, k):
        return pltpu.make_async_remote_copy(
            src_ref=src, dst_ref=dst, send_sem=s_send.at[k], recv_sem=s_recv.at[k], device_id=other, device_id_type=MESH
        )

    x_swap = swap(x, x_nbr, 0)
    dy_swap = swap(dy, dy_nbr, 1)
    h_swap = [swap(made.at[k], h_nbr.at[k], 2 + k) for k in range(GIVEN)]
    x_load = pltpu.make_async_copy(x_nbr, nxt, s_load)
    h_load = [pltpu.make_async_copy(h_nbr.at[k], nxt, s_load) for k in range(GIVEN)]

    def at(s, l, c):
        return pl.when(jnp.logical_and(tokens_of == s, jnp.logical_and(layer == l, j == c)))

    @at(0, 0, 0)
    def _():
        barrier = pltpu.get_barrier_semaphore()
        pl.semaphore_signal(barrier, inc=1, device_id=other, device_id_type=MESH)
        hid[...] = x_ref[...]
        pl.semaphore_wait(barrier, 1)
        x_swap.start()
        dy_swap.start()

    for k in range(GIVEN):

        @at(0, first_given + k, 0)
        def _(k=k):
            h_swap[k].start()

        @at(1, first_given + k - 1, chunks - 1)
        def _(k=k):
            h_swap[k].wait_recv()
            h_load[k].start()

        @at(1, first_given + k, 0)
        def _(k=k):
            h_load[k].wait()
            hid[...] = nxt[...]

    @at(0, layers - 1, 0)
    def _():
        x_swap.wait()
        x_load.start()

    @at(1, 0, 0)
    def _():
        x_load.wait()
        hid[...] = nxt[...]

    @at(1, layers - 1, chunks - 1)
    def _():
        for copy in h_swap:
            copy.wait_send()
        dy_swap.wait()

    def keep(dst, src):
        for k in range(src.shape[1] // rows):
            dst[0, 0, :, k * part : (k + 1) * part] = src[:, pl.ds(pl.multiple_of(k * rows + shift, part), part)]

    @pl.when(j == 0)
    def _():
        keep(h_ref, hid)
        acc[...] = hid[...].astype(F32)

    def up():
        pre = mm(hid[...], w1_ref[0], 1, 0).astype(BF16)
        u_ref[0, 0] = pre
        act = gelu(pre.astype(F32)).astype(BF16)
        act_s[...] = act
        keep(a_ref, act_s)
        return act

    def up_only():
        step = hid.shape[0] // UP_BLOCKS
        spans = [slice(k * step, (k + 1) * step) for k in range(UP_BLOCKS)]
        pre = [mm(hid[span], w1_ref[0], 1, 0).astype(BF16) for span in spans]
        for span, p in zip(spans, pre):
            u_ref[0, 0, span] = p
            act_s[span] = gelu(p.astype(F32)).astype(BF16)
        keep(a_ref, act_s)

    full = layer < layers - 1 - tokens_of * GIVEN

    @pl.when(full)
    def _():
        acc[...] += mm(up(), w2_ref[0], 1, 0)

        @pl.when(j == chunks - 1)
        def _():
            hid[...] = acc[...].astype(BF16)

    @pl.when(jnp.logical_not(full))
    def _():
        up_only()

    for k in range(GIVEN):

        @at(0, first_given + k - 1, chunks - 1)
        def _(k=k):
            made[k] = hid[...]


def forward(x, dy, w_one, w_two, rows):
    layers, width, wide = w_one.shape
    tokens = x.shape[0]
    chunk = width
    chunks = wide // chunk
    shape = jax.ShapeDtypeStruct
    hbm = pl.BlockSpec(memory_space=pl.ANY)
    dma = pltpu.SemaphoreType.DMA
    return pl.pallas_call(
        functools.partial(forward_body, layers=layers, chunks=chunks, rows=rows),
        grid=(2, layers, chunks),
        out_shape=[
            shape((2, layers, tokens, wide), BF16),
            shape((2, layers, tokens, wide // 2), BF16),
            shape((2, layers, tokens, width // 2), BF16),
            shape(x.shape, BF16),
            shape(x.shape, BF16),
            shape((GIVEN, tokens, width), BF16),
        ],
        in_specs=[
            pl.BlockSpec((tokens, width), lambda s, l, j: (0, 0)),
            hbm,
            hbm,
            pl.BlockSpec((1, width, chunk), lambda s, l, j: (l, 0, j)),
            pl.BlockSpec((1, chunk, width), lambda s, l, j: (l, j, 0)),
        ],
        out_specs=[
            pl.BlockSpec((1, 1, tokens, chunk), lambda s, l, j: (s, l, 0, j)),
            pl.BlockSpec((1, 1, tokens, chunk // 2), lambda s, l, j: (s, l, 0, j)),
            pl.BlockSpec((1, 1, tokens, width // 2), lambda s, l, j: (s, l, 0, 0)),
            hbm,
            hbm,
            hbm,
        ],
        scratch_shapes=[
            pltpu.VMEM((tokens, width), BF16),
            pltpu.VMEM((tokens, width), F32),
            pltpu.VMEM((tokens, chunk), BF16),
            pltpu.VMEM((tokens, width), BF16),
            pltpu.VMEM((GIVEN, tokens, width), BF16),
            dma((2 + GIVEN,)),
            dma((2 + GIVEN,)),
            dma,
        ],
        compiler_params=pltpu.CompilerParams(
            collective_id=1, has_side_effects=True, vmem_limit_bytes=VMEM_LIMIT
        ),
        name="forward",
    )(x, x, dy, w_one, w_two)


def backward_body(
    w1, w2, u, a, h, dy_own, dy_nbr,
    tot, dx, last,
    a_cat, du_cat, h_cat, gb_cat, g, w2c, w1c, uc, unit, part0, rcv0, rcv1, rcv2,
    s_rs1, s_rs2, s_ag1, s_ag2, s_ag3, s_fwd, s_own, r_ag1, r_ag2, r_ag3, r_fwd,
    r_rs1, r_rs2, c_rs1, c_rs2, s_rs0, r_rs0, c_rs0,
    l_a, l_gb, l_h, l_w2, l_w1, l_u, l_dx,
    *, layers, tokens, width, wide, rows,
):
    half = wide // 2
    part = rows // 2
    nu = half // rows
    hn = nu // 2
    nm = width // rows
    nf = nu // nm
    chunk = wide // nu
    units = 2 * nu * layers
    pieces = 2 * units
    whole = pieces - 2 * nu
    early = (hn + 1) // 2
    narrow = width // 2
    step = tokens // 2
    z, rest = lax.axis_index("replica"), lax.axis_index("data")
    core, x, y = rest % 2, (rest // 2) % 2, rest // 4

    def choose(axis):
        return (1 - axis) * (2 - axis) // 2, axis * (2 - axis), axis * (axis - 1) // 2

    def peer(axis):
        ex, ey, ez = choose(axis)
        px, py, pz = x + ex * (1 - 2 * x), y + ey * (1 - 2 * y), z + ez * (1 - 2 * z)
        return (pz, (py * 2 + px) * 2 + core)

    sibling = (z, (y * 2 + x) * 2 + 1 - core)

    def send(src, dst, ssem, rsem, to):
        return pltpu.make_async_remote_copy(src_ref=src, dst_ref=dst, send_sem=ssem, recv_sem=rsem, device_id=to, device_id_type=MESH)

    def place(m):
        mid = (m % 3) // 2
        a_axis = (1 - mid) * (m % 3) + mid * ((m // 3) % 2)
        b_axis = 1 - a_axis
        bit_a = x + a_axis * (y - x)
        bit_b = x + b_axis * (y - x)
        own = (1 - mid) * (4 * z + 2 * bit_a + bit_b) + mid * (4 * bit_a + 2 * z + bit_b)
        return mid, a_axis, b_axis, bit_a, bit_b, own

    def rs0(n):
        return send(part0.at[n % PARTS], rcv0.at[n % RECV0], s_rs0.at[n % PARTS], r_rs0.at[n % RECV0], sibling)

    def rs1(m):
        mid, a_axis, b_axis, bit_a, bit_b, own = place(m)
        return send(unit.at[m % SLOTS, pl.ds(2 - 2 * bit_a, 2)], rcv1.at[m % RECV], s_rs1.at[m % SEMS], r_rs1.at[m % RECV], peer(a_axis))

    def rs2(m):
        mid, a_axis, b_axis, bit_a, bit_b, own = place(m)
        return send(unit.at[m % SLOTS, pl.ds(2 * bit_a + 1 - bit_b, 1)], rcv2.at[m % RECV], s_rs2.at[m % SEMS], r_rs2.at[m % RECV], peer(b_axis))

    def own_copy(m):
        mid, a_axis, b_axis, bit_a, bit_b, own = place(m)
        return pltpu.make_async_copy(unit.at[m % SLOTS, pl.ds(2 * bit_a + bit_b, 1)], tot.at[m, core, pl.ds(own, 1)], s_own.at[m % SEMS])

    def last_copy(m):
        mid, a_axis, b_axis, bit_a, bit_b, own = place(m)
        return pltpu.make_async_copy(unit.at[m % SLOTS, pl.ds(2 * bit_a + bit_b, 1)], last.at[pl.ds(m - whole, 1)], s_own.at[m % SEMS])

    def ag1(m):
        mid, a_axis, b_axis, bit_a, bit_b, own = place(m)
        return send(
            unit.at[m % SLOTS, pl.ds(2 * bit_a + bit_b, 1)], tot.at[m, core, pl.ds(own, 1)], s_ag1.at[m % SEMS], r_ag1.at[m % SEMS], peer(b_axis)
        )

    def ag2(m):
        mid, a_axis, b_axis, bit_a, bit_b, own = place(m)
        span = tot.at[m, core, pl.ds(own // 2 * 2, 2)]
        return send(span, span, s_ag2.at[m % SEMS], r_ag2.at[m % SEMS], peer(a_axis + mid * (Z - a_axis)))

    def ag3(m):
        mid, a_axis, b_axis, bit_a, bit_b, own = place(m)
        span = tot.at[m, core, pl.ds(own // 4 * 4, 4)]
        return send(span, span, s_ag3.at[m % SEMS], r_ag3.at[m % SEMS], peer(Z + mid * (a_axis - Z)))

    def fwd(m):
        span = tot.at[m, core]
        return send(span, span, s_fwd.at[m % SEMS], r_fwd.at[m % SEMS], sibling)

    def add(m, block, other):
        unit[m % SLOTS, block] = (unit[m % SLOTS, block].astype(F32) + other.astype(F32)).astype(BF16)

    def credit(sem, n, slots, count, to):
        @pl.when(n + slots < count)
        def _():
            pl.semaphore_signal(sem.at[n % slots], inc=1, device_id=to, device_id_type=MESH)

    def spend(sem, n, slots):
        @pl.when(n >= slots)
        def _():
            pl.semaphore_wait(sem.at[n % slots], 1)

    def live(m):
        return jnp.logical_and(m >= 0, m < pieces)

    def spread_out(m):
        return jnp.logical_and(m >= 0, m < whole)

    def left(m):
        return jnp.logical_and(m >= whole, m < pieces)

    def make(n, theirs, mine):
        part0[n % PARTS] = theirs.reshape(4, rows // 8, width).astype(BF16)
        kept = mine.reshape(4, rows // 8, width).astype(BF16)
        for c in range(2):
            unit[(2 * n + c) % SLOTS] = kept[:, :, c * narrow : (c + 1) * narrow]

    def push(n):
        spend(c_rs0, n, RECV0)
        rs0(n).start()

    def pair_sum(n):
        rs0(n).wait()
        for c in range(2):
            for block in range(4):
                add(2 * n + c, block, rcv0[n % RECV0, block, :, c * narrow : (c + 1) * narrow])
        credit(c_rs0, n, RECV0, units, sibling)

    def comm(r, carry):
        m0, m1, m2, m3, m4, m5 = (r - k * LAG for k in range(6))
        m6 = m5 - LAG

        @pl.when(live(m2))
        def _():
            mid, a_axis, b_axis, bit_a, bit_b, own = place(m2)
            rs2(m2).wait_recv()
            add(m2, 2 * bit_a + bit_b, rcv2[m2 % RECV, 0])
            credit(c_rs2, m2, RECV, pieces, peer(b_axis))
            rs1(m2).wait_send()

        @pl.when(live(m1))
        def _():
            mid, a_axis, b_axis, bit_a, bit_b, own = place(m1)
            rs1(m1).wait_recv()
            add(m1, 2 * bit_a + 1 - bit_b, rcv1[m1 % RECV, 1 - bit_b])
            add(m1, 2 * bit_a + bit_b, rcv1[m1 % RECV, bit_b])
            credit(c_rs1, m1, RECV, pieces, peer(a_axis))

        @pl.when(live(m0))
        def _():
            spend(c_rs1, m0, RECV)
            rs1(m0).start()

        @pl.when(spread_out(m2))
        def _():
            own_copy(m2).start()
            ag1(m2).start()

        @pl.when(left(m2))
        def _():
            last_copy(m2).start()

        @pl.when(live(m1))
        def _():
            spend(c_rs2, m1, RECV)
            rs2(m1).start()

        @pl.when(live(m3))
        def _():
            rs2(m3).wait_send()

        @pl.when(left(m3))
        def _():
            last_copy(m3).wait()

        @pl.when(spread_out(m3))
        def _():
            own_copy(m3).wait()
            ag1(m3).wait()
            ag2(m3).start()

        @pl.when(spread_out(m4))
        def _():
            ag2(m4).wait()
            ag3(m4).start()

        @pl.when(spread_out(m5))
        def _():
            ag3(m5).wait()
            fwd(m5).start()

        @pl.when(spread_out(m6))
        def _():
            fwd(m6).wait()

        return carry

    def rounds(lo, hi):
        lax.fori_loop(lo, hi, comm, 0)

    def ramp(lo, hi, i, n):
        return lo + (hi - lo) * i * i // (n * n)

    sets = (0, 1)
    dys = (dy_own, dy_nbr)

    def of(k):
        return pl.ds(k * tokens, tokens)

    def chunk_at(i):
        late, wait = hn - early, i // (2 * early)
        first = i // early * hn + i % early
        second = early + (i - 2 * early) // late * hn + (i - 2 * early) % late
        return first + wait * (second - first)

    def loads(layer, i):
        f0, slot = pl.multiple_of(chunk_at(i) * chunk, 128), i % 2
        return (
            pltpu.make_async_copy(w2.at[layer, pl.ds(f0, chunk)], w2c.at[slot], l_w2.at[slot]),
            pltpu.make_async_copy(w1.at[layer, :, pl.ds(f0, chunk)], w1c.at[slot], l_w1.at[slot]),
            *(pltpu.make_async_copy(u.at[k, layer, :, pl.ds(f0, chunk)], uc.at[slot, k], l_u.at[slot, k]) for k in sets),
        )

    def cols(i, size):
        return pl.ds(pl.multiple_of(i * size, 128), size)

    def a_load(layer, k):
        return pltpu.make_async_copy(a.at[k, layer], a_cat.at[of(k)], l_a.at[k])

    def h_load(layer, k):
        return pltpu.make_async_copy(h.at[k, layer], h_cat.at[of(k)], l_h.at[k])

    def gb_load(k):
        return pltpu.make_async_copy(dys[k], gb_cat.at[of(k)], l_gb.at[k])

    def dx_store():
        return pltpu.make_async_copy(gb_cat.at[of(0)], dx, l_dx)

    barrier = pltpu.get_barrier_semaphore()
    for to in (peer(X), peer(Y), peer(Z), sibling):
        pl.semaphore_signal(barrier, inc=1, device_id=to, device_id_type=MESH)
    for k in sets:
        gb_load(k).start()
        a_load(layers - 1, k).start()
    for k in sets:
        gb_load(k).wait()
    pl.semaphore_wait(barrier, 4)

    def layer_step(li, carry):
        layer = layers - 1 - li
        base = li * 2 * nu
        late = jnp.minimum(li, 1)
        due = [late * (4 * nu * (li - 1) + PACE[4] * nu // 10)]
        for p, q in zip(PACE_FIRST, PACE):
            due.append(4 * nu * li + p * nu // 10 + late * (q * nu // 10 - p * nu // 10))
        for k in sets:
            a_load(layer, k).wait()

        def second_weight(i, carry):
            n = base + i
            lhs = jnp.concatenate([a_cat[:, cols((1 - core) * nu + i, part)], a_cat[:, cols(core * nu + i, part)]], axis=1)
            out = mm(lhs, gb_cat[...], 0, 0)
            make(n, out[:part], out[part:])

            @pl.when(i >= 2)
            def _():
                pair_sum(n - 2)

            push(n)
            rounds(ramp(due[0], due[1], i, nu), ramp(due[0], due[1], i + 1, nu))
            return carry

        lax.fori_loop(0, nu, second_weight, 0)
        pair_sum(base + nu - 2)
        pair_sum(base + nu - 1)
        for k in sets:
            h_load(layer, k).start()

        @pl.when(li == 0)
        def _():
            for load in loads(layer, 0):
                load.start()
            for k in sets:
                g[of(k)] = gb_cat[of(k)].astype(F32)

        @pl.when(layer > 0)
        def _():
            for k in sets:
                a_load(layer - 1, k).start()

        def hidden_chunk(from_i, to_i, start, stop, i, carry):
            for load in loads(layer, i):
                load.wait()

            @pl.when(i < nu - 1)
            def _():
                for load in loads(layer, i + 1):
                    load.start()

            def token_set(k, carry):
                at = [pl.ds(q * step, step) for q in range(2)]
                rows_q = [pl.ds(pl.multiple_of(k * tokens + q * step, 16), step) for q in range(2)]
                d_act = [mm(gb_cat[r], w2c[i % 2], 1, 1) for r in rows_q]
                for q in range(2):
                    du = (d_act[q] * gelu_slope(uc[i % 2, k, at[q]].astype(F32))).astype(BF16)
                    du_cat[rows_q[q], cols(chunk_at(i), chunk)] = du
                    g[rows_q[q]] += mm(du, w1c[i % 2], 1, 1)
                s = 2 * (i - from_i) + k
                rounds(start + (stop - start) * s // (4 * early), start + (stop - start) * (s + 1) // (4 * early))
                return carry

            lax.fori_loop(0, 2, token_set, 0)
            return carry

        def first_weight(fi, start, stop, mi, carry):
            n = base + nu + fi * nm + mi
            lhs = h_cat[:, cols(mi, part)]
            make(
                n,
                mm(lhs, du_cat[:, cols((1 - core) * nf + fi, width)], 0, 0),
                mm(lhs, du_cat[:, cols(core * nf + fi, width)], 0, 0),
            )

            @pl.when(mi >= 2)
            def _():
                pair_sum(n - 2)

            push(n)
            rounds(ramp(start, stop, mi, nm), ramp(start, stop, mi + 1, nm))
            return carry

        def half_step(fi, carry):
            d0, d1, d2 = (due[k] + fi * (due[k + 2] - due[k]) for k in (1, 2, 3))
            from_i, to_i = fi * 2 * early, 2 * early + fi * (nu - 2 * early)
            lax.fori_loop(from_i, to_i, functools.partial(hidden_chunk, from_i, to_i, d0, d1), 0)
            rounds(d0 + (d1 - d0) * (to_i - from_i) // (2 * early), d1)

            @pl.when(fi == 0)
            def _():
                for k in sets:
                    h_load(layer, k).wait()

            @pl.when(fi == 1)
            def _():
                for k in sets:
                    gb_cat[of(k)] = g[of(k)].astype(BF16)

                @pl.when(layer > 0)
                def _():
                    for load in loads(layer - 1, 0):
                        load.start()

                @pl.when(layer == 0)
                def _():
                    dx_store().start()

            lax.fori_loop(0, nm, functools.partial(first_weight, fi, d1, d2), 0)
            pair_sum(base + nu + fi * nm + nm - 2)
            pair_sum(base + nu + fi * nm + nm - 1)
            return carry

        lax.fori_loop(0, nf, half_step, 0)
        return carry

    lax.fori_loop(0, layers, layer_step, 0)
    rounds(4 * nu * (layers - 1) + PACE[4] * nu // 10, pieces + 4 * LAG)
    dx_store().wait()


def backward(w_one, w_two, u, a, h, dy, dy_nbr, rows):
    layers, width, wide = w_one.shape
    tokens = dy.shape[0]
    half = wide // 2
    nu = half // rows
    chunk = wide // nu
    units = 2 * nu * layers
    dma, reg = pltpu.SemaphoreType.DMA, pltpu.SemaphoreType.REGULAR
    hbm = pl.BlockSpec(memory_space=pl.ANY)
    sub, narrow = rows // 8, width // 2
    shape = jax.ShapeDtypeStruct
    scratch = [
        pltpu.VMEM((2 * tokens, half), BF16),
        pltpu.VMEM((2 * tokens, wide), BF16),
        pltpu.VMEM((2 * tokens, width // 2), BF16),
        pltpu.VMEM((2 * tokens, width), BF16),
        pltpu.VMEM((2 * tokens, width), F32),
        pltpu.VMEM((2, chunk, width), BF16),
        pltpu.VMEM((2, width, chunk), BF16),
        pltpu.VMEM((2, 2, tokens, chunk), BF16),
        pltpu.VMEM((SLOTS, 4, sub, narrow), BF16),
        pltpu.VMEM((PARTS, 4, sub, width), BF16),
        pltpu.VMEM((RECV0, 4, sub, width), BF16),
        pltpu.VMEM((RECV, 2, sub, narrow), BF16),
        pltpu.VMEM((RECV, 1, sub, narrow), BF16),
        *[dma((SEMS,))] * 11,
        *[dma((RECV,))] * 2,
        *[reg((RECV,))] * 2,
        dma((PARTS,)), dma((RECV0,)), reg((RECV0,)),
        dma((2,)), dma((2,)), dma((2,)), dma((2,)), dma((2,)), dma((2, 2)), dma,
    ]
    return pl.pallas_call(
        functools.partial(backward_body, layers=layers, tokens=tokens, width=width, wide=wide, rows=rows),
        out_shape=[
            shape((2 * units - 2 * nu, 2, 8, sub, narrow), BF16),
            shape((tokens, width), BF16),
            shape((2 * nu, sub, narrow), BF16),
        ],
        in_specs=[hbm] * 7,
        out_specs=[hbm] * 3,
        scratch_shapes=scratch,
        compiler_params=pltpu.CompilerParams(collective_id=0, has_side_effects=True, vmem_limit_bytes=VMEM_LIMIT),
        name="backward",
    )(w_one, w_two, u, a, h, dy, dy_nbr)


COPY_SLOTS, COPY_LEAD = 40, 16


def assemble_body(tot, dx_in, one, two, dx, buf, dx_buf, s_in, s_out, s_dx, *, layers, nu, nm, width):
    items = 2 * tot.shape[0]
    narrow = width // 2

    def load(j):
        return pltpu.make_async_copy(tot.at[j // 2, j % 2], buf.at[j % COPY_SLOTS], s_in.at[j % COPY_SLOTS])

    def stores(j, run):
        m, core, slot = j // 2, j % 2, j % COPY_SLOTS
        n, side = m // 2, m % 2
        layer, i = layers - 1 - n // (2 * nu), n % nu
        mid = (m % 3) // 2
        for q in range(4):
            src = (1 - mid) * q + mid * (q % 2 * 2 + q // 2)
            span = buf.at[slot, pl.ds(src * 2, 2)]

            @pl.when((n // nu) % 2 == 0)
            def _():
                cols = pl.ds(pl.multiple_of(side * narrow, 128), narrow)
                run(pltpu.make_async_copy(span, two.at[layer, core * nu + i, pl.ds(2 * q, 2), :, cols], s_out.at[slot, q]))

            @pl.when((n // nu) % 2 == 1)
            def _():
                cols = pl.ds(pl.multiple_of((core * (nu // nm) + i // nm) * width + side * narrow, 128), narrow)
                run(pltpu.make_async_copy(span, one.at[layer, i % nm, pl.ds(2 * q, 2), :, cols], s_out.at[slot, q]))

    def step(j, carry):
        @pl.when(j >= COPY_SLOTS)
        def _():
            stores(j - COPY_SLOTS, lambda c: c.wait())

        @pl.when(j < items)
        def _():
            load(j).start()

        @pl.when(jnp.logical_and(j >= COPY_LEAD, j < items + COPY_LEAD))
        def _():
            load(j - COPY_LEAD).wait()
            stores(j - COPY_LEAD, lambda c: c.start())

        return carry

    dx_load = pltpu.make_async_copy(dx_in, dx_buf, s_dx.at[0])
    dx_store = pltpu.make_async_copy(dx_buf, dx, s_dx.at[1])
    dx_load.start()
    lax.fori_loop(0, COPY_SLOTS, step, 0)
    dx_load.wait()
    dx_store.start()
    lax.fori_loop(COPY_SLOTS, items + COPY_SLOTS, step, 0)
    dx_store.wait()


def finish_body(last, one_in, one, buf, s_in, s_out, *, nm, width, first):
    devices, count = last.shape[:2]
    narrow = width // 2

    def load(d):
        return pltpu.make_async_copy(last.at[d], buf.at[d], s_in.at[d])

    def store(d, p):
        m = first + p
        z, y, x, core = d // 8, d // 4 % 2, d // 2 % 2, d % 2
        mid = (m % 3) // 2
        a_axis = (1 - mid) * (m % 3) + mid * ((m // 3) % 2)
        row = 4 * z + 2 * (x + a_axis * (y - x)) + y + a_axis * (x - y)
        i, side = p // 2, p % 2
        cols = pl.ds(pl.multiple_of((core * 2 + i // nm) * width + side * narrow, 128), narrow)
        return pltpu.make_async_copy(buf.at[d, p], one.at[0, i % nm, row, :, cols], s_out)

    for d in range(devices):
        load(d).start()

    def out(d, carry):
        load(d).wait()
        for p in range(count):
            store(d, p).start()
        return carry

    lax.fori_loop(0, devices, out, 0)

    def done(d, carry):
        for p in range(count):
            store(d, p).wait()
        return carry

    lax.fori_loop(0, devices, done, 0)


def assemble(tot, dx, layers, width, wide, rows):
    nu, nm, sub = wide // 2 // rows, width // rows, rows // 8
    shape = jax.ShapeDtypeStruct
    hbm = pl.BlockSpec(memory_space=pl.ANY)
    return pl.pallas_call(
        functools.partial(assemble_body, layers=layers, nu=nu, nm=nm, width=width),
        out_shape=[shape((layers, nm, 8, sub, wide), BF16), shape((layers, 2 * nu, 8, sub, width), BF16), shape(dx.shape, BF16)],
        in_specs=[hbm] * 2,
        out_specs=[hbm] * 3,
        scratch_shapes=[
            pltpu.VMEM((COPY_SLOTS, 8, sub, width // 2), BF16),
            pltpu.VMEM(dx.shape, BF16),
            pltpu.SemaphoreType.DMA((COPY_SLOTS,)),
            pltpu.SemaphoreType.DMA((COPY_SLOTS, 4)),
            pltpu.SemaphoreType.DMA((2,)),
        ],
        compiler_params=pltpu.CompilerParams(vmem_limit_bytes=VMEM_LIMIT),
        cost_estimate=pl.CostEstimate(flops=400 * tot.size, bytes_accessed=4 * tot.size, transcendentals=0),
        name="assemble",
    )(tot, dx)


def finish(last, one, first, nm, width):
    hbm = pl.BlockSpec(memory_space=pl.ANY)
    return pl.pallas_call(
        functools.partial(finish_body, nm=nm, width=width, first=first),
        out_shape=jax.ShapeDtypeStruct(one.shape, BF16),
        in_specs=[hbm] * 2,
        out_specs=hbm,
        scratch_shapes=[pltpu.VMEM(last.shape, BF16), pltpu.SemaphoreType.DMA((last.shape[0],)), pltpu.SemaphoreType.DMA],
        input_output_aliases={1: 0},
        compiler_params=pltpu.CompilerParams(vmem_limit_bytes=VMEM_LIMIT),
        cost_estimate=pl.CostEstimate(flops=400 * last.size, bytes_accessed=4 * last.size, transcendentals=0),
        name="finish",
    )(last, one)


def solution(mesh, rows=UNIT_ROWS):
    batch_spec = P(AXES)

    def per_device(w_one, w_two, x_loc, dy_loc):
        layers, width, wide = w_one.shape
        x = x_loc.reshape(-1, width)
        dy = dy_loc.reshape(-1, width)
        u, a, h, _, dy_nbr, _ = forward(x, dy, w_one, w_two, rows)
        tot, dx, last = backward(w_one, w_two, u, a, h, dy, dy_nbr, rows)
        everyone = lax.all_gather(last, AXES)
        one, two, dx = assemble(tot, dx, layers, width, wide, rows)
        one = finish(everyone, one, tot.shape[0], width // rows, width)
        return one.reshape(w_one.shape), two.reshape(w_two.shape), dx.reshape(x_loc.shape)

    return jax.shard_map(per_device, mesh=mesh, in_specs=(P(), P(), batch_spec, batch_spec), out_specs=(P(), P(), batch_spec), check_vma=False)
```

```python
import functools

import jax
import jax.numpy as jnp
from jax import lax
from jax.experimental import pallas as pl
from jax.experimental.pallas import tpu as pltpu
from jax.sharding import PartitionSpec as P

AXES = ("replica", "data")
MESH = pl.DeviceIdType.MESH
BF16, F32 = jnp.bfloat16, jnp.float32
VMEM_LIMIT = 67_043_328
C0, C1 = 0.7978845608028654, 0.044715
UNIT_ROWS = 256
LAG = 4
SLOTS, SEMS, RECV, PARTS, RECV0 = 44, 12, 10, 3, 4
PACE_FIRST, PACE = (6, 18, 20, 28, 30), (-2, 12, 16, 26, 30)
X, Y, Z = 0, 1, 2
UP_BLOCKS = 4


def gelu(v):
    half = 0.5 * v
    return half + half * jnp.tanh(v * (C0 + C0 * C1 * (v * v)))


def gelu_slope(v):
    sq = v * v
    t = jnp.tanh(v * (C0 + C0 * C1 * sq))
    return 0.5 + 0.5 * t + v * (1.0 - t * t) * (0.5 * C0 + 1.5 * C0 * C1 * sq)


def mm(lhs, rhs, lhs_dim, rhs_dim):
    return lax.dot_general(lhs, rhs, (((lhs_dim,), (rhs_dim,)), ((), ())), preferred_element_type=F32)


def forward_body(
    x_ref, x, dy, w1_ref, w2_ref, u_ref, a_ref, h_ref, x_nbr, dy_nbr, h_nbr,
    hid, acc, act_s, nxt, made, s_send, s_recv, s_load,
    *, layers, chunks, rows,
):
    tokens_of, layer, j = pl.program_id(0), pl.program_id(1), pl.program_id(2)
    z = lax.axis_index("replica")
    part = rows // 2
    shift = z * part
    other = (1 - z, lax.axis_index("data"))
    tokens = x.shape[0]
    third, most = tokens // 3, tokens // 3 * 2

    def swap(src, dst, k):
        return pltpu.make_async_remote_copy(
            src_ref=src, dst_ref=dst, send_sem=s_send.at[k], recv_sem=s_recv.at[k], device_id=other, device_id_type=MESH
        )

    head, tail = pl.ds(0, third), pl.ds(third, most)
    x_swap = swap(x, x_nbr, 0)
    dy_swap = [swap(dy.at[head], dy_nbr.at[head], 1), swap(dy.at[tail], dy_nbr.at[tail], 2)]
    x_load = pltpu.make_async_copy(x_nbr, nxt, s_load)
    sizes = (most, tokens)
    h_swap = [swap(made.at[k, pl.ds(0, sizes[k])], h_nbr.at[k, pl.ds(0, sizes[k])], 3 + k) for k in range(2)]
    h_load = [pltpu.make_async_copy(h_nbr.at[k, pl.ds(0, sizes[k])], nxt.at[pl.ds(0, sizes[k])], s_load) for k in range(2)]

    def at(s, l, c):
        return pl.when(jnp.logical_and(tokens_of == s, jnp.logical_and(layer == l, j == c)))

    @at(0, 0, 0)
    def _():
        barrier = pltpu.get_barrier_semaphore()
        pl.semaphore_signal(barrier, inc=1, device_id=other, device_id_type=MESH)
        hid[...] = x_ref[...]
        pl.semaphore_wait(barrier, 1)
        x_swap.start()
        dy_swap[0].start()

    for k in range(2):
        block = layers - 2 + k

        @at(0, block, 0)
        def _(k=k):
            h_swap[k].start()

        @at(1, block - 1, chunks - 1)
        def _(k=k):
            h_swap[k].wait_recv()
            h_load[k].start()

        @at(1, block, 0)
        def _(k=k):
            h_load[k].wait()
            hid[: sizes[k]] = nxt[: sizes[k]]

    @at(0, layers - 1, 0)
    def _():
        dy_swap[1].start()
        x_swap.wait()
        x_load.start()

    @at(1, 0, 0)
    def _():
        x_load.wait()
        hid[...] = nxt[...]

    @at(1, layers - 1, chunks - 1)
    def _():
        for copy in h_swap:
            copy.wait_send()
        for copy in dy_swap:
            copy.wait()

    def keep(dst, src):
        for k in range(src.shape[1] // rows):
            dst[0, 0, :, k * part : (k + 1) * part] = src[:, pl.ds(pl.multiple_of(k * rows + shift, part), part)]

    @pl.when(j == 0)
    def _():
        keep(h_ref, hid)
        acc[...] = hid[...].astype(F32)

    def up_only():
        step = hid.shape[0] // UP_BLOCKS
        spans = [slice(k * step, (k + 1) * step) for k in range(UP_BLOCKS)]
        pre = [mm(hid[span], w1_ref[0], 1, 0).astype(BF16) for span in spans]
        for span, p in zip(spans, pre):
            u_ref[0, 0, span] = p
            act_s[span] = gelu(p.astype(F32)).astype(BF16)
        keep(a_ref, act_s)

    full = layer < layers - 1 - 2 * tokens_of
    partly = jnp.logical_and(tokens_of == 1, layer == layers - 3)

    @pl.when(full)
    def _():
        pre = mm(hid[...], w1_ref[0], 1, 0).astype(BF16)
        u_ref[0, 0] = pre
        act = gelu(pre.astype(F32)).astype(BF16)
        act_s[...] = act
        acc[...] += mm(act, w2_ref[0], 1, 0)
        keep(a_ref, act_s)

        @pl.when(j == chunks - 1)
        def _():
            hid[...] = acc[...].astype(BF16)

    @pl.when(jnp.logical_not(full))
    def _():
        up_only()

    @pl.when(partly)
    def _():
        acc[most:] += mm(act_s[most:], w2_ref[0], 1, 0)

        @pl.when(j == chunks - 1)
        def _():
            hid[most:] = acc[most:].astype(BF16)

    for k in range(2):

        @at(0, layers - 3 + k, chunks - 1)
        def _(k=k):
            made[k] = hid[...]


def forward(x, dy, w_one, w_two, rows):
    layers, width, wide = w_one.shape
    tokens = x.shape[0]
    chunk = width
    chunks = wide // chunk
    shape = jax.ShapeDtypeStruct
    hbm = pl.BlockSpec(memory_space=pl.ANY)
    dma = pltpu.SemaphoreType.DMA
    return pl.pallas_call(
        functools.partial(forward_body, layers=layers, chunks=chunks, rows=rows),
        grid=(2, layers, chunks),
        out_shape=[
            shape((2, layers, tokens, wide), BF16),
            shape((2, layers, tokens, wide // 2), BF16),
            shape((2, layers, tokens, width // 2), BF16),
            shape(x.shape, BF16),
            shape(x.shape, BF16),
            shape((2, tokens, width), BF16),
        ],
        in_specs=[
            pl.BlockSpec((tokens, width), lambda s, l, j: (0, 0)),
            hbm,
            hbm,
            pl.BlockSpec((1, width, chunk), lambda s, l, j: (l, 0, j)),
            pl.BlockSpec((1, chunk, width), lambda s, l, j: (l, j, 0)),
        ],
        out_specs=[
            pl.BlockSpec((1, 1, tokens, chunk), lambda s, l, j: (s, l, 0, j)),
            pl.BlockSpec((1, 1, tokens, chunk // 2), lambda s, l, j: (s, l, 0, j)),
            pl.BlockSpec((1, 1, tokens, width // 2), lambda s, l, j: (s, l, 0, 0)),
            hbm,
            hbm,
            hbm,
        ],
        scratch_shapes=[
            pltpu.VMEM((tokens, width), BF16),
            pltpu.VMEM((tokens, width), F32),
            pltpu.VMEM((tokens, chunk), BF16),
            pltpu.VMEM((tokens, width), BF16),
            pltpu.VMEM((2, tokens, width), BF16),
            dma((5,)),
            dma((5,)),
            dma,
        ],
        compiler_params=pltpu.CompilerParams(
            collective_id=1, has_side_effects=True, vmem_limit_bytes=VMEM_LIMIT
        ),
        name="forward",
    )(x, x, dy, w_one, w_two)


def backward_body(
    w1, w2, u, a, h, dy_own, dy_nbr,
    tot, dx, last,
    a_cat, du_cat, h_cat, gb_cat, g, w2c, w1c, uc, unit, part0, rcv0, rcv1, rcv2,
    s_rs1, s_rs2, s_ag1, s_ag2, s_ag3, s_fwd, s_own, r_ag1, r_ag2, r_ag3, r_fwd,
    r_rs1, r_rs2, c_rs1, c_rs2, s_rs0, r_rs0, c_rs0,
    l_a, l_gb, l_h, l_w2, l_w1, l_u, l_dx,
    *, layers, tokens, width, wide, rows,
):
    half = wide // 2
    part = rows // 2
    nu = half // rows
    hn = nu // 2
    nm = width // rows
    nf = nu // nm
    chunk = wide // nu
    units = 2 * nu * layers
    pieces = 2 * units
    whole = pieces - 2 * nu
    early = (hn + 1) // 2
    narrow = width // 2
    step = tokens // 2
    z, rest = lax.axis_index("replica"), lax.axis_index("data")
    core, x, y = rest % 2, (rest // 2) % 2, rest // 4

    def choose(axis):
        return (1 - axis) * (2 - axis) // 2, axis * (2 - axis), axis * (axis - 1) // 2

    def peer(axis):
        ex, ey, ez = choose(axis)
        px, py, pz = x + ex * (1 - 2 * x), y + ey * (1 - 2 * y), z + ez * (1 - 2 * z)
        return (pz, (py * 2 + px) * 2 + core)

    sibling = (z, (y * 2 + x) * 2 + 1 - core)

    def send(src, dst, ssem, rsem, to):
        return pltpu.make_async_remote_copy(src_ref=src, dst_ref=dst, send_sem=ssem, recv_sem=rsem, device_id=to, device_id_type=MESH)

    def place(m):
        mid = (m % 3) // 2
        a_axis = (1 - mid) * (m % 3) + mid * ((m // 3) % 2)
        b_axis = 1 - a_axis
        bit_a = x + a_axis * (y - x)
        bit_b = x + b_axis * (y - x)
        own = (1 - mid) * (4 * z + 2 * bit_a + bit_b) + mid * (4 * bit_a + 2 * z + bit_b)
        return mid, a_axis, b_axis, bit_a, bit_b, own

    def rs0(n):
        return send(part0.at[n % PARTS], rcv0.at[n % RECV0], s_rs0.at[n % PARTS], r_rs0.at[n % RECV0], sibling)

    def rs1(m):
        mid, a_axis, b_axis, bit_a, bit_b, own = place(m)
        return send(unit.at[m % SLOTS, pl.ds(2 - 2 * bit_a, 2)], rcv1.at[m % RECV], s_rs1.at[m % SEMS], r_rs1.at[m % RECV], peer(a_axis))

    def rs2(m):
        mid, a_axis, b_axis, bit_a, bit_b, own = place(m)
        return send(unit.at[m % SLOTS, pl.ds(2 * bit_a + 1 - bit_b, 1)], rcv2.at[m % RECV], s_rs2.at[m % SEMS], r_rs2.at[m % RECV], peer(b_axis))

    def own_copy(m):
        mid, a_axis, b_axis, bit_a, bit_b, own = place(m)
        return pltpu.make_async_copy(unit.at[m % SLOTS, pl.ds(2 * bit_a + bit_b, 1)], tot.at[m, core, pl.ds(own, 1)], s_own.at[m % SEMS])

    def last_copy(m):
        mid, a_axis, b_axis, bit_a, bit_b, own = place(m)
        return pltpu.make_async_copy(unit.at[m % SLOTS, pl.ds(2 * bit_a + bit_b, 1)], last.at[pl.ds(m - whole, 1)], s_own.at[m % SEMS])

    def ag1(m):
        mid, a_axis, b_axis, bit_a, bit_b, own = place(m)
        return send(
            unit.at[m % SLOTS, pl.ds(2 * bit_a + bit_b, 1)], tot.at[m, core, pl.ds(own, 1)], s_ag1.at[m % SEMS], r_ag1.at[m % SEMS], peer(b_axis)
        )

    def ag2(m):
        mid, a_axis, b_axis, bit_a, bit_b, own = place(m)
        span = tot.at[m, core, pl.ds(own // 2 * 2, 2)]
        return send(span, span, s_ag2.at[m % SEMS], r_ag2.at[m % SEMS], peer(a_axis + mid * (Z - a_axis)))

    def ag3(m):
        mid, a_axis, b_axis, bit_a, bit_b, own = place(m)
        span = tot.at[m, core, pl.ds(own // 4 * 4, 4)]
        return send(span, span, s_ag3.at[m % SEMS], r_ag3.at[m % SEMS], peer(Z + mid * (a_axis - Z)))

    def fwd(m):
        span = tot.at[m, core]
        return send(span, span, s_fwd.at[m % SEMS], r_fwd.at[m % SEMS], sibling)

    def add(m, block, other):
        unit[m % SLOTS, block] = (unit[m % SLOTS, block].astype(F32) + other.astype(F32)).astype(BF16)

    def credit(sem, n, slots, count, to):
        @pl.when(n + slots < count)
        def _():
            pl.semaphore_signal(sem.at[n % slots], inc=1, device_id=to, device_id_type=MESH)

    def spend(sem, n, slots):
        @pl.when(n >= slots)
        def _():
            pl.semaphore_wait(sem.at[n % slots], 1)

    def live(m):
        return jnp.logical_and(m >= 0, m < pieces)

    def spread_out(m):
        return jnp.logical_and(m >= 0, m < whole)

    def left(m):
        return jnp.logical_and(m >= whole, m < pieces)

    def make(n, theirs, mine):
        part0[n % PARTS] = theirs.reshape(4, rows // 8, width).astype(BF16)
        kept = mine.reshape(4, rows // 8, width).astype(BF16)
        for c in range(2):
            unit[(2 * n + c) % SLOTS] = kept[:, :, c * narrow : (c + 1) * narrow]

    def push(n):
        spend(c_rs0, n, RECV0)
        rs0(n).start()

    def pair_sum(n):
        rs0(n).wait()
        for c in range(2):
            for block in range(4):
                add(2 * n + c, block, rcv0[n % RECV0, block, :, c * narrow : (c + 1) * narrow])
        credit(c_rs0, n, RECV0, units, sibling)

    def comm(r, carry):
        m0, m1, m2, m3, m4, m5 = (r - k * LAG for k in range(6))
        m6 = m5 - LAG

        @pl.when(live(m2))
        def _():
            mid, a_axis, b_axis, bit_a, bit_b, own = place(m2)
            rs2(m2).wait_recv()
            add(m2, 2 * bit_a + bit_b, rcv2[m2 % RECV, 0])
            credit(c_rs2, m2, RECV, pieces, peer(b_axis))
            rs1(m2).wait_send()

        @pl.when(live(m1))
        def _():
            mid, a_axis, b_axis, bit_a, bit_b, own = place(m1)
            rs1(m1).wait_recv()
            add(m1, 2 * bit_a + 1 - bit_b, rcv1[m1 % RECV, 1 - bit_b])
            add(m1, 2 * bit_a + bit_b, rcv1[m1 % RECV, bit_b])
            credit(c_rs1, m1, RECV, pieces, peer(a_axis))

        @pl.when(live(m0))
        def _():
            spend(c_rs1, m0, RECV)
            rs1(m0).start()

        @pl.when(spread_out(m2))
        def _():
            own_copy(m2).start()
            ag1(m2).start()

        @pl.when(left(m2))
        def _():
            last_copy(m2).start()

        @pl.when(live(m1))
        def _():
            spend(c_rs2, m1, RECV)
            rs2(m1).start()

        @pl.when(live(m3))
        def _():
            rs2(m3).wait_send()

        @pl.when(left(m3))
        def _():
            last_copy(m3).wait()

        @pl.when(spread_out(m3))
        def _():
            own_copy(m3).wait()
            ag1(m3).wait()
            ag2(m3).start()

        @pl.when(spread_out(m4))
        def _():
            ag2(m4).wait()
            ag3(m4).start()

        @pl.when(spread_out(m5))
        def _():
            ag3(m5).wait()
            fwd(m5).start()

        @pl.when(spread_out(m6))
        def _():
            fwd(m6).wait()

        return carry

    def rounds(lo, hi):
        lax.fori_loop(lo, hi, comm, 0)

    def ramp(lo, hi, i, n):
        return lo + (hi - lo) * i * i // (n * n)

    sets = (0, 1)
    dys = (dy_own, dy_nbr)

    def of(k):
        return pl.ds(k * tokens, tokens)

    def chunk_at(i):
        late, wait = hn - early, i // (2 * early)
        first = i // early * hn + i % early
        second = early + (i - 2 * early) // late * hn + (i - 2 * early) % late
        return first + wait * (second - first)

    def loads(layer, i):
        f0, slot = pl.multiple_of(chunk_at(i) * chunk, 128), i % 2
        return (
            pltpu.make_async_copy(w2.at[layer, pl.ds(f0, chunk)], w2c.at[slot], l_w2.at[slot]),
            pltpu.make_async_copy(w1.at[layer, :, pl.ds(f0, chunk)], w1c.at[slot], l_w1.at[slot]),
            *(pltpu.make_async_copy(u.at[k, layer, :, pl.ds(f0, chunk)], uc.at[slot, k], l_u.at[slot, k]) for k in sets),
        )

    def cols(i, size):
        return pl.ds(pl.multiple_of(i * size, 128), size)

    def a_load(layer, k):
        return pltpu.make_async_copy(a.at[k, layer], a_cat.at[of(k)], l_a.at[k])

    def h_load(layer, k):
        return pltpu.make_async_copy(h.at[k, layer], h_cat.at[of(k)], l_h.at[k])

    def gb_load(k):
        return pltpu.make_async_copy(dys[k], gb_cat.at[of(k)], l_gb.at[k])

    def dx_store():
        return pltpu.make_async_copy(gb_cat.at[of(0)], dx, l_dx)

    barrier = pltpu.get_barrier_semaphore()
    for to in (peer(X), peer(Y), peer(Z), sibling):
        pl.semaphore_signal(barrier, inc=1, device_id=to, device_id_type=MESH)
    for k in sets:
        gb_load(k).start()
        a_load(layers - 1, k).start()
    for k in sets:
        gb_load(k).wait()
    pl.semaphore_wait(barrier, 4)

    def layer_step(li, carry):
        layer = layers - 1 - li
        base = li * 2 * nu
        late = jnp.minimum(li, 1)
        due = [late * (4 * nu * (li - 1) + PACE[4] * nu // 10)]
        for p, q in zip(PACE_FIRST, PACE):
            due.append(4 * nu * li + p * nu // 10 + late * (q * nu // 10 - p * nu // 10))
        for k in sets:
            a_load(layer, k).wait()

        def second_weight(i, carry):
            n = base + i
            lhs = jnp.concatenate([a_cat[:, cols((1 - core) * nu + i, part)], a_cat[:, cols(core * nu + i, part)]], axis=1)
            out = mm(lhs, gb_cat[...], 0, 0)
            make(n, out[:part], out[part:])

            @pl.when(i >= 2)
            def _():
                pair_sum(n - 2)

            push(n)
            rounds(ramp(due[0], due[1], i, nu), ramp(due[0], due[1], i + 1, nu))
            return carry

        lax.fori_loop(0, nu, second_weight, 0)
        pair_sum(base + nu - 2)
        pair_sum(base + nu - 1)
        for k in sets:
            h_load(layer, k).start()

        @pl.when(li == 0)
        def _():
            for load in loads(layer, 0):
                load.start()
            for k in sets:
                g[of(k)] = gb_cat[of(k)].astype(F32)

        @pl.when(layer > 0)
        def _():
            for k in sets:
                a_load(layer - 1, k).start()

        def hidden_chunk(from_i, to_i, start, stop, i, carry):
            for load in loads(layer, i):
                load.wait()

            @pl.when(i < nu - 1)
            def _():
                for load in loads(layer, i + 1):
                    load.start()

            def token_set(k, carry):
                at = [pl.ds(q * step, step) for q in range(2)]
                rows_q = [pl.ds(pl.multiple_of(k * tokens + q * step, 16), step) for q in range(2)]
                d_act = [mm(gb_cat[r], w2c[i % 2], 1, 1) for r in rows_q]
                for q in range(2):
                    du = (d_act[q] * gelu_slope(uc[i % 2, k, at[q]].astype(F32))).astype(BF16)
                    du_cat[rows_q[q], cols(chunk_at(i), chunk)] = du
                    g[rows_q[q]] += mm(du, w1c[i % 2], 1, 1)
                s = 2 * (i - from_i) + k
                rounds(start + (stop - start) * s // (4 * early), start + (stop - start) * (s + 1) // (4 * early))
                return carry

            lax.fori_loop(0, 2, token_set, 0)
            return carry

        def first_weight(fi, start, stop, mi, carry):
            n = base + nu + fi * nm + mi
            lhs = h_cat[:, cols(mi, part)]
            make(
                n,
                mm(lhs, du_cat[:, cols((1 - core) * nf + fi, width)], 0, 0),
                mm(lhs, du_cat[:, cols(core * nf + fi, width)], 0, 0),
            )

            @pl.when(mi >= 2)
            def _():
                pair_sum(n - 2)

            push(n)
            rounds(ramp(start, stop, mi, nm), ramp(start, stop, mi + 1, nm))
            return carry

        def half_step(fi, carry):
            d0, d1, d2 = (due[k] + fi * (due[k + 2] - due[k]) for k in (1, 2, 3))
            from_i, to_i = fi * 2 * early, 2 * early + fi * (nu - 2 * early)
            lax.fori_loop(from_i, to_i, functools.partial(hidden_chunk, from_i, to_i, d0, d1), 0)
            rounds(d0 + (d1 - d0) * (to_i - from_i) // (2 * early), d1)

            @pl.when(fi == 0)
            def _():
                for k in sets:
                    h_load(layer, k).wait()

            @pl.when(fi == 1)
            def _():
                for k in sets:
                    gb_cat[of(k)] = g[of(k)].astype(BF16)

                @pl.when(layer > 0)
                def _():
                    for load in loads(layer - 1, 0):
                        load.start()

                @pl.when(layer == 0)
                def _():
                    dx_store().start()

            lax.fori_loop(0, nm, functools.partial(first_weight, fi, d1, d2), 0)
            pair_sum(base + nu + fi * nm + nm - 2)
            pair_sum(base + nu + fi * nm + nm - 1)
            return carry

        lax.fori_loop(0, nf, half_step, 0)
        return carry

    lax.fori_loop(0, layers, layer_step, 0)
    rounds(4 * nu * (layers - 1) + PACE[4] * nu // 10, pieces + 4 * LAG)
    dx_store().wait()


def backward(w_one, w_two, u, a, h, dy, dy_nbr, rows):
    layers, width, wide = w_one.shape
    tokens = dy.shape[0]
    half = wide // 2
    nu = half // rows
    chunk = wide // nu
    units = 2 * nu * layers
    dma, reg = pltpu.SemaphoreType.DMA, pltpu.SemaphoreType.REGULAR
    hbm = pl.BlockSpec(memory_space=pl.ANY)
    sub, narrow = rows // 8, width // 2
    shape = jax.ShapeDtypeStruct
    scratch = [
        pltpu.VMEM((2 * tokens, half), BF16),
        pltpu.VMEM((2 * tokens, wide), BF16),
        pltpu.VMEM((2 * tokens, width // 2), BF16),
        pltpu.VMEM((2 * tokens, width), BF16),
        pltpu.VMEM((2 * tokens, width), F32),
        pltpu.VMEM((2, chunk, width), BF16),
        pltpu.VMEM((2, width, chunk), BF16),
        pltpu.VMEM((2, 2, tokens, chunk), BF16),
        pltpu.VMEM((SLOTS, 4, sub, narrow), BF16),
        pltpu.VMEM((PARTS, 4, sub, width), BF16),
        pltpu.VMEM((RECV0, 4, sub, width), BF16),
        pltpu.VMEM((RECV, 2, sub, narrow), BF16),
        pltpu.VMEM((RECV, 1, sub, narrow), BF16),
        *[dma((SEMS,))] * 11,
        *[dma((RECV,))] * 2,
        *[reg((RECV,))] * 2,
        dma((PARTS,)), dma((RECV0,)), reg((RECV0,)),
        dma((2,)), dma((2,)), dma((2,)), dma((2,)), dma((2,)), dma((2, 2)), dma,
    ]
    return pl.pallas_call(
        functools.partial(backward_body, layers=layers, tokens=tokens, width=width, wide=wide, rows=rows),
        out_shape=[
            shape((2 * units - 2 * nu, 2, 8, sub, narrow), BF16),
            shape((tokens, width), BF16),
            shape((2 * nu, sub, narrow), BF16),
        ],
        in_specs=[hbm] * 7,
        out_specs=[hbm] * 3,
        scratch_shapes=scratch,
        compiler_params=pltpu.CompilerParams(collective_id=0, has_side_effects=True, vmem_limit_bytes=VMEM_LIMIT),
        name="backward",
    )(w_one, w_two, u, a, h, dy, dy_nbr)


COPY_SLOTS, COPY_LEAD = 40, 16


def assemble_body(tot, dx_in, one, two, dx, buf, dx_buf, s_in, s_out, s_dx, *, layers, nu, nm, width):
    items = 2 * tot.shape[0]
    narrow = width // 2

    def load(j):
        return pltpu.make_async_copy(tot.at[j // 2, j % 2], buf.at[j % COPY_SLOTS], s_in.at[j % COPY_SLOTS])

    def stores(j, run):
        m, core, slot = j // 2, j % 2, j % COPY_SLOTS
        n, side = m // 2, m % 2
        layer, i = layers - 1 - n // (2 * nu), n % nu
        mid = (m % 3) // 2
        for q in range(4):
            src = (1 - mid) * q + mid * (q % 2 * 2 + q // 2)
            span = buf.at[slot, pl.ds(src * 2, 2)]

            @pl.when((n // nu) % 2 == 0)
            def _():
                cols = pl.ds(pl.multiple_of(side * narrow, 128), narrow)
                run(pltpu.make_async_copy(span, two.at[layer, core * nu + i, pl.ds(2 * q, 2), :, cols], s_out.at[slot, q]))

            @pl.when((n // nu) % 2 == 1)
            def _():
                cols = pl.ds(pl.multiple_of((core * (nu // nm) + i // nm) * width + side * narrow, 128), narrow)
                run(pltpu.make_async_copy(span, one.at[layer, i % nm, pl.ds(2 * q, 2), :, cols], s_out.at[slot, q]))

    def step(j, carry):
        @pl.when(j >= COPY_SLOTS)
        def _():
            stores(j - COPY_SLOTS, lambda c: c.wait())

        @pl.when(j < items)
        def _():
            load(j).start()

        @pl.when(jnp.logical_and(j >= COPY_LEAD, j < items + COPY_LEAD))
        def _():
            load(j - COPY_LEAD).wait()
            stores(j - COPY_LEAD, lambda c: c.start())

        return carry

    dx_load = pltpu.make_async_copy(dx_in, dx_buf, s_dx.at[0])
    dx_store = pltpu.make_async_copy(dx_buf, dx, s_dx.at[1])
    dx_load.start()
    lax.fori_loop(0, COPY_SLOTS, step, 0)
    dx_load.wait()
    dx_store.start()
    lax.fori_loop(COPY_SLOTS, items + COPY_SLOTS, step, 0)
    dx_store.wait()


def finish_body(last, one_in, one, buf, s_in, s_out, *, nm, width, first):
    devices, count = last.shape[:2]
    narrow = width // 2

    def load(d):
        return pltpu.make_async_copy(last.at[d], buf.at[d], s_in.at[d])

    def store(d, p):
        m = first + p
        z, y, x, core = d // 8, d // 4 % 2, d // 2 % 2, d % 2
        mid = (m % 3) // 2
        a_axis = (1 - mid) * (m % 3) + mid * ((m // 3) % 2)
        row = 4 * z + 2 * (x + a_axis * (y - x)) + y + a_axis * (x - y)
        i, side = p // 2, p % 2
        cols = pl.ds(pl.multiple_of((core * 2 + i // nm) * width + side * narrow, 128), narrow)
        return pltpu.make_async_copy(buf.at[d, p], one.at[0, i % nm, row, :, cols], s_out)

    for d in range(devices):
        load(d).start()

    def out(d, carry):
        load(d).wait()
        for p in range(count):
            store(d, p).start()
        return carry

    lax.fori_loop(0, devices, out, 0)

    def done(d, carry):
        for p in range(count):
            store(d, p).wait()
        return carry

    lax.fori_loop(0, devices, done, 0)


def assemble(tot, dx, layers, width, wide, rows):
    nu, nm, sub = wide // 2 // rows, width // rows, rows // 8
    shape = jax.ShapeDtypeStruct
    hbm = pl.BlockSpec(memory_space=pl.ANY)
    return pl.pallas_call(
        functools.partial(assemble_body, layers=layers, nu=nu, nm=nm, width=width),
        out_shape=[shape((layers, nm, 8, sub, wide), BF16), shape((layers, 2 * nu, 8, sub, width), BF16), shape(dx.shape, BF16)],
        in_specs=[hbm] * 2,
        out_specs=[hbm] * 3,
        scratch_shapes=[
            pltpu.VMEM((COPY_SLOTS, 8, sub, width // 2), BF16),
            pltpu.VMEM(dx.shape, BF16),
            pltpu.SemaphoreType.DMA((COPY_SLOTS,)),
            pltpu.SemaphoreType.DMA((COPY_SLOTS, 4)),
            pltpu.SemaphoreType.DMA((2,)),
        ],
        compiler_params=pltpu.CompilerParams(vmem_limit_bytes=VMEM_LIMIT),
        cost_estimate=pl.CostEstimate(flops=400 * tot.size, bytes_accessed=4 * tot.size, transcendentals=0),
        name="assemble",
    )(tot, dx)


def finish(last, one, first, nm, width):
    hbm = pl.BlockSpec(memory_space=pl.ANY)
    return pl.pallas_call(
        functools.partial(finish_body, nm=nm, width=width, first=first),
        out_shape=jax.ShapeDtypeStruct(one.shape, BF16),
        in_specs=[hbm] * 2,
        out_specs=hbm,
        scratch_shapes=[pltpu.VMEM(last.shape, BF16), pltpu.SemaphoreType.DMA((last.shape[0],)), pltpu.SemaphoreType.DMA],
        input_output_aliases={1: 0},
        compiler_params=pltpu.CompilerParams(vmem_limit_bytes=VMEM_LIMIT),
        cost_estimate=pl.CostEstimate(flops=400 * last.size, bytes_accessed=4 * last.size, transcendentals=0),
        name="finish",
    )(last, one)


def solution(mesh, rows=UNIT_ROWS):
    batch_spec = P(AXES)

    def per_device(w_one, w_two, x_loc, dy_loc):
        layers, width, wide = w_one.shape
        x = x_loc.reshape(-1, width)
        dy = dy_loc.reshape(-1, width)
        u, a, h, _, dy_nbr, _ = forward(x, dy, w_one, w_two, rows)
        tot, dx, last = backward(w_one, w_two, u, a, h, dy, dy_nbr, rows)
        everyone = lax.all_gather(last, AXES)
        one, two, dx = assemble(tot, dx, layers, width, wide, rows)
        one = finish(everyone, one, tot.shape[0], width // rows, width)
        return one.reshape(w_one.shape), two.reshape(w_two.shape), dx.reshape(x_loc.shape)

    return jax.shard_map(per_device, mesh=mesh, in_specs=(P(), P(), batch_spec, batch_spec), out_specs=(P(), P(), batch_spec), check_vma=False)
```

```python
import functools

import jax
import jax.numpy as jnp
from jax import lax
from jax.experimental import pallas as pl
from jax.experimental.pallas import tpu as pltpu
from jax.sharding import PartitionSpec as P

AXES = ("replica", "data")
MESH = pl.DeviceIdType.MESH
BF16, F32 = jnp.bfloat16, jnp.float32
VMEM_LIMIT = 67_043_328
C0, C1 = 0.7978845608028654, 0.044715
UNIT_ROWS = 256
LAG = 4
SLOTS, SEMS, RECV, PARTS, RECV0 = 44, 12, 10, 3, 4
PACE_FIRST, PACE = (6, 18, 20, 28, 32), (2, 16, 18, 28, 32)
X, Y, Z = 0, 1, 2
UP_BLOCKS = 4


def gelu(v):
    half = 0.5 * v
    return half + half * jnp.tanh(v * (C0 + C0 * C1 * (v * v)))


def gelu_slope(v):
    sq = v * v
    t = jnp.tanh(v * (C0 + C0 * C1 * sq))
    return 0.5 + 0.5 * t + v * (1.0 - t * t) * (0.5 * C0 + 1.5 * C0 * C1 * sq)


def mm(lhs, rhs, lhs_dim, rhs_dim):
    return lax.dot_general(lhs, rhs, (((lhs_dim,), (rhs_dim,)), ((), ())), preferred_element_type=F32)


def forward_body(
    x_ref, x, dy, w1_ref, w2_ref, u_ref, a_ref, h_ref, x_nbr, dy_nbr, h_nbr,
    hid, acc, act_s, nxt, made, s_send, s_recv, s_load,
    *, layers, chunks, rows,
):
    tokens_of, layer, j = pl.program_id(0), pl.program_id(1), pl.program_id(2)
    z = lax.axis_index("replica")
    part = rows // 2
    shift = z * part
    other = (1 - z, lax.axis_index("data"))
    tokens = x.shape[0]
    third, most = tokens // 3, tokens // 3 * 2

    def swap(src, dst, k):
        return pltpu.make_async_remote_copy(
            src_ref=src, dst_ref=dst, send_sem=s_send.at[k], recv_sem=s_recv.at[k], device_id=other, device_id_type=MESH
        )

    head, tail = pl.ds(0, third), pl.ds(third, most)
    x_swap = swap(x, x_nbr, 0)
    dy_swap = [swap(dy.at[head], dy_nbr.at[head], 1), swap(dy.at[tail], dy_nbr.at[tail], 2)]
    x_load = pltpu.make_async_copy(x_nbr, nxt, s_load)
    sizes = (most, tokens)
    h_swap = [swap(made.at[k, pl.ds(0, sizes[k])], h_nbr.at[k, pl.ds(0, sizes[k])], 3 + k) for k in range(2)]
    h_load = [pltpu.make_async_copy(h_nbr.at[k, pl.ds(0, sizes[k])], nxt.at[pl.ds(0, sizes[k])], s_load) for k in range(2)]

    def at(s, l, c):
        return pl.when(jnp.logical_and(tokens_of == s, jnp.logical_and(layer == l, j == c)))

    @at(0, 0, 0)
    def _():
        barrier = pltpu.get_barrier_semaphore()
        pl.semaphore_signal(barrier, inc=1, device_id=other, device_id_type=MESH)
        hid[...] = x_ref[...]
        pl.semaphore_wait(barrier, 1)
        x_swap.start()
        dy_swap[0].start()

    for k in range(2):
        block = layers - 2 + k

        @at(0, block, 0)
        def _(k=k):
            h_swap[k].start()

        @at(1, block - 1, chunks - 1)
        def _(k=k):
            h_swap[k].wait_recv()
            h_load[k].start()

        @at(1, block, 0)
        def _(k=k):
            h_load[k].wait()
            hid[: sizes[k]] = nxt[: sizes[k]]

    @at(0, layers - 1, 0)
    def _():
        dy_swap[1].start()
        x_swap.wait()
        x_load.start()

    @at(1, 0, 0)
    def _():
        x_load.wait()
        hid[...] = nxt[...]

    @at(1, layers - 1, chunks - 1)
    def _():
        for copy in h_swap:
            copy.wait_send()
        for copy in dy_swap:
            copy.wait()

    def keep(dst, src):
        for k in range(src.shape[1] // rows):
            dst[0, 0, :, k * part : (k + 1) * part] = src[:, pl.ds(pl.multiple_of(k * rows + shift, part), part)]

    full = layer < layers - 1 - 2 * tokens_of
    partly = jnp.logical_and(tokens_of == 1, layer == layers - 3)

    @pl.when(j == 0)
    def _():
        keep(h_ref, hid)

        @pl.when(jnp.logical_or(full, partly))
        def _():
            acc[...] = hid[...].astype(F32)

    def up_only():
        step = hid.shape[0] // UP_BLOCKS
        spans = [slice(k * step, (k + 1) * step) for k in range(UP_BLOCKS)]
        pre = [mm(hid[span], w1_ref[0], 1, 0).astype(BF16) for span in spans]
        for span, p in zip(spans, pre):
            u_ref[0, 0, span] = p
            act_s[span] = gelu(p.astype(F32)).astype(BF16)
        keep(a_ref, act_s)

    @pl.when(full)
    def _():
        pre = mm(hid[...], w1_ref[0], 1, 0).astype(BF16)
        u_ref[0, 0] = pre
        act = gelu(pre.astype(F32)).astype(BF16)
        act_s[...] = act
        acc[...] += mm(act, w2_ref[0], 1, 0)
        keep(a_ref, act_s)

        @pl.when(j == chunks - 1)
        def _():
            hid[...] = acc[...].astype(BF16)

    @pl.when(jnp.logical_not(full))
    def _():
        up_only()

    @pl.when(partly)
    def _():
        acc[most:] += mm(act_s[most:], w2_ref[0], 1, 0)

        @pl.when(j == chunks - 1)
        def _():
            hid[most:] = acc[most:].astype(BF16)

    for k in range(2):

        @at(0, layers - 3 + k, chunks - 1)
        def _(k=k):
            made[k] = hid[...]


def forward(x, dy, w_one, w_two, rows):
    layers, width, wide = w_one.shape
    tokens = x.shape[0]
    chunk = width
    chunks = wide // chunk
    shape = jax.ShapeDtypeStruct
    hbm = pl.BlockSpec(memory_space=pl.ANY)
    dma = pltpu.SemaphoreType.DMA
    return pl.pallas_call(
        functools.partial(forward_body, layers=layers, chunks=chunks, rows=rows),
        grid=(2, layers, chunks),
        out_shape=[
            shape((2, layers, tokens, wide), BF16),
            shape((2, layers, tokens, wide // 2), BF16),
            shape((2, layers, tokens, width // 2), BF16),
            shape(x.shape, BF16),
            shape(x.shape, BF16),
            shape((2, tokens, width), BF16),
        ],
        in_specs=[
            pl.BlockSpec((tokens, width), lambda s, l, j: (0, 0)),
            hbm,
            hbm,
            pl.BlockSpec((1, width, chunk), lambda s, l, j: (l, 0, j)),
            pl.BlockSpec((1, chunk, width), lambda s, l, j: (l, j, 0)),
        ],
        out_specs=[
            pl.BlockSpec((1, 1, tokens, chunk), lambda s, l, j: (s, l, 0, j)),
            pl.BlockSpec((1, 1, tokens, chunk // 2), lambda s, l, j: (s, l, 0, j)),
            pl.BlockSpec((1, 1, tokens, width // 2), lambda s, l, j: (s, l, 0, 0)),
            hbm,
            hbm,
            hbm,
        ],
        scratch_shapes=[
            pltpu.VMEM((tokens, width), BF16),
            pltpu.VMEM((tokens, width), F32),
            pltpu.VMEM((tokens, chunk), BF16),
            pltpu.VMEM((tokens, width), BF16),
            pltpu.VMEM((2, tokens, width), BF16),
            dma((5,)),
            dma((5,)),
            dma,
        ],
        compiler_params=pltpu.CompilerParams(
            collective_id=1, has_side_effects=True, vmem_limit_bytes=VMEM_LIMIT
        ),
        name="forward",
    )(x, x, dy, w_one, w_two)


def backward_body(
    w1, w2, u, a, h, dy_own, dy_nbr,
    tot, dx, last,
    a_cat, du_cat, h_cat, gb_cat, g, w2c, w1c, uc, unit, part0, rcv0, rcv1, rcv2,
    s_rs1, s_rs2, s_ag1, s_ag2, s_ag3, s_fwd, s_own, r_ag1, r_ag2, r_ag3, r_fwd,
    r_rs1, r_rs2, c_rs1, c_rs2, s_rs0, r_rs0, c_rs0,
    l_a, l_gb, l_h, l_w2, l_w1, l_u, l_dx,
    *, layers, tokens, width, wide, rows,
):
    half = wide // 2
    part = rows // 2
    nu = half // rows
    hn = nu // 2
    nm = width // rows
    nf = nu // nm
    chunk = wide // nu
    units = 2 * nu * layers
    pieces = 2 * units
    whole = pieces - 2 * nu
    early = (hn + 1) // 2
    narrow = width // 2
    step = tokens // 2
    z, rest = lax.axis_index("replica"), lax.axis_index("data")
    core, x, y = rest % 2, (rest // 2) % 2, rest // 4

    def choose(axis):
        return (1 - axis) * (2 - axis) // 2, axis * (2 - axis), axis * (axis - 1) // 2

    def peer(axis):
        ex, ey, ez = choose(axis)
        px, py, pz = x + ex * (1 - 2 * x), y + ey * (1 - 2 * y), z + ez * (1 - 2 * z)
        return (pz, (py * 2 + px) * 2 + core)

    sibling = (z, (y * 2 + x) * 2 + 1 - core)

    def send(src, dst, ssem, rsem, to):
        return pltpu.make_async_remote_copy(src_ref=src, dst_ref=dst, send_sem=ssem, recv_sem=rsem, device_id=to, device_id_type=MESH)

    def place(m):
        mid = (m % 3) // 2
        a_axis = (1 - mid) * (m % 3) + mid * ((m // 3) % 2)
        b_axis = 1 - a_axis
        bit_a = x + a_axis * (y - x)
        bit_b = x + b_axis * (y - x)
        own = (1 - mid) * (4 * z + 2 * bit_a + bit_b) + mid * (4 * bit_a + 2 * z + bit_b)
        return mid, a_axis, b_axis, bit_a, bit_b, own

    def rs0(n):
        return send(part0.at[n % PARTS], rcv0.at[n % RECV0], s_rs0.at[n % PARTS], r_rs0.at[n % RECV0], sibling)

    def rs1(m):
        mid, a_axis, b_axis, bit_a, bit_b, own = place(m)
        return send(unit.at[m % SLOTS, pl.ds(2 - 2 * bit_a, 2)], rcv1.at[m % RECV], s_rs1.at[m % SEMS], r_rs1.at[m % RECV], peer(a_axis))

    def rs2(m):
        mid, a_axis, b_axis, bit_a, bit_b, own = place(m)
        return send(unit.at[m % SLOTS, pl.ds(2 * bit_a + 1 - bit_b, 1)], rcv2.at[m % RECV], s_rs2.at[m % SEMS], r_rs2.at[m % RECV], peer(b_axis))

    def own_copy(m):
        mid, a_axis, b_axis, bit_a, bit_b, own = place(m)
        return pltpu.make_async_copy(unit.at[m % SLOTS, pl.ds(2 * bit_a + bit_b, 1)], tot.at[m, core, pl.ds(own, 1)], s_own.at[m % SEMS])

    def last_copy(m):
        mid, a_axis, b_axis, bit_a, bit_b, own = place(m)
        return pltpu.make_async_copy(unit.at[m % SLOTS, pl.ds(2 * bit_a + bit_b, 1)], last.at[pl.ds(m - whole, 1)], s_own.at[m % SEMS])

    def ag1(m):
        mid, a_axis, b_axis, bit_a, bit_b, own = place(m)
        return send(
            unit.at[m % SLOTS, pl.ds(2 * bit_a + bit_b, 1)], tot.at[m, core, pl.ds(own, 1)], s_ag1.at[m % SEMS], r_ag1.at[m % SEMS], peer(b_axis)
        )

    def ag2(m):
        mid, a_axis, b_axis, bit_a, bit_b, own = place(m)
        span = tot.at[m, core, pl.ds(own // 2 * 2, 2)]
        return send(span, span, s_ag2.at[m % SEMS], r_ag2.at[m % SEMS], peer(a_axis + mid * (Z - a_axis)))

    def ag3(m):
        mid, a_axis, b_axis, bit_a, bit_b, own = place(m)
        span = tot.at[m, core, pl.ds(own // 4 * 4, 4)]
        return send(span, span, s_ag3.at[m % SEMS], r_ag3.at[m % SEMS], peer(Z + mid * (a_axis - Z)))

    def fwd(m):
        span = tot.at[m, core]
        return send(span, span, s_fwd.at[m % SEMS], r_fwd.at[m % SEMS], sibling)

    def add(m, block, other):
        unit[m % SLOTS, block] = (unit[m % SLOTS, block].astype(F32) + other.astype(F32)).astype(BF16)

    def credit(sem, n, slots, count, to):
        @pl.when(n + slots < count)
        def _():
            pl.semaphore_signal(sem.at[n % slots], inc=1, device_id=to, device_id_type=MESH)

    def spend(sem, n, slots):
        @pl.when(n >= slots)
        def _():
            pl.semaphore_wait(sem.at[n % slots], 1)

    def live(m):
        return jnp.logical_and(m >= 0, m < pieces)

    def spread_out(m):
        return jnp.logical_and(m >= 0, m < whole)

    def left(m):
        return jnp.logical_and(m >= whole, m < pieces)

    def make(n, theirs, mine):
        part0[n % PARTS] = theirs.reshape(4, rows // 8, width).astype(BF16)
        kept = mine.reshape(4, rows // 8, width).astype(BF16)
        for c in range(2):
            unit[(2 * n + c) % SLOTS] = kept[:, :, c * narrow : (c + 1) * narrow]

    def push(n):
        spend(c_rs0, n, RECV0)
        rs0(n).start()

    def pair_sum(n):
        rs0(n).wait()
        for c in range(2):
            for block in range(4):
                add(2 * n + c, block, rcv0[n % RECV0, block, :, c * narrow : (c + 1) * narrow])
        credit(c_rs0, n, RECV0, units, sibling)

    def comm(r, carry):
        m0, m1, m2, m3, m4, m5 = (r - k * LAG for k in range(6))
        m6 = m5 - LAG

        @pl.when(live(m2))
        def _():
            mid, a_axis, b_axis, bit_a, bit_b, own = place(m2)
            rs2(m2).wait_recv()
            add(m2, 2 * bit_a + bit_b, rcv2[m2 % RECV, 0])
            credit(c_rs2, m2, RECV, pieces, peer(b_axis))
            rs1(m2).wait_send()

        @pl.when(live(m1))
        def _():
            mid, a_axis, b_axis, bit_a, bit_b, own = place(m1)
            rs1(m1).wait_recv()
            add(m1, 2 * bit_a + 1 - bit_b, rcv1[m1 % RECV, 1 - bit_b])
            add(m1, 2 * bit_a + bit_b, rcv1[m1 % RECV, bit_b])
            credit(c_rs1, m1, RECV, pieces, peer(a_axis))

        @pl.when(live(m0))
        def _():
            spend(c_rs1, m0, RECV)
            rs1(m0).start()

        @pl.when(spread_out(m2))
        def _():
            own_copy(m2).start()
            ag1(m2).start()

        @pl.when(left(m2))
        def _():
            last_copy(m2).start()

        @pl.when(live(m1))
        def _():
            spend(c_rs2, m1, RECV)
            rs2(m1).start()

        @pl.when(live(m3))
        def _():
            rs2(m3).wait_send()

        @pl.when(left(m3))
        def _():
            last_copy(m3).wait()

        @pl.when(spread_out(m3))
        def _():
            own_copy(m3).wait()
            ag1(m3).wait()
            ag2(m3).start()

        @pl.when(spread_out(m4))
        def _():
            ag2(m4).wait()
            ag3(m4).start()

        @pl.when(spread_out(m5))
        def _():
            ag3(m5).wait()
            fwd(m5).start()

        @pl.when(spread_out(m6))
        def _():
            fwd(m6).wait()

        return carry

    def rounds(lo, hi):
        lax.fori_loop(lo, hi, comm, 0)

    def ramp(lo, hi, i, n):
        return lo + (hi - lo) * i * i // (n * n)

    sets = (0, 1)
    dys = (dy_own, dy_nbr)

    def of(k):
        return pl.ds(k * tokens, tokens)

    def chunk_at(i):
        late, wait = hn - early, i // (2 * early)
        first = i // early * hn + i % early
        second = early + (i - 2 * early) // late * hn + (i - 2 * early) % late
        return first + wait * (second - first)

    def loads(layer, i):
        f0, slot = pl.multiple_of(chunk_at(i) * chunk, 128), i % 2
        return (
            pltpu.make_async_copy(w2.at[layer, pl.ds(f0, chunk)], w2c.at[slot], l_w2.at[slot]),
            pltpu.make_async_copy(w1.at[layer, :, pl.ds(f0, chunk)], w1c.at[slot], l_w1.at[slot]),
            *(pltpu.make_async_copy(u.at[k, layer, :, pl.ds(f0, chunk)], uc.at[slot, k], l_u.at[slot, k]) for k in sets),
        )

    def cols(i, size):
        return pl.ds(pl.multiple_of(i * size, 128), size)

    def a_load(layer, k):
        return pltpu.make_async_copy(a.at[k, layer], a_cat.at[of(k)], l_a.at[k])

    def h_load(layer, k):
        return pltpu.make_async_copy(h.at[k, layer], h_cat.at[of(k)], l_h.at[k])

    def gb_load(k):
        return pltpu.make_async_copy(dys[k], gb_cat.at[of(k)], l_gb.at[k])

    def dx_store():
        return pltpu.make_async_copy(gb_cat.at[of(0)], dx, l_dx)

    barrier = pltpu.get_barrier_semaphore()
    for to in (peer(X), peer(Y), peer(Z), sibling):
        pl.semaphore_signal(barrier, inc=1, device_id=to, device_id_type=MESH)
    for k in sets:
        gb_load(k).start()
        a_load(layers - 1, k).start()
    for k in sets:
        gb_load(k).wait()
    pl.semaphore_wait(barrier, 4)

    def layer_step(li, carry):
        layer = layers - 1 - li
        base = li * 2 * nu
        late = jnp.minimum(li, 1)
        due = [late * (4 * nu * (li - 1) + PACE[4] * nu // 10)]
        for p, q in zip(PACE_FIRST, PACE):
            due.append(4 * nu * li + p * nu // 10 + late * (q * nu // 10 - p * nu // 10))
        for k in sets:
            a_load(layer, k).wait()

        def second_weight(i, carry):
            n = base + i
            lhs = jnp.concatenate([a_cat[:, cols((1 - core) * nu + i, part)], a_cat[:, cols(core * nu + i, part)]], axis=1)
            out = mm(lhs, gb_cat[...], 0, 0)
            make(n, out[:part], out[part:])

            @pl.when(i >= 2)
            def _():
                pair_sum(n - 2)

            push(n)
            rounds(ramp(due[0], due[1], i, nu), ramp(due[0], due[1], i + 1, nu))
            return carry

        lax.fori_loop(0, nu, second_weight, 0)
        pair_sum(base + nu - 2)
        pair_sum(base + nu - 1)
        for k in sets:
            h_load(layer, k).start()

        @pl.when(li == 0)
        def _():
            for load in loads(layer, 0):
                load.start()
            for k in sets:
                g[of(k)] = gb_cat[of(k)].astype(F32)

        @pl.when(layer > 0)
        def _():
            for k in sets:
                a_load(layer - 1, k).start()

        def hidden_chunk(from_i, to_i, start, stop, i, carry):
            for load in loads(layer, i):
                load.wait()

            @pl.when(i < nu - 1)
            def _():
                for load in loads(layer, i + 1):
                    load.start()

            def token_set(k, carry):
                at = [pl.ds(q * step, step) for q in range(2)]
                rows_q = [pl.ds(pl.multiple_of(k * tokens + q * step, 16), step) for q in range(2)]
                d_act = [mm(gb_cat[r], w2c[i % 2], 1, 1) for r in rows_q]
                for q in range(2):
                    du = (d_act[q] * gelu_slope(uc[i % 2, k, at[q]].astype(F32))).astype(BF16)
                    du_cat[rows_q[q], cols(chunk_at(i), chunk)] = du
                    g[rows_q[q]] += mm(du, w1c[i % 2], 1, 1)
                s = 2 * (i - from_i) + k
                rounds(start + (stop - start) * s // (4 * early), start + (stop - start) * (s + 1) // (4 * early))
                return carry

            lax.fori_loop(0, 2, token_set, 0)
            return carry

        def first_weight(fi, start, stop, mi, carry):
            n = base + nu + fi * nm + mi
            lhs = h_cat[:, cols(mi, part)]
            make(
                n,
                mm(lhs, du_cat[:, cols((1 - core) * nf + fi, width)], 0, 0),
                mm(lhs, du_cat[:, cols(core * nf + fi, width)], 0, 0),
            )

            @pl.when(mi >= 2)
            def _():
                pair_sum(n - 2)

            push(n)
            rounds(ramp(start, stop, mi, nm), ramp(start, stop, mi + 1, nm))
            return carry

        def half_step(fi, carry):
            d0, d1, d2 = (due[k] + fi * (due[k + 2] - due[k]) for k in (1, 2, 3))
            from_i, to_i = fi * 2 * early, 2 * early + fi * (nu - 2 * early)
            lax.fori_loop(from_i, to_i, functools.partial(hidden_chunk, from_i, to_i, d0, d1), 0)
            rounds(d0 + (d1 - d0) * (to_i - from_i) // (2 * early), d1)

            @pl.when(fi == 0)
            def _():
                for k in sets:
                    h_load(layer, k).wait()

            @pl.when(fi == 1)
            def _():
                for k in sets:
                    gb_cat[of(k)] = g[of(k)].astype(BF16)

                @pl.when(layer > 0)
                def _():
                    for load in loads(layer - 1, 0):
                        load.start()

                @pl.when(layer == 0)
                def _():
                    dx_store().start()

            lax.fori_loop(0, nm, functools.partial(first_weight, fi, d1, d2), 0)
            pair_sum(base + nu + fi * nm + nm - 2)
            pair_sum(base + nu + fi * nm + nm - 1)
            return carry

        lax.fori_loop(0, nf, half_step, 0)
        return carry

    lax.fori_loop(0, layers, layer_step, 0)
    rounds(4 * nu * (layers - 1) + PACE[4] * nu // 10, pieces + 4 * LAG)
    dx_store().wait()


def backward(w_one, w_two, u, a, h, dy, dy_nbr, rows):
    layers, width, wide = w_one.shape
    tokens = dy.shape[0]
    half = wide // 2
    nu = half // rows
    chunk = wide // nu
    units = 2 * nu * layers
    dma, reg = pltpu.SemaphoreType.DMA, pltpu.SemaphoreType.REGULAR
    hbm = pl.BlockSpec(memory_space=pl.ANY)
    sub, narrow = rows // 8, width // 2
    shape = jax.ShapeDtypeStruct
    scratch = [
        pltpu.VMEM((2 * tokens, half), BF16),
        pltpu.VMEM((2 * tokens, wide), BF16),
        pltpu.VMEM((2 * tokens, width // 2), BF16),
        pltpu.VMEM((2 * tokens, width), BF16),
        pltpu.VMEM((2 * tokens, width), F32),
        pltpu.VMEM((2, chunk, width), BF16),
        pltpu.VMEM((2, width, chunk), BF16),
        pltpu.VMEM((2, 2, tokens, chunk), BF16),
        pltpu.VMEM((SLOTS, 4, sub, narrow), BF16),
        pltpu.VMEM((PARTS, 4, sub, width), BF16),
        pltpu.VMEM((RECV0, 4, sub, width), BF16),
        pltpu.VMEM((RECV, 2, sub, narrow), BF16),
        pltpu.VMEM((RECV, 1, sub, narrow), BF16),
        *[dma((SEMS,))] * 11,
        *[dma((RECV,))] * 2,
        *[reg((RECV,))] * 2,
        dma((PARTS,)), dma((RECV0,)), reg((RECV0,)),
        dma((2,)), dma((2,)), dma((2,)), dma((2,)), dma((2,)), dma((2, 2)), dma,
    ]
    return pl.pallas_call(
        functools.partial(backward_body, layers=layers, tokens=tokens, width=width, wide=wide, rows=rows),
        out_shape=[
            shape((2 * units - 2 * nu, 2, 8, sub, narrow), BF16),
            shape((tokens, width), BF16),
            shape((2 * nu, sub, narrow), BF16),
        ],
        in_specs=[hbm] * 7,
        out_specs=[hbm] * 3,
        scratch_shapes=scratch,
        compiler_params=pltpu.CompilerParams(collective_id=0, has_side_effects=True, vmem_limit_bytes=VMEM_LIMIT),
        name="backward",
    )(w_one, w_two, u, a, h, dy, dy_nbr)


COPY_SLOTS, COPY_LEAD = 40, 16


def assemble_body(tot, dx_in, one, two, dx, buf, dx_buf, s_in, s_out, s_dx, *, layers, nu, nm, width):
    items = 2 * tot.shape[0]
    narrow = width // 2

    def load(j):
        return pltpu.make_async_copy(tot.at[j // 2, j % 2], buf.at[j % COPY_SLOTS], s_in.at[j % COPY_SLOTS])

    def stores(j, run):
        m, core, slot = j // 2, j % 2, j % COPY_SLOTS
        n, side = m // 2, m % 2
        layer, i = layers - 1 - n // (2 * nu), n % nu
        mid = (m % 3) // 2
        for q in range(4):
            src = (1 - mid) * q + mid * (q % 2 * 2 + q // 2)
            span = buf.at[slot, pl.ds(src * 2, 2)]

            @pl.when((n // nu) % 2 == 0)
            def _():
                cols = pl.ds(pl.multiple_of(side * narrow, 128), narrow)
                run(pltpu.make_async_copy(span, two.at[layer, core * nu + i, pl.ds(2 * q, 2), :, cols], s_out.at[slot, q]))

            @pl.when((n // nu) % 2 == 1)
            def _():
                cols = pl.ds(pl.multiple_of((core * (nu // nm) + i // nm) * width + side * narrow, 128), narrow)
                run(pltpu.make_async_copy(span, one.at[layer, i % nm, pl.ds(2 * q, 2), :, cols], s_out.at[slot, q]))

    def step(j, carry):
        @pl.when(j >= COPY_SLOTS)
        def _():
            stores(j - COPY_SLOTS, lambda c: c.wait())

        @pl.when(j < items)
        def _():
            load(j).start()

        @pl.when(jnp.logical_and(j >= COPY_LEAD, j < items + COPY_LEAD))
        def _():
            load(j - COPY_LEAD).wait()
            stores(j - COPY_LEAD, lambda c: c.start())

        return carry

    dx_load = pltpu.make_async_copy(dx_in, dx_buf, s_dx.at[0])
    dx_store = pltpu.make_async_copy(dx_buf, dx, s_dx.at[1])
    dx_load.start()
    lax.fori_loop(0, COPY_SLOTS, step, 0)
    dx_load.wait()
    dx_store.start()
    lax.fori_loop(COPY_SLOTS, items + COPY_SLOTS, step, 0)
    dx_store.wait()


def finish_body(last, one_in, one, buf, s_in, s_out, *, nm, width, first):
    devices, count = last.shape[:2]
    narrow = width // 2

    def load(d):
        return pltpu.make_async_copy(last.at[d], buf.at[d], s_in.at[d])

    def store(d, p):
        m = first + p
        z, y, x, core = d // 8, d // 4 % 2, d // 2 % 2, d % 2
        mid = (m % 3) // 2
        a_axis = (1 - mid) * (m % 3) + mid * ((m // 3) % 2)
        row = 4 * z + 2 * (x + a_axis * (y - x)) + y + a_axis * (x - y)
        i, side = p // 2, p % 2
        cols = pl.ds(pl.multiple_of((core * 2 + i // nm) * width + side * narrow, 128), narrow)
        return pltpu.make_async_copy(buf.at[d, p], one.at[0, i % nm, row, :, cols], s_out)

    for d in range(devices):
        load(d).start()

    def out(d, carry):
        load(d).wait()
        for p in range(count):
            store(d, p).start()
        return carry

    lax.fori_loop(0, devices, out, 0)

    def done(d, carry):
        for p in range(count):
            store(d, p).wait()
        return carry

    lax.fori_loop(0, devices, done, 0)


def assemble(tot, dx, layers, width, wide, rows):
    nu, nm, sub = wide // 2 // rows, width // rows, rows // 8
    shape = jax.ShapeDtypeStruct
    hbm = pl.BlockSpec(memory_space=pl.ANY)
    return pl.pallas_call(
        functools.partial(assemble_body, layers=layers, nu=nu, nm=nm, width=width),
        out_shape=[shape((layers, nm, 8, sub, wide), BF16), shape((layers, 2 * nu, 8, sub, width), BF16), shape(dx.shape, BF16)],
        in_specs=[hbm] * 2,
        out_specs=[hbm] * 3,
        scratch_shapes=[
            pltpu.VMEM((COPY_SLOTS, 8, sub, width // 2), BF16),
            pltpu.VMEM(dx.shape, BF16),
            pltpu.SemaphoreType.DMA((COPY_SLOTS,)),
            pltpu.SemaphoreType.DMA((COPY_SLOTS, 4)),
            pltpu.SemaphoreType.DMA((2,)),
        ],
        compiler_params=pltpu.CompilerParams(vmem_limit_bytes=VMEM_LIMIT),
        cost_estimate=pl.CostEstimate(flops=400 * tot.size, bytes_accessed=4 * tot.size, transcendentals=0),
        name="assemble",
    )(tot, dx)


def finish(last, one, first, nm, width):
    hbm = pl.BlockSpec(memory_space=pl.ANY)
    return pl.pallas_call(
        functools.partial(finish_body, nm=nm, width=width, first=first),
        out_shape=jax.ShapeDtypeStruct(one.shape, BF16),
        in_specs=[hbm] * 2,
        out_specs=hbm,
        scratch_shapes=[pltpu.VMEM(last.shape, BF16), pltpu.SemaphoreType.DMA((last.shape[0],)), pltpu.SemaphoreType.DMA],
        input_output_aliases={1: 0},
        compiler_params=pltpu.CompilerParams(vmem_limit_bytes=VMEM_LIMIT),
        cost_estimate=pl.CostEstimate(flops=400 * last.size, bytes_accessed=4 * last.size, transcendentals=0),
        name="finish",
    )(last, one)


def solution(mesh, rows=UNIT_ROWS):
    batch_spec = P(AXES)

    def per_device(w_one, w_two, x_loc, dy_loc):
        layers, width, wide = w_one.shape
        x = x_loc.reshape(-1, width)
        dy = dy_loc.reshape(-1, width)
        u, a, h, _, dy_nbr, _ = forward(x, dy, w_one, w_two, rows)
        tot, dx, last = backward(w_one, w_two, u, a, h, dy, dy_nbr, rows)
        everyone = lax.all_gather(last, AXES)
        one, two, dx = assemble(tot, dx, layers, width, wide, rows)
        one = finish(everyone, one, tot.shape[0], width // rows, width)
        return one.reshape(w_one.shape), two.reshape(w_two.shape), dx.reshape(x_loc.shape)

    return jax.shard_map(per_device, mesh=mesh, in_specs=(P(), P(), batch_spec, batch_spec), out_specs=(P(), P(), batch_spec), check_vma=False)
```
